32 devices in a mesh: group: 4 (over z), expert: 8 (over y, x, core).
Axes of the slice: x: 2, y: 2, z: 4, core: 2. Of those that a mesh axis runs over, the one named last changes fastest.
Arguments:
- tokens_in: bfloat16 [16384, 1024], P(('group', 'expert')), may hold values from -6 to 6
- cotangent: bfloat16 [16384, 1024], P(('group', 'expert')), may hold values from -6 to 6
- hash_ids: int32 [16384, 1], P(('group', 'expert')), may hold values from 0 to 7; in each aligned block of 512 rows (0 to 511, 512 to 1023, ...) at most 128 rows name the same one
- norm1_gain: float32 [1024], replicated, may hold values from 0.5 to 1.5
- norm1_bias: float32 [1024], replicated, may hold values from -1 to 1
- w_query: bfloat16 [1024, 1024], replicated, may hold values from -0.25 to 0.25
- w_key: bfloat16 [1024, 1024], replicated, may hold values from -0.1875 to 0.1875
- w_value: bfloat16 [1024, 1024], replicated, may hold values from -0.1875 to 0.1875
- w_output: bfloat16 [1024, 1024], replicated, may hold values from -1.5 to 1.5
- norm2_gain: float32 [1024], replicated, may hold values from 0.5 to 1.5
- norm2_bias: float32 [1024], replicated, may hold values from -1 to 1
- expert_in: bfloat16 [8, 1024, 4096], P('expert'), may hold values from -0.1875 to 0.1875
- expert_out: bfloat16 [8, 4096, 1024], P('expert'), may hold values from -0.125 to 0.125
Outputs:
- result: bfloat16 [16384, 1024], P(('group', 'expert'))
- grad_tokens: bfloat16 [16384, 1024], P(('group', 'expert'))
- grad_norm1_gain: float32 [1024], P(('group', 'expert'))
- grad_norm1_bias: float32 [1024], P(('group', 'expert'))
- grad_w_query: float32 [1024, 1024], P(('group', 'expert'))
- grad_w_key: float32 [1024, 1024], P(('group', 'expert'))
- grad_w_value: float32 [1024, 1024], P(('group', 'expert'))
- grad_w_output: float32 [1024, 1024], P(('group', 'expert'))
- grad_norm2_gain: float32 [1024], P(('group', 'expert'))
- grad_norm2_bias: float32 [1024], P(('group', 'expert'))
- grad_expert_in: float32 [8, 1024, 4096], P('expert', 'group')
- grad_expert_out: float32 [8, 4096, 1024], P('expert', 'group')
The draws below stay inside these ranges and needn't reach their ends.
Inputs may be any that keep to these rules, and one draw needn't show every extreme that they name: `hash_ids`: each token's expert; among the 512 rows of one device at most 128 name one expert, a bound that some block reaches.
All inputs are finite; a program needn't handle non-finite values.
Results may differ from the reference program's by a relative error of at most 0.028.
Values may be sent and summed in bfloat16 or wider, within the bound.
No kernel may reach another device: no remote copies, remote signals or barrier semaphores. Data moves between devices by JAX's collectives and lax.ppermute only.
A program may use at most 320 MiB of HBM per device.

```python
import math
from functools import partial
import jax
import jax.numpy as jnp
import numpy as np
from jax import lax

D = 1024
HEADS = 16
HEAD = 64
FF = 4096
PROMPT_DEV = 128
CONT_DEV = 384
TOK_DEV = 512
EXPERTS = 8
CAP = 128
TOKENS = 16384
N_GROUP = 4
N_EXPERT = 8


def spiked(array, stream_key, source, target, shards_of, factor):
    def block_of(dim):
        return (jnp.arange(array.shape[dim]) // (array.shape[dim] // shards_of)).reshape((-1,) + (1,) * (array.ndim - 1 - dim))

    near = jax.random.permutation(stream_key, shards_of)[block_of(target)]
    far = (block_of(target) + shards_of // 2) % shards_of
    return jnp.where((block_of(source) == near) | (block_of(source) == far), factor * array, array)


def level_of(rng, shape, cuts, least, largest):
    factor_of, own = 1.0, jax.random.fold_in(rng, 6)
    for dim, shards_of in cuts:
        draws = jnp.exp(jax.random.uniform(jax.random.fold_in(own, dim), (shards_of,), jnp.float32, least / len(cuts), largest / len(cuts)))
        factor_of = factor_of * jnp.repeat(draws, shape[dim] // shards_of).reshape([-1 if axis == dim else 1 for axis in range(len(shape))])
    return factor_of


def shared_out(rng, own, number, rows, count, top, reach, lean):
    ranking = jax.random.permutation(rng, count)
    crowded, usual = portions_of(count, rows * top, reach, lean, True), portions_of(count, rows * top, reach, lean, False)
    places = jnp.arange(count)

    def named(lengths, rotation):
        used = int((lengths > 0).sum())
        fixed = max(1, used // 4)
        passed = fixed + (places - fixed + rotation * (used - fixed)) % max(1, count - fixed)
        return jnp.zeros((count,), jnp.int32).at[ranking[jnp.where(places < fixed, places, passed)]].set(jnp.asarray(lengths, jnp.int32))

    lengths = jnp.where(number % 4 == 0, named(crowded, number // 4), named(usual, number - number // 4 - 1))
    mixed = jax.random.permutation(jax.random.fold_in(own, 3), count)
    giver, sink = mixed[0:count // 2 * 2:2], mixed[1:count // 2 * 2:2]
    room = jnp.minimum(lengths[giver] - 1, reach - lengths[sink]) // 2
    room = jnp.where((giver == ranking[0]) | (sink == ranking[0]) | (lengths[sink] == 0), 0, jnp.maximum(room, 0))
    passed = jax.random.randint(jax.random.fold_in(own, 4), (count // 2,), 0, 1 << 20) % (room + 1)
    lengths = lengths.at[giver].add(-passed).at[sink].add(passed)
    members = jnp.searchsorted(jnp.cumsum(lengths), jnp.arange(rows * top), side="right").astype(jnp.int32)
    listing = members.reshape(top, rows).T
    listing = listing[jax.random.permutation(jax.random.fold_in(own, 1), rows)]
    rotation = jax.random.randint(jax.random.fold_in(own, 2), (rows, 1), 0, top)
    return jnp.take_along_axis(listing, (jnp.arange(top)[None, :] + rotation) % top, axis=1)


def portions_of(count, total, limit, skew, full):
    weights = [(1 << 20) // math.isqrt(standing ** skew) + 1 for standing in range(1, count + 1)]
    largest = limit if full else min(limit, max(-(-total // count), total * weights[0] // sum(weights)))
    least = 1 if total - largest >= count - 1 else 0
    given, spare = [largest] + [least] * (count - 1), total - largest - least * (count - 1)
    while spare > 0:
        candidates = [i for i in range(1, count) if given[i] < largest] or [i for i in range(1, count) if given[i] < limit]
        whole, budget = sum([weights[i] for i in candidates]), spare
        for i in candidates:
            addition = min(limit - given[i], max(1, budget * weights[i] // whole), spare)
            given[i] = given[i] + addition
            spare = spare - addition
    return np.array(given)


def gaussian(key, extent, spread, most, cuts=(), kind=jnp.bfloat16):
    drawn = jax.random.normal(key, extent, jnp.float32) * spread
    if len(cuts) > 0:
        drawn = level_of(key, extent, cuts, -0.22, 0.18) * drawn
    return jnp.clip(drawn, min=-most, max=most).astype(kind)


def gaussian_with(key, dims, scale, limit, shards, heavy, kind=jnp.bfloat16):
    values = scale * jax.random.normal(key, dims, jnp.float32)
    if shards:
        values = values * level_of(key, dims, shards, -0.22, 0.18)
    return jnp.clip(spiked(values, jax.random.fold_in(key, 3), *heavy), -limit, limit).astype(kind)


def setup_inputs(seed: int = 0) -> dict:
    streams_of = jax.random.split(jax.random.key(seed), 14)
    tokens_in = gaussian_with(streams_of[0], (TOKENS, D), 1.0, 6.0, ((0, 32),), (0, 1, 32, 2.75))
    cotangent = gaussian(streams_of[1], (TOKENS, D), 1.0, 6.0, ((0, 32),))
    hash_ids_keys = jax.random.split(jax.random.fold_in(streams_of[2], 1), TOKENS // TOK_DEV)
    hash_ids_turns = jax.random.permutation(jax.random.fold_in(streams_of[2], 3), TOKENS // TOK_DEV)
    hash_ids = jax.vmap(lambda own, number: shared_out(jax.random.fold_in(streams_of[2], 2), own, number, TOK_DEV, EXPERTS, 1, CAP, 2))(hash_ids_keys, hash_ids_turns).reshape((TOKENS, 1))
    norm1_gain = jnp.clip(1.0 + 0.1 * jax.random.normal(streams_of[3], (D,), jnp.float32), 0.5, 1.5)
    norm1_bias = gaussian(streams_of[4], (D,), 0.2, 1.0, (), jnp.float32)
    w_query = gaussian(streams_of[5], (D, D), (D // 2) ** -0.5, 0.25)
    w_key = gaussian(streams_of[6], (D, D), D ** -0.5, 0.1875)
    w_value = gaussian(streams_of[7], (D, D), D ** -0.5, 0.1875)
    w_output = gaussian(streams_of[8], (D, D), (D // 64) ** -0.5, 1.5)
    norm2_gain = jnp.clip(1.0 + 0.1 * jax.random.normal(streams_of[9], (D,), jnp.float32), 0.5, 1.5)
    norm2_bias = gaussian(streams_of[10], (D,), 0.2, 1.0, (), jnp.float32)
    expert_in = gaussian(streams_of[11], (EXPERTS, D, FF), D ** -0.5, 0.1875, ((0, 8),))
    expert_out = gaussian(streams_of[12], (EXPERTS, FF, D), (FF // 2) ** -0.5, 0.125, ((0, 8),))
    return {"tokens_in": tokens_in, "cotangent": cotangent, "hash_ids": hash_ids, "norm1_gain": norm1_gain, "norm1_bias": norm1_bias, "w_query": w_query, "w_key": w_key, "w_value": w_value, "w_output": w_output, "norm2_gain": norm2_gain, "norm2_bias": norm2_bias, "expert_in": expert_in, "expert_out": expert_out}


@jax.custom_vjp
def low(v):
    return lax.optimization_barrier(v.astype(jnp.bfloat16)).astype(jnp.float32)

@jax.custom_vjp
def low_back(v):
    return v

def low_keep(v):
    return (low(v), None)

def low_pass(kept, grad):
    return (grad,)

def back_keep(v):
    return (v, None)

def back_low(kept, grad):
    return (low(grad),)
low.defvjp(low_keep, low_pass)
low_back.defvjp(back_keep, back_low)
norm_eps = 1e-05
masked_score = -1e+30
highest = lax.Precision.HIGHEST

def layer_norm(values, gain, shift):
    average = lax.optimization_barrier(jnp.mean(values, axis=-1, keepdims=True))
    centered = values - average
    variance = lax.optimization_barrier(jnp.mean(centered * centered, axis=-1, keepdims=True))
    return centered * lax.rsqrt(variance + norm_eps) * gain + shift

def attention_mask():
    token_index = jnp.arange(N_EXPERT * TOK_DEV, dtype=jnp.int32)
    device = token_index // TOK_DEV
    within = token_index % TOK_DEV
    prompt = within < PROMPT_DEV
    positions = jnp.where(prompt, device * PROMPT_DEV + within, device % 2 * CONT_DEV + within - PROMPT_DEV)
    member = jnp.where(prompt, -1, device // 2)
    earlier = positions[None, :] <= positions[:, None]
    from_prompt = prompt[None, :] & (jnp.logical_not(prompt)[:, None] | earlier)
    same_cont = jnp.logical_not(prompt)[None, :] & jnp.logical_not(prompt)[:, None] & (member[None, :] == member[:, None]) & earlier
    return from_prompt | same_cont

def expert_slots(hash_ids):
    per_device = hash_ids.reshape(N_GROUP * N_EXPERT, TOK_DEV).astype(jnp.int32)
    routed = (per_device[:, :, None] == jnp.arange(EXPERTS, dtype=jnp.int32)[None, None, :]).astype(jnp.int32)
    running = jnp.cumsum(routed, axis=1)
    rank = lax.optimization_barrier(jnp.sum(running * routed, axis=-1)) - 1
    device = jnp.arange(N_GROUP * N_EXPERT, dtype=jnp.int32)[:, None]
    group_index = device // N_EXPERT
    source = device % N_EXPERT
    return (((group_index * EXPERTS + per_device) * N_EXPERT + source) * CAP + rank).reshape(-1).astype(jnp.int32)

def split_heads(matrix):
    return matrix.reshape(matrix.shape[0], HEADS, HEAD).transpose(1, 0, 2)

def attention_group(operands, allowed):
    queries, key_rows, value_rows = operands
    score_scale = 1.0 / math.sqrt(HEAD)

    def one_head(head_operands):
        query_head, key_head, value_head = head_operands
        scores = low_back(score_scale * jnp.einsum('qd,kd->qk', query_head, key_head, precision=highest))
        scores = jnp.where(allowed, scores, masked_score)
        probabilities = low(jax.nn.softmax(scores, axis=-1))
        return jnp.einsum('qk,kd->qd', probabilities, value_head, precision=highest)
    stacked = lax.map(jax.checkpoint(one_head), (split_heads(queries), split_heads(key_rows), split_heads(value_rows)))
    return stacked.transpose(1, 0, 2).reshape(queries.shape[0], D)

def expert_pass(operands):
    rows, first_matrix, second_matrix = operands
    pre_act = low_back(jnp.einsum('grd,df->grf', rows, first_matrix, precision=highest))
    hidden = low(jax.nn.silu(pre_act))
    return low_back(low(jnp.einsum('grf,fd->grd', hidden, second_matrix, precision=highest)))

def forward(inputs, gain1, bias1, w_q, w_k, w_v, w_o, gain2, bias2, w_in, w_out, slots, allowed):
    grouped = inputs.reshape(N_GROUP, N_EXPERT * TOK_DEV, D)
    attn_in = low(layer_norm(grouped, gain1, bias1))
    queries = low_back(low(jnp.einsum('gtd,de->gte', attn_in, w_q, precision=highest)))
    key_rows = low_back(low(jnp.einsum('gtd,de->gte', attn_in, w_k, precision=highest)))
    value_rows = low_back(low(jnp.einsum('gtd,de->gte', attn_in, w_v, precision=highest)))
    attended = lax.map(partial(attention_group, allowed=allowed), (queries, key_rows, value_rows))
    attended = low_back(low(attended))
    attn_out = low_back(jnp.einsum('gtd,de->gte', attended, w_o, precision=highest))
    residual = grouped + attn_out
    ffn_in = low_back(low(layer_norm(residual, gain2, bias2)))
    flat = ffn_in.reshape(-1, D)
    buffer = jnp.zeros((N_GROUP * EXPERTS * N_EXPERT * CAP, D), jnp.float32).at[slots].set(flat)
    blocks = buffer.reshape(N_GROUP, EXPERTS, N_EXPERT * CAP, D).transpose(1, 0, 2, 3)
    produced = lax.map(jax.checkpoint(expert_pass), (blocks, w_in, w_out))
    flat_out = produced.transpose(1, 0, 2, 3).reshape(-1, D)
    expert_rows = flat_out[slots]
    return residual.reshape(-1, D) + expert_rows

def reference(tokens_in, cotangent, hash_ids, norm1_gain, norm1_bias, w_query, w_key, w_value, w_output, norm2_gain, norm2_bias, expert_in, expert_out):
    slots = expert_slots(hash_ids)
    allowed = attention_mask()
    function = partial(forward, slots=slots, allowed=allowed)
    primals = (tokens_in.astype(jnp.float32), norm1_gain.astype(jnp.float32), norm1_bias.astype(jnp.float32), w_query.astype(jnp.float32), w_key.astype(jnp.float32), w_value.astype(jnp.float32), w_output.astype(jnp.float32), norm2_gain.astype(jnp.float32), norm2_bias.astype(jnp.float32), expert_in.astype(jnp.float32), expert_out.astype(jnp.float32))
    output, pullback = jax.vjp(function, *primals)
    grads = pullback(cotangent.astype(jnp.float32))
    return (output.astype(jnp.bfloat16), grads[0].astype(jnp.bfloat16), grads[1], grads[2], grads[3], grads[4], grads[5], grads[6], grads[7], grads[8], grads[9], grads[10])
```

```python
import functools
import math

import jax
import jax.numpy as jnp
from jax import lax
from jax.experimental import pallas as pl
from jax.experimental.pallas import tpu as pltpu
from jax.sharding import PartitionSpec as P

HEADS = 16
PROMPT_DEV = 128
CONT_DEV = 384


norm_eps = 1e-05
masked_score = -1e30
bf16 = jnp.bfloat16
f32 = jnp.float32
MIB = 1 << 20
share = 0.05
link_pieces = 2


def swapped(block, axis, mask):
    return lax.ppermute(block, axis, [(i, i ^ mask) for i in range(lax.axis_size(axis))])


def rounded(values):
    return values.astype(bf16)


def normalize(values, gain, shift):
    average = jnp.mean(values, axis=-1, keepdims=True)
    centered = values - average
    variance = jnp.mean(centered * centered, axis=-1, keepdims=True)
    inverse = lax.rsqrt(variance + norm_eps)
    normed = centered * inverse
    return (normed * gain + shift, normed, inverse)


def norm_back(grad_out, gain, normed, inverse):
    scaled = grad_out * gain
    first_mean = jnp.mean(scaled, axis=-1, keepdims=True)
    second = jnp.mean(scaled * normed, axis=-1, keepdims=True)
    return inverse * (scaled - first_mean - normed * second)


def matmul(a, b, kind=f32):
    return jnp.dot(a, b, preferred_element_type=f32).astype(kind)


def matmul_nt(a, b, kind=f32):
    return lax.dot_general(a, b, (((1,), (1,)), ((), ())), preferred_element_type=f32).astype(kind)


def matmul_tn(a, b, kind=f32):
    return lax.dot_general(a, b, (((0,), (0,)), ((), ())), preferred_element_type=f32).astype(kind)


def outer_bits(size):
    return range(size.bit_length() - 2, 0, -1)


def gather_relative(block, axis, more):
    size = lax.axis_size(axis)
    pieces = {0: block}
    ready = [0]
    while ready:
        fresh = {}
        for r in ready:
            for bit in outer_bits(size):
                if r ^ (1 << bit) not in pieces and r ^ (1 << bit) not in fresh:
                    fresh[r ^ (1 << bit)] = swapped(pieces[r], axis, 1 << bit)
        fresh, more = lax.optimization_barrier((fresh, more))
        pieces.update(fresh)
        ready = list(fresh)
    near = sorted(pieces)
    for r in near:
        pieces[r ^ 1] = swapped(pieces[r], axis, 1)
    order = near + [r ^ 1 for r in near]
    return [pieces[r] for r in order], order, more


def scatter_relative(near, far, axis):
    size = lax.axis_size(axis)
    both = added(near, swapped(far, axis, 1))
    count = size // 2
    rows = both.shape[1] // count
    pieces = {2 * i: rounded(both[:, i * rows : (i + 1) * rows]) for i in range(count)}
    bits = list(outer_bits(size))
    for r in sorted(pieces, key=lambda r: -bin(r).count("1")):
        ways = [bit for bit in bits if r >> bit & 1]
        if not ways:
            continue
        piece = pieces.pop(r)
        part = rows // len(ways) if rows % len(ways) == 0 else rows
        if part % 16 or len(ways) == 1:
            ways, part = ways[:1], rows
        for i, bit in enumerate(ways):
            got = swapped(piece[:, i * part : (i + 1) * part], axis, 1 << bit)
            target = pieces[r ^ (1 << bit)]
            span = slice(i * part, (i + 1) * part)
            pieces[r ^ (1 << bit)] = rounded(
                jnp.concatenate(
                    [
                        target[:, : span.start].astype(f32),
                        added(target[:, span], got),
                        target[:, span.stop :].astype(f32),
                    ],
                    axis=1,
                )
            )
    return pieces[0]


def halved(blocks, place, axis, bit):
    own = (lax.axis_index(axis) >> bit) & 1
    return (
        lax.dynamic_index_in_dim(blocks, own, place, keepdims=False),
        lax.dynamic_index_in_dim(blocks, 1 - own, place, keepdims=False),
    )


def added(keep, got):
    return keep.astype(f32) + got.astype(f32)


def places_of(bits, bit, value):
    rest = [other for other in bits if other != bit]
    weight = {other: 1 << (len(bits) - 1 - i) for i, other in enumerate(bits)}
    places = []
    for number in range(1 << len(rest)):
        place = value * weight[bit]
        for i, other in enumerate(rest):
            place = place + (number >> (len(rest) - 1 - i) & 1) * weight[other]
        places.append(place)
    return places


def halve_kernel(bits, bit, own_ref, keep_ref, got_ref, own_out_ref, send_ref):
    own = (own_ref[0] >> bit) & 1
    for ref, value in ((own_out_ref, own), (send_ref, 1 - own)):
        for i, place in enumerate(places_of(bits, bit, value)):
            ref[0, 0, i] = rounded(added(keep_ref[0, 0, place], got_ref[0, 0, place]))


def halve(number, keep, got, first, bits, bit):
    _, groups, count, rows, width = keep.shape
    shape = (2, groups, count // 2, rows, width)
    came = pl.BlockSpec((1, 1, count, rows, width), lambda i, j: (first + i, j, 0, 0, 0))
    out = pl.BlockSpec((1, 1, count // 2, rows, width), lambda i, j: (i, j, 0, 0, 0))
    return pl.pallas_call(
        functools.partial(halve_kernel, bits, bit),
        grid=(2, groups),
        in_specs=[pl.BlockSpec(memory_space=pltpu.SMEM), came, came],
        out_specs=[out, out],
        out_shape=[jax.ShapeDtypeStruct(shape, bf16)] * 2,
        compiler_params=params("arbitrary", "arbitrary"),
        cost_estimate=cost(2 * keep.size, 4 * keep.size),
        name="halve",
    )(number, keep, got)


def turn_kernel(own_ref, *refs):
    (*sets, own_out_ref, send_ref) = refs
    own = own_ref[0] & 1
    start = 0
    for keep_ref, got_ref in zip(sets[::2], sets[1::2]):
        for i in range(keep_ref.shape[0]):
            for j in range(keep_ref.shape[1] // 2):
                for ref, value in ((own_out_ref, own), (send_ref, 1 - own)):
                    place = 2 * j + value
                    ref[start + i, j] = rounded(added(keep_ref[i, place, 0], got_ref[i, place, 0]))
        start += keep_ref.shape[0]


def turn(number, sets):
    _, groups, _, rows, width = sets[0].shape
    shape = (4, groups // 2, rows, width)
    return pl.pallas_call(
        turn_kernel,
        in_specs=[pl.BlockSpec(memory_space=pltpu.SMEM)]
        + [pl.BlockSpec(memory_space=pltpu.VMEM)] * len(sets),
        out_specs=[pl.BlockSpec(memory_space=pltpu.VMEM)] * 2,
        out_shape=[jax.ShapeDtypeStruct(shape, bf16)] * 2,
        compiler_params=params(),
        cost_estimate=cost(8 * sets[0].size, 8 * sets[0].size),
        name="turn",
    )(number, *sets)


def expert_sums(keep, send, link_step):
    bits = list(range(1, lax.axis_size("expert").bit_length() - 1))
    number = lax.axis_index("expert")[None]
    got = swapped(send, "expert", 1)
    states = [(keep, got, 0, bits[::-1]), (keep, got, 2, bits[::-1])]
    for step, pair in enumerate(zip(bits, bits[::-1])):
        halves = [
            halve(number, keep, got, first, left, bit)
            for (keep, got, first, left), bit in zip(states, pair)
        ]
        states = [
            (keep, swapped(send, "expert", 1 << bit), 0, [other for other in state[3] if other != bit])
            for state, bit, (keep, send) in zip(states, pair, halves)
        ]
        if step == 0:
            gots = link_step([state[1] for state in states])
            states = [(keep, got, zero, left) for (keep, _, zero, left), got in zip(states, gots)]
    sets = [value for state in states for value in state[:2]]
    return turn(lax.axis_index("group")[None], sets)


def group_sums(keep, send):
    groups = lax.axis_size("group")
    both = added(keep, swapped(send, "group", 1))
    bits = list(range(1, groups.bit_length() - 1))
    both = both.reshape((4,) + (2,) * len(bits) + both.shape[-2:])
    left = bits[::-1]
    for bit in bits:
        keep, send = halved(rounded(both), 1 + left.index(bit), "group", bit)
        left.remove(bit)
        both = added(keep, swapped(send, "group", 1 << bit))
    return [both[i] for i in range(both.shape[0])]


def vector_sums(vectors):
    axes = ("group", "expert")
    count = lax.axis_size("group") * lax.axis_size("expert")
    stacked = jnp.stack(vectors)
    pieces = stacked.reshape(len(vectors), count, -1).transpose(1, 0, 2)
    got = lax.all_to_all(pieces, axes, split_axis=0, concat_axis=0, tiled=True)
    return jnp.sum(got, axis=0)


def params(*semantics, vmem=48):
    return pltpu.CompilerParams(dimension_semantics=semantics, vmem_limit_bytes=vmem * MIB)


def cost(flops, total_bytes, exps=0):
    return pl.CostEstimate(
        flops=int(flops * share), bytes_accessed=int(total_bytes * share), transcendentals=int(exps * share)
    )


def logistic(values):
    return 0.5 * jnp.tanh(0.5 * values) + 0.5


def back_kernel(cot_ref, wout_ref, out_ref):
    out_ref[...] = matmul_nt(cot_ref[...], wout_ref[0], bf16)


def expert_back(cot, expert_out):
    count, width = cot.shape
    ff = expert_out.shape[1]
    block = 1024
    return pl.pallas_call(
        back_kernel,
        grid=(ff // block,),
        in_specs=[
            pl.BlockSpec((count, width), lambda j: (0, 0)),
            pl.BlockSpec((1, block, width), lambda j: (0, j, 0)),
        ],
        out_specs=pl.BlockSpec((count, block), lambda j: (0, j)),
        out_shape=jax.ShapeDtypeStruct((count, ff), bf16),
        compiler_params=params("arbitrary"),
        cost_estimate=cost(2 * count * width * ff, 2 * count * ff + 2 * width * ff),
        name="expert_back",
    )(cot, expert_out)


def front_kernel(parts, rows_ref, gh_ref, win_ref, hidden_ref, pre_ref, out_ref, acc_ref):
    step = pl.program_id(0)
    count = rows_ref.shape[0] // parts

    @pl.when(step == 0)
    def _():
        acc_ref[...] = jnp.zeros_like(acc_ref)

    first = lambda i: matmul(rows_ref[i * count : (i + 1) * count, :], win_ref[0])
    pre = first(0)
    for i in range(parts):
        later = first(i + 1) if i + 1 < parts else None
        here = pl.ds(i * count, count)
        sig = logistic(pre)
        hidden = pre * sig
        hidden_ref[here, :] = rounded(hidden)
        grad_pre = rounded(gh_ref[here, :].astype(f32) * sig * (1.0 + pre - hidden))
        pre_ref[here, :] = grad_pre
        acc_ref[here, :] += matmul_nt(grad_pre, win_ref[0])
        pre = later

    @pl.when(step == pl.num_programs(0) - 1)
    def _():
        out_ref[...] = rounded(acc_ref[...])


def expert_front(rows, grad_hidden, expert_in):
    count, width = rows.shape
    ff = expert_in.shape[2]
    block = 1024
    whole = pl.BlockSpec((count, width), lambda j: (0, 0))
    part = pl.BlockSpec((count, block), lambda j: (0, j))
    return pl.pallas_call(
        functools.partial(front_kernel, 4),
        grid=(ff // block,),
        in_specs=[whole, part, pl.BlockSpec((1, width, block), lambda j: (0, 0, j))],
        out_specs=[part, part, whole],
        out_shape=[
            jax.ShapeDtypeStruct((count, ff), bf16),
            jax.ShapeDtypeStruct((count, ff), bf16),
            jax.ShapeDtypeStruct((count, width), bf16),
        ],
        scratch_shapes=[pltpu.VMEM((count, width), f32)],
        compiler_params=params("arbitrary"),
        cost_estimate=cost(4 * count * width * ff, 6 * count * ff + 2 * width * ff, count * ff),
        name="expert_front",
    )(rows, grad_hidden, expert_in)


def produce_kernel(hidden_ref, wout_ref, out_ref, acc_ref):
    step = pl.program_id(0)
    part = matmul(hidden_ref[...], wout_ref[0])

    @pl.when(step == 0)
    def _():
        acc_ref[...] = part

    @pl.when(step > 0)
    def _():
        acc_ref[...] += part

    @pl.when(step == pl.num_programs(0) - 1)
    def _():
        out_ref[...] = rounded(acc_ref[...])


def expert_produce(hidden, expert_out):
    count, ff = hidden.shape
    width = expert_out.shape[2]
    block = 1024
    return pl.pallas_call(
        produce_kernel,
        grid=(ff // block,),
        in_specs=[
            pl.BlockSpec((count, block), lambda j: (0, j)),
            pl.BlockSpec((1, block, width), lambda j: (0, j, 0)),
        ],
        out_specs=pl.BlockSpec((count, width), lambda j: (0, 0)),
        out_shape=jax.ShapeDtypeStruct((count, width), bf16),
        scratch_shapes=[pltpu.VMEM((count, width), f32)],
        compiler_params=params("arbitrary"),
        cost_estimate=cost(2 * count * width * ff, 2 * count * ff + 2 * width * ff),
        name="expert_produce",
    )(hidden, expert_out)


def partner_kernel(rows_ref, cot_ref, win_ref, wout_ref, pre_ref):
    pre = matmul(rows_ref[...], win_ref[0])
    grad_hidden = matmul_nt(cot_ref[...], wout_ref[0])
    sig = logistic(pre)
    pre_ref[...] = rounded(grad_hidden * sig * (1.0 + pre * (1.0 - sig)))


def expert_partner(rows, cot, expert_in, expert_out):
    count, width = rows.shape
    ff = expert_in.shape[2]
    block = 512
    whole = pl.BlockSpec((count, width), lambda j: (0, 0))
    return pl.pallas_call(
        partner_kernel,
        grid=(ff // block,),
        in_specs=[
            whole,
            whole,
            pl.BlockSpec((1, width, block), lambda j: (0, 0, j)),
            pl.BlockSpec((1, block, width), lambda j: (0, j, 0)),
        ],
        out_specs=pl.BlockSpec((count, block), lambda j: (0, j)),
        out_shape=jax.ShapeDtypeStruct((count, ff), bf16),
        compiler_params=params("arbitrary"),
        cost_estimate=cost(4 * count * width * ff, 2 * count * ff + 4 * width * ff, count * ff),
        name="expert_partner",
    )(rows, cot, expert_in, expert_out)


def out_kernel(which_ref, hidden_ref, cot_ref, rows_ref, win_ref, cot_par_ref, *refs):
    pre = matmul(rows_ref[...], win_ref[0])
    total = matmul_tn(hidden_ref[...], cot_ref[...])
    hidden_par = rounded(pre * logistic(pre))
    total = total + matmul_tn(hidden_par, cot_par_ref[...])
    for ref in refs[:-1]:
        total = total + ref[...].astype(f32)
    refs[-1][...] = total.astype(refs[-1].dtype)


def out_slice(which, hidden, cot, rows_par, expert_in, cot_par, groups, kind, more=()):
    count, ff = hidden.shape
    width = cot.shape[1]
    part = ff // groups
    block = min(512, part)
    per = part // block
    whole = pl.BlockSpec((count, width), lambda j, w: (0, 0))
    piece = pl.BlockSpec((block, width), lambda j, w: (j, 0))
    return pl.pallas_call(
        out_kernel,
        grid_spec=pltpu.PrefetchScalarGridSpec(
            num_scalar_prefetch=1,
            grid=(per,),
            in_specs=[
                pl.BlockSpec((count, block), lambda j, w: (0, w[0] * per + j)),
                whole,
                whole,
                pl.BlockSpec((1, width, block), lambda j, w: (0, 0, w[0] * per + j)),
                whole,
            ]
            + [piece] * len(more),
            out_specs=piece,
        ),
        out_shape=jax.ShapeDtypeStruct((part, width), kind),
        compiler_params=params("arbitrary"),
        cost_estimate=cost(6 * count * width * part, 6 * count * width + 4 * width * part, count * part),
        name="out_slice",
    )(which, hidden, cot, rows_par, expert_in, cot_par, *more)


def in_kernel(which_ref, rows_ref, pre_ref, rows_par_ref, pre_par_ref, *out_refs):
    total = matmul_tn(rows_ref[...], pre_ref[...]) + matmul_tn(rows_par_ref[...], pre_par_ref[...])
    if len(out_refs) == 1:
        out_refs[0][...] = total.astype(out_refs[0].dtype)
    else:
        step = pl.program_id(0)
        width = total.shape[1]
        for i, ref in enumerate(out_refs):
            for j in range(ref.shape[1] // width):

                @pl.when(step == i * (ref.shape[1] // width) + j)
                def _(ref=ref, j=j):
                    ref[:, j * width : (j + 1) * width] = total.astype(ref.dtype)


def in_slice(which, rows, grad_pre, rows_par, pre_par, groups, kind, pieces=1):
    count, width = rows.shape
    ff = grad_pre.shape[1]
    part = width // groups
    block = 1024
    left = pl.BlockSpec((count, part), lambda j, w: (0, w[0]))
    right = pl.BlockSpec((count, block), lambda j, w: (0, j))
    if pieces == 1:
        outs = [pl.BlockSpec((part, block), lambda j, w: (0, j))]
    else:
        outs = [pl.BlockSpec((part, ff // pieces), lambda j, w: (0, 0))] * pieces
    return pl.pallas_call(
        in_kernel,
        grid_spec=pltpu.PrefetchScalarGridSpec(
            num_scalar_prefetch=1,
            grid=(ff // block,),
            in_specs=[left, right, left, right],
            out_specs=outs,
        ),
        out_shape=[jax.ShapeDtypeStruct((part, ff // pieces), kind)] * pieces,
        compiler_params=params("arbitrary"),
        cost_estimate=cost(4 * count * ff * part, 4 * count * (ff + part) + 4 * ff * part),
        name="in_slice",
    )(which, rows, grad_pre, rows_par, pre_par)


def sum_pieces(own, parts):
    rows, ff = own.shape
    pieces = len(parts[0])
    block = ff // pieces
    whole = pl.BlockSpec((rows, ff), lambda j: (0, 0))

    def kernel(own_ref, *refs):
        out_ref = refs[-1]
        for i in range(pieces):
            here = pl.ds(i * block, block)
            total = own_ref[:, here]
            for k in range(len(parts)):
                total = total + refs[k * pieces + i][...].astype(f32)
            out_ref[0, :, here] = total

    tall = min(rows, 64)
    return pl.pallas_call(
        kernel,
        grid=(rows // tall,),
        in_specs=[pl.BlockSpec((tall, ff), lambda j: (j, 0))]
        + [pl.BlockSpec((tall, block), lambda j: (j, 0))] * (pieces * len(parts)),
        out_specs=pl.BlockSpec((1, tall, ff), lambda j: (0, j, 0)),
        out_shape=jax.ShapeDtypeStruct((1, rows, ff), f32),
        compiler_params=params("arbitrary"),
        cost_estimate=cost(rows * ff, 10 * rows * ff),
        name="sum_pieces",
    )(own, *[p for some in parts for p in some])


def project_kernel(count, gain_ref, bias_ref, wq_ref, wk_ref, wv_ref, *refs):
    pieces, (in_ref, q_ref, k_ref, v_ref, scratch) = refs[:count], refs[count:]

    @pl.when(pl.program_id(0) == 0)
    def _():
        start = 0
        for ref in pieces:
            end = start + ref.shape[0]
            values = normalize(ref[...].astype(f32), gain_ref[...], bias_ref[...])[0]
            scratch[start:end, :] = rounded(values)
            start = end
        in_ref[...] = scratch[...]

    first, last = pieces[0].shape[0], pieces[-1].shape[0]
    size = scratch.shape[0]
    q_ref[:first, :] = matmul(scratch[:first, :], wq_ref[...], bf16)
    q_ref[first:, :] = matmul(scratch[size - last :, :], wq_ref[...], bf16)
    k_ref[...] = matmul(scratch[...], wk_ref[...], bf16)
    v_ref[...] = matmul(scratch[...], wv_ref[...], bf16)


def project(pieces, gain, shift, w_query, w_key, w_value):
    width = gain.shape[0]
    size = sum(p.shape[0] for p in pieces)
    own = pieces[0].shape[0] + pieces[-1].shape[0]
    block = 512
    whole = lambda rows: pl.BlockSpec((rows, width), lambda j: (0, 0))
    weights = pl.BlockSpec((width, block), lambda j: (0, j))
    columns = lambda rows: pl.BlockSpec((rows, block), lambda j: (0, j))
    return pl.pallas_call(
        functools.partial(project_kernel, len(pieces)),
        grid=(width // block,),
        in_specs=[whole(1), whole(1)] + [weights] * 3 + [whole(p.shape[0]) for p in pieces],
        out_specs=[whole(size), columns(own), columns(size), columns(size)],
        out_shape=[jax.ShapeDtypeStruct((rows, width), bf16) for rows in (size, own, size, size)],
        scratch_shapes=[pltpu.VMEM((size, width), bf16)],
        compiler_params=params("arbitrary"),
        cost_estimate=cost(4 * size * width * width, 8 * size * width + 4 * width * width),
        name="project",
    )(gain[None], shift[None], w_query, w_key, w_value, *pieces)


def weights_kernel(odd_ref, *refs):
    attended_ref, others_ref, grad_ref, dq_ref, *backs = refs[:-2]
    keep_ref, send_ref = refs[-2:]
    size = others_ref.shape[0]
    totals = [
        matmul_tn(attended_ref[...], grad_ref[...]),
        matmul_tn(others_ref[:PROMPT_DEV, :], dq_ref[:PROMPT_DEV, :])
        + matmul_tn(others_ref[size - CONT_DEV :, :], dq_ref[PROMPT_DEV:, :]),
    ]
    for i in range(2):
        total, start = None, 0
        for ref in backs:
            count = ref.shape[1]
            part = matmul_tn(others_ref[start : start + count, :], ref[i])
            total = part if total is None else total + part
            start += count
        totals.append(total)
    half, rows = keep_ref.shape[2:4]

    def put(even_ref, odd_ref):
        for i, total in enumerate(totals):
            for j in range(half):
                start = 2 * j * rows
                even_ref[i, 0, j] = rounded(total[start : start + rows])
                odd_ref[i, 0, j] = rounded(total[start + rows : start + 2 * rows])

    @pl.when(odd_ref[0] == 0)
    def _():
        put(keep_ref, send_ref)

    @pl.when(odd_ref[0] != 0)
    def _():
        put(send_ref, keep_ref)


def weight_parts(odd, attended, others_in, grad_attn, grad_queries, backs, groups, experts):
    width = attended.shape[1]
    part = width // groups
    rows = part // experts
    left = lambda m: pl.BlockSpec((m.shape[0], part), lambda j: (0, j))
    whole = lambda m: pl.BlockSpec(m.shape, lambda j: (0,) * m.ndim)
    lefts, rights = [attended, others_in], [grad_attn, grad_queries, *backs]
    shape = (4, groups, experts // 2, rows, width)
    out = pl.BlockSpec((4, 1) + shape[2:], lambda j: (0, j, 0, 0, 0))
    return pl.pallas_call(
        weights_kernel,
        grid=(groups,),
        in_specs=[pl.BlockSpec(memory_space=pltpu.SMEM)]
        + [left(m) for m in lefts]
        + [whole(m) for m in rights],
        out_specs=[out, out],
        out_shape=[jax.ShapeDtypeStruct(shape, bf16)] * 2,
        compiler_params=params("arbitrary"),
        cost_estimate=cost(10e9, 30e6),
        name="weight_parts",
    )(odd, *lefts, *rights)


def head_stack(block):
    first = lax.broadcasted_iota(jnp.int32, block.shape, 1) < block.shape[1] // 2
    zero = jnp.zeros_like(block)
    return jnp.concatenate([jnp.where(first, block, zero), jnp.where(first, zero, block)])


def head_merge(turned):
    half, rows = turned.shape[0] // 2, turned.shape[1] // 2
    return jnp.concatenate([turned[:half, :rows], turned[half:, rows:]]).T


def chunk_scores(chunk, keys, stack, near_bias, bias_ref, prompt_len):
    scores = matmul_nt(keys, stack)
    if chunk == 0:
        bias = bias_ref[...]
        return scores + jnp.concatenate([bias, bias], axis=1)
    tri = (PROMPT_DEV, PROMPT_DEV)
    after = lax.broadcasted_iota(jnp.int32, tri, 0) > lax.broadcasted_iota(jnp.int32, tri, 1)
    diag = jnp.where(after, f32(masked_score), f32(0.0))
    last = keys.shape[0] - PROMPT_DEV
    near_end = prompt_len + CONT_DEV
    pieces = [scores[:prompt_len], scores[prompt_len:near_end] + near_bias]
    if last > near_end:
        pieces.append(scores[near_end:last])
    pieces.append(scores[last:] + jnp.concatenate([diag, diag], axis=1))
    return jnp.concatenate(pieces)


def chunk_keys(chunk, prompt_len):
    return prompt_len if chunk == 0 else prompt_len + CONT_DEV + PROMPT_DEV * chunk


def attend_kernel(prompt_len, near_ref, q_ref, k_ref, v_ref, bias_ref, out_ref, log_ref):
    scale = bf16(1.0 / math.sqrt(q_ref.shape[1] // 2))
    chunks = q_ref.shape[0] // PROMPT_DEV

    def scores_of(chunk):
        stack = head_stack(q_ref[pl.ds(chunk * PROMPT_DEV, PROMPT_DEV), :] * scale)
        keys = k_ref[: chunk_keys(chunk, prompt_len), :]
        return chunk_scores(chunk, keys, stack, near_ref[0], bias_ref, prompt_len)

    scores = scores_of(0)
    for chunk in range(chunks):
        rows = pl.ds(chunk * PROMPT_DEV, PROMPT_DEV)
        size = chunk_keys(chunk, prompt_len)
        later = scores_of(chunk + 1) if chunk + 1 < chunks else None
        top = jnp.max(scores, axis=0, keepdims=True)
        weights = jnp.exp(scores - top)
        total = jnp.sum(weights, axis=0, keepdims=True)
        mixed = matmul_tn(v_ref[:size, :], rounded(weights)) / total
        out_ref[rows, :] = rounded(head_merge(mixed))
        log_ref[0, chunk : chunk + 1, :] = top + jnp.log(total)
        scores = later


def attend_back_kernel(
    prompt_len,
    near_ref,
    q_ref,
    k_ref,
    v_ref,
    bias_ref,
    log_ref,
    out_ref,
    grad_ref,
    dq_ref,
    first_ref,
    second_ref,
    near_out_ref,
    own_ref,
    dk_ref,
    dv_ref,
):
    scale = 1.0 / math.sqrt(q_ref.shape[1] // 2)
    half = q_ref.shape[1] // 2
    dk_ref[...] = jnp.zeros_like(dk_ref)
    dv_ref[...] = jnp.zeros_like(dv_ref)
    for chunk in range(q_ref.shape[0] // PROMPT_DEV):
        rows = pl.ds(chunk * PROMPT_DEV, PROMPT_DEV)
        size = chunk_keys(chunk, prompt_len)
        stack = head_stack(q_ref[rows, :] * bf16(scale))
        grad = grad_ref[rows, :]
        grad_stack = head_stack(grad)
        product = (grad.astype(f32) * out_ref[rows, :].astype(f32)).T
        inner = jnp.concatenate(
            [
                jnp.sum(product[:half], axis=0, keepdims=True),
                jnp.sum(product[half:], axis=0, keepdims=True),
            ],
            axis=1,
        )
        keys = k_ref[:size, :]
        scores = chunk_scores(chunk, keys, stack, near_ref[0], bias_ref, prompt_len)
        weights = jnp.exp(scores - log_ref[0, chunk : chunk + 1, :])
        dv_ref[:size, :] += matmul(rounded(weights), grad_stack)
        grad_prob = matmul_nt(v_ref[:size, :], grad_stack)
        grad_score = rounded(weights * (grad_prob - inner))
        dk_ref[:size, :] += matmul(grad_score, stack)
        dq_ref[rows, :] = rounded(head_merge(matmul_tn(keys, grad_score)) * scale)
    start = 0
    for ref in (first_ref, second_ref, near_out_ref, own_ref):
        count = ref.shape[1]
        ref[0] = rounded(dk_ref[start : start + count, :])
        ref[1] = rounded(dv_ref[start : start + count, :])
        start += count


def attend(near_bias, queries, keys, values, bias):
    rows, width = queries.shape
    size = keys.shape[0]
    prompt_len = bias.shape[0]
    lanes = 2 * width // HEADS
    pairs = HEADS // 2
    chunks = rows // PROMPT_DEV
    block = lambda count: pl.BlockSpec((count, lanes), lambda j: (0, j))
    return pl.pallas_call(
        functools.partial(attend_kernel, prompt_len),
        grid=(pairs,),
        in_specs=[
            pl.BlockSpec(memory_space=pltpu.SMEM),
            block(rows),
            block(size),
            block(size),
            pl.BlockSpec((prompt_len, PROMPT_DEV), lambda j: (0, 0)),
        ],
        out_specs=[
            block(rows),
            pl.BlockSpec((1, chunks, 2 * PROMPT_DEV), lambda j: (j, 0, 0)),
        ],
        out_shape=[
            jax.ShapeDtypeStruct((rows, width), bf16),
            jax.ShapeDtypeStruct((pairs, chunks, 2 * PROMPT_DEV), f32),
        ],
        compiler_params=params("arbitrary"),
        cost_estimate=cost(16 * rows * size * width, 4 * (rows + size) * width, rows * size * HEADS),
        name="attend",
    )(near_bias, queries, keys, values, bias)


def attend_back(near_bias, queries, keys, values, bias, log_total, attended, grad):
    rows, width = queries.shape
    size = keys.shape[0]
    prompt_len = bias.shape[0]
    lanes = 2 * width // HEADS
    pairs = HEADS // 2
    chunks = rows // PROMPT_DEV
    block = lambda count: pl.BlockSpec((count, lanes), lambda j: (0, j))
    counts = (prompt_len // 2, prompt_len // 2, CONT_DEV, CONT_DEV)
    return pl.pallas_call(
        functools.partial(attend_back_kernel, prompt_len),
        grid=(pairs,),
        in_specs=[
            pl.BlockSpec(memory_space=pltpu.SMEM),
            block(rows),
            block(size),
            block(size),
            pl.BlockSpec((prompt_len, PROMPT_DEV), lambda j: (0, 0)),
            pl.BlockSpec((1, chunks, 2 * PROMPT_DEV), lambda j: (j, 0, 0)),
            block(rows),
            block(rows),
        ],
        out_specs=[block(rows)]
        + [pl.BlockSpec((2, count, lanes), lambda j: (0, 0, j)) for count in counts],
        out_shape=[jax.ShapeDtypeStruct((rows, width), bf16)]
        + [jax.ShapeDtypeStruct((2, count, width), bf16) for count in counts],
        scratch_shapes=[pltpu.VMEM((size, lanes), f32), pltpu.VMEM((size, lanes), f32)],
        compiler_params=params("arbitrary"),
        cost_estimate=cost(40 * rows * size * width, 8 * (rows + size) * width, rows * size * HEADS),
        name="attend_back",
    )(near_bias, queries, keys, values, bias, log_total, attended, grad)


def local(
    tokens_in,
    cotangent,
    hash_ids,
    norm1_gain,
    norm1_bias,
    w_query,
    w_key,
    w_value,
    w_output,
    norm2_gain,
    norm2_bias,
    expert_in,
    expert_out,
):
    row_count, width = tokens_in.shape
    experts = lax.axis_size("expert")
    groups = lax.axis_size("group")
    position = lax.axis_index("expert")
    group = lax.axis_index("group")
    capacity = 2 * row_count // experts
    slots = experts * capacity

    near_tokens = lax.ppermute(
        tokens_in[PROMPT_DEV:], "expert", [(i, i + 1) for i in range(0, experts, 2)]
    )
    prompts, prompt_ids, near_tokens = gather_relative(
        tokens_in[:PROMPT_DEV], "expert", near_tokens
    )

    row_index = jnp.arange(row_count, dtype=jnp.int32)
    routed = rounded(hash_ids == jnp.arange(experts, dtype=jnp.int32)[None, :])
    lower = rounded(row_index[:, None] >= row_index[None, :])
    running = matmul(lower, routed)
    rank = (jnp.sum(running * routed.astype(f32), axis=-1) - 1.0).astype(jnp.int32)
    slot = hash_ids[:, 0] * capacity + rank
    spread = rounded(slot[None, :] == jnp.arange(slots, dtype=jnp.int32)[:, None])

    def exchanged(values):
        got = lax.all_to_all(
            values.reshape(experts, capacity, width), "expert", split_axis=0, concat_axis=0, tiled=True
        )
        return got.reshape(slots, width)

    def to_experts(values):
        return exchanged(matmul(spread, values, bf16))

    inputs_f = tokens_in.astype(f32)
    others_in, queries, keys, values = project(
        prompts + [near_tokens, tokens_in[PROMPT_DEV:]],
        norm1_gain,
        norm1_bias,
        w_query,
        w_key,
        w_value,
    )

    block_pos = jnp.stack([(position ^ r) * PROMPT_DEV for r in prompt_ids])
    prompt_pos = jnp.arange(PROMPT_DEV, dtype=jnp.int32)
    key_pos = (block_pos[:, None] + prompt_pos[None, :]).reshape(-1)
    query_pos = position * PROMPT_DEV + row_index[:PROMPT_DEV]
    bias = jnp.where(key_pos[:, None] <= query_pos[None, :], f32(0.0), f32(masked_score))
    near_bias = jnp.where(position % 2 == 1, f32(0.0), f32(masked_score))[None]
    cot_sent, _ = lax.optimization_barrier((matmul(spread, cotangent, bf16), prompts))
    cot_rows = exchanged(cot_sent)
    cot_rows, keys, values = lax.optimization_barrier((cot_rows, keys, values))
    cot_par = swapped(cot_rows, "group", 1)
    attended, log_total = attend(near_bias, queries, keys, values, bias)

    residual = inputs_f + matmul(attended, w_output)
    normed_b, normed2, inverse2 = normalize(residual, norm2_gain, norm2_bias)
    ffn_in = rounded(normed_b)
    cot_late, ffn_in = lax.optimization_barrier((cot_rows, ffn_in))
    rows = to_experts(ffn_in)
    grad_hidden = expert_back(cot_late, expert_out)
    rows, grad_hidden, cot_par = lax.optimization_barrier((rows, grad_hidden, cot_par))
    rows_par = swapped(rows, "group", 1)
    hidden, grad_pre, grad_rows = expert_front(rows, grad_hidden, expert_in)
    grad_got = exchanged(grad_rows)
    produced = expert_produce(hidden, expert_out)
    rows_par, produced = lax.optimization_barrier((rows_par, produced))

    def to_group(piece, step):
        return lax.ppermute(piece, "group", [(i, (i + step) % groups) for i in range(groups)])

    steps = list(range(2, groups, 2))
    places = {step: ((group + step) % groups)[None] for step in [0] + steps}
    out_pieces = {
        step: out_slice(places[step], hidden, cot_rows, rows_par, expert_in, cot_par, groups, bf16)
        for step in steps
    }
    grad_got, out_pieces = lax.optimization_barrier((grad_got, out_pieces))
    sums_out = [to_group(out_pieces[step], step) for step in steps]
    grad_ffn = matmul_tn(spread, grad_got)
    produced, _ = lax.optimization_barrier((produced, grad_got))
    result_got = exchanged(produced)

    grad_gain2 = jnp.sum(grad_ffn * normed2, axis=0)
    grad_bias2 = jnp.sum(grad_ffn, axis=0)
    grad_resid = cotangent.astype(f32) + norm_back(grad_ffn, norm2_gain, normed2, inverse2)
    grad_attn = rounded(grad_resid)
    grad_attended = matmul_nt(grad_attn, w_output, bf16)
    grad_queries, back_first, back_second, back_near, back_own = attend_back(
        near_bias, queries, keys, values, bias, log_total, attended, grad_attended
    )
    rows_late, back_own, result_got = lax.optimization_barrier((rows_par, back_own, result_got))
    result = rounded(residual + matmul_tn(spread, result_got))
    pre_par = expert_partner(rows_late, cot_par, expert_in, expert_out)
    in_pieces = {
        step: in_slice(places[step], rows, grad_pre, rows_par, pre_par, groups, bf16, link_pieces)
        for step in steps
    }
    in_pieces, sums_out = lax.optimization_barrier((in_pieces, sums_out))
    waiting = [(step, piece) for step in steps for piece in in_pieces[step]]
    came = []

    def link_step(values):
        if not waiting:
            return values
        step, piece = waiting.pop(0)
        piece, _ = lax.optimization_barrier((piece, came[-1:]))
        values, got = lax.optimization_barrier((values, to_group(piece, step)))
        came.append(got)
        return values

    near_back = lax.ppermute(
        back_near, "expert", [(i + 1, i) for i in range(0, experts, 2)]
    )
    prompt_back = scatter_relative(back_first, back_second, "expert")
    queries_late, _ = lax.optimization_barrier((grad_queries, in_pieces))
    keep, send = weight_parts(
        (position & 1)[None],
        attended,
        others_in,
        grad_attn,
        queries_late,
        (back_first, back_second, back_near, back_own),
        groups,
        experts,
    )
    which, _ = lax.optimization_barrier((places[0], keep))
    own_out = out_slice(
        which, hidden, cot_rows, rows_par, expert_in, cot_par, groups, f32, sums_out
    )
    own_in = in_slice(which, rows, grad_pre, rows_par, pre_par, groups, f32)[0]
    keep, send, own_out, own_in = link_step((keep, send, own_out, own_in))
    keep_w, send_w = expert_sums(keep, send, link_step)
    while waiting:
        link_step(())
    sums_in = [came[i * link_pieces : (i + 1) * link_pieces] for i in range(len(steps))]
    own_back = rounded(back_own.astype(f32) + near_back.astype(f32))
    grad_keys, grad_values = jnp.concatenate([prompt_back, own_back], axis=1)
    grad_attn_in = (
        matmul_nt(grad_queries, w_query)
        + matmul_nt(grad_keys, w_key)
        + matmul_nt(grad_values, w_value)
    )
    _, normed1, inverse1 = normalize(inputs_f, norm1_gain, norm1_bias)
    grad_gain1 = jnp.sum(grad_attn_in * normed1, axis=0)
    grad_bias1 = jnp.sum(grad_attn_in, axis=0)
    grad_tokens = rounded(grad_resid + norm_back(grad_attn_in, norm1_gain, normed1, inverse1))
    keep_w, send_w, vectors, sums_in, own_out, own_in = lax.optimization_barrier(
        (
            keep_w,
            send_w,
            [grad_gain1, grad_bias1, grad_gain2, grad_bias2],
            sums_in,
            own_out,
            own_in,
        )
    )
    grad_w_output, grad_w_query, grad_w_key, grad_w_value = group_sums(keep_w, send_w)
    sums = vector_sums(vectors)
    grad_expert_out = own_out[None]
    grad_expert_in = sum_pieces(own_in, sums_in)
    return (
        result,
        grad_tokens,
        sums[0],
        sums[1],
        grad_w_query,
        grad_w_key,
        grad_w_value,
        grad_w_output,
        sums[2],
        sums[3],
        grad_expert_in,
        grad_expert_out,
    )


def solution(mesh):
    both = ("group", "expert")
    return jax.shard_map(
        local,
        mesh=mesh,
        in_specs=(
            P(both, None),
            P(both, None),
            P(both, None),
            P(),
            P(),
            P(),
            P(),
            P(),
            P(),
            P(),
            P(),
            P("expert", None, None),
            P("expert", None, None),
        ),
        out_specs=(
            P(both, None),
            P(both, None),
            P(both),
            P(both),
            P(both, None),
            P(both, None),
            P(both, None),
            P(both, None),
            P(both),
            P(both),
            P("expert", "group", None),
            P("expert", "group", None),
        ),
        check_vma=False,
    )
```

```python
import functools
import math

import jax
import jax.numpy as jnp
from jax import lax
from jax.experimental import pallas as pl
from jax.experimental.pallas import tpu as pltpu
from jax.sharding import PartitionSpec as P

HEADS = 16
PROMPT_DEV = 128
CONT_DEV = 384


norm_eps = 1e-05
masked_score = -1e30
bf16 = jnp.bfloat16
f32 = jnp.float32
MIB = 1 << 20
share = 0.05


def swapped(block, axis, mask):
    return lax.ppermute(block, axis, [(i, i ^ mask) for i in range(lax.axis_size(axis))])


def rounded(values):
    return values.astype(bf16)


def normalize(values, gain, shift):
    average = jnp.mean(values, axis=-1, keepdims=True)
    centered = values - average
    variance = jnp.mean(centered * centered, axis=-1, keepdims=True)
    inverse = lax.rsqrt(variance + norm_eps)
    normed = centered * inverse
    return (normed * gain + shift, normed, inverse)


def norm_back(grad_out, gain, normed, inverse):
    scaled = grad_out * gain
    first_mean = jnp.mean(scaled, axis=-1, keepdims=True)
    second = jnp.mean(scaled * normed, axis=-1, keepdims=True)
    return inverse * (scaled - first_mean - normed * second)


def matmul(a, b, kind=f32):
    return jnp.dot(a, b, preferred_element_type=f32).astype(kind)


def matmul_nt(a, b, kind=f32):
    return lax.dot_general(a, b, (((1,), (1,)), ((), ())), preferred_element_type=f32).astype(kind)


def matmul_tn(a, b, kind=f32):
    return lax.dot_general(a, b, (((0,), (0,)), ((), ())), preferred_element_type=f32).astype(kind)


def outer_bits(size):
    return range(size.bit_length() - 2, 0, -1)


def gather_relative(block, axis, more):
    size = lax.axis_size(axis)
    pieces = {0: block}
    ready, last = [0], []
    while ready:
        fresh = {}
        for r in ready:
            for bit in outer_bits(size):
                if r ^ (1 << bit) not in pieces and r ^ (1 << bit) not in fresh:
                    fresh[r ^ (1 << bit)] = swapped(pieces[r], axis, 1 << bit)
        fresh, more = lax.optimization_barrier((fresh, more))
        pieces.update(fresh)
        ready, last = list(fresh), list(fresh.values()) or last
    near = sorted(pieces)
    for r in near:
        pieces[r ^ 1] = swapped(pieces[r], axis, 1)
    order = near + [r ^ 1 for r in near]
    return [pieces[r] for r in order], order, more, last


def scatter_relative(near, far, axis):
    size = lax.axis_size(axis)
    got = yield swapped(far, axis, 1)
    both = added(near, got)
    count = size // 2
    rows = both.shape[1] // count
    pieces = {2 * i: rounded(both[:, i * rows : (i + 1) * rows]) for i in range(count)}
    bits = list(outer_bits(size))
    for level in range(len(bits), 0, -1):
        sent, spans = [], []
        for r in [r for r in sorted(pieces) if bin(r).count("1") == level]:
            ways = [bit for bit in bits if r >> bit & 1]
            if rows % (16 * len(ways)):
                ways = ways[:1]
            part = rows // len(ways)
            piece = pieces.pop(r)
            for i, bit in enumerate(ways):
                span = (i * part, (i + 1) * part)
                sent.append(swapped(piece[:, span[0] : span[1]], axis, 1 << bit))
                spans.append((r ^ (1 << bit), span))
        gots = yield sent
        for r in sorted(pieces):
            total = pieces[r].astype(f32)
            for got, (target, span) in zip(gots, spans):
                if target == r:
                    outside = ((0, 0), (span[0], rows - span[1]), (0, 0))
                    total = total + jnp.pad(got.astype(f32), outside)
            pieces[r] = rounded(total)
    return pieces[0]


def halved(blocks, place, axis, bit):
    own = (lax.axis_index(axis) >> bit) & 1
    return (
        lax.dynamic_index_in_dim(blocks, own, place, keepdims=False),
        lax.dynamic_index_in_dim(blocks, 1 - own, place, keepdims=False),
    )


def added(keep, got):
    return keep.astype(f32) + got.astype(f32)


def places_of(bits, bit, value):
    rest = [other for other in bits if other != bit]
    weight = {other: 1 << (len(bits) - 1 - i) for i, other in enumerate(bits)}
    places = []
    for number in range(1 << len(rest)):
        place = value * weight[bit]
        for i, other in enumerate(rest):
            place = place + (number >> (len(rest) - 1 - i) & 1) * weight[other]
        places.append(place)
    return places


def halve_kernel(lefts, bits, own_ref, *refs):
    sets = len(lefts)
    for k, (left, bit) in enumerate(zip(lefts, bits)):
        keep_ref, got_ref = refs[2 * k : 2 * k + 2]
        outs = refs[2 * sets + 2 * k : 2 * sets + 2 * k + 2]
        own = (own_ref[0] >> bit) & 1
        for ref, value in zip(outs, (own, 1 - own)):
            for i, place in enumerate(places_of(left, bit, value)):
                for j in range(ref.shape[1]):
                    ref[0, j, i] = rounded(added(keep_ref[0, j, place], got_ref[0, j, place]))


def halve(number, states, bits):
    _, groups, count, rows, width = states[0][0].shape
    shape = (2, groups, count // 2, rows, width)
    came = lambda first: pl.BlockSpec(
        (1, groups, count, rows, width), lambda i: (first + i if first else i, 0, 0, 0, 0)
    )
    out = pl.BlockSpec((1, groups, count // 2, rows, width), lambda i: (i, 0, 0, 0, 0))
    size = 2 * math.prod(shape)
    outs = pl.pallas_call(
        functools.partial(halve_kernel, [state[3] for state in states], bits),
        grid=(2,),
        in_specs=[pl.BlockSpec(memory_space=pltpu.SMEM)]
        + [came(state[2]) for state in states for _ in range(2)],
        out_specs=[out] * (2 * len(states)),
        out_shape=[jax.ShapeDtypeStruct(shape, bf16)] * (2 * len(states)),
        compiler_params=params("arbitrary"),
        cost_estimate=cost(2 * size, 12 * size),
        name="halve",
    )(number, *[value for state in states for value in state[:2]])
    return list(zip(outs[::2], outs[1::2]))


def turn_kernel(own_ref, *refs):
    (*sets, own_out_ref, send_ref) = refs
    own = own_ref[0] & 1
    start = 0
    for keep_ref, got_ref in zip(sets[::2], sets[1::2]):
        for i in range(keep_ref.shape[0]):
            for j in range(keep_ref.shape[1] // 2):
                for ref, value in ((own_out_ref, own), (send_ref, 1 - own)):
                    place = 2 * j + value
                    ref[start + i, j] = rounded(added(keep_ref[i, place, 0], got_ref[i, place, 0]))
        start += keep_ref.shape[0]


def turn(number, sets):
    _, groups, _, rows, width = sets[0].shape
    shape = (4, groups // 2, rows, width)
    return pl.pallas_call(
        turn_kernel,
        in_specs=[pl.BlockSpec(memory_space=pltpu.SMEM)]
        + [pl.BlockSpec(memory_space=pltpu.VMEM)] * len(sets),
        out_specs=[pl.BlockSpec(memory_space=pltpu.VMEM)] * 2,
        out_shape=[jax.ShapeDtypeStruct(shape, bf16)] * 2,
        compiler_params=params(),
        cost_estimate=cost(8 * sets[0].size, 8 * sets[0].size),
        name="turn",
    )(number, *sets)


def weight_chain(keep, send):
    bits = list(range(1, lax.axis_size("expert").bit_length() - 1))
    number = lax.axis_index("expert")[None]
    got = yield swapped(send, "expert", 1)
    states = [(keep, got, 0, bits[::-1]), (keep, got, 2, bits[::-1])]
    for pair in zip(bits, bits[::-1]):
        halves = halve(number, states, pair)
        gots = yield [swapped(send, "expert", 1 << bit) for bit, (_, send) in zip(pair, halves)]
        states = [
            (keep, got, 0, [other for other in state[3] if other != bit])
            for state, bit, (keep, _), got in zip(states, pair, halves, gots)
        ]
    keep, send = turn(
        lax.axis_index("group")[None], [value for state in states for value in state[:2]]
    )
    got = yield swapped(send, "group", 1)
    both = added(keep, got)
    bits = list(range(1, lax.axis_size("group").bit_length() - 1))
    both = both.reshape((4,) + (2,) * len(bits) + both.shape[-2:])
    left = bits[::-1]
    for bit in bits:
        keep, send = halved(rounded(both), 1 + left.index(bit), "group", bit)
        left.remove(bit)
        got = yield swapped(send, "group", 1 << bit)
        both = added(keep, got)
    return [both[i] for i in range(both.shape[0])]


def moved_on(chain, came):
    try:
        return chain.send(came), None
    except StopIteration as stop:
        return None, stop.value


def vector_sums(vectors):
    axes = ("group", "expert")
    devices = lax.axis_size("group") * lax.axis_size("expert")
    count, width = vectors.shape
    pieces = vectors.reshape(count, devices, width // devices).swapaxes(0, 1)
    got = lax.all_to_all(pieces, axes, split_axis=0, concat_axis=0, tiled=True)
    return jnp.sum(got, axis=0)


def params(*semantics):
    return pltpu.CompilerParams(dimension_semantics=semantics, vmem_limit_bytes=60 * MIB)


def cost(flops, total_bytes, exps=0):
    return pl.CostEstimate(
        flops=int(flops * share), bytes_accessed=int(total_bytes * share), transcendentals=int(exps * share)
    )


def logistic(values):
    return 0.5 * jnp.tanh(0.5 * values) + 0.5


def back_kernel(cot_ref, wout_ref, out_ref):
    out_ref[...] = matmul_nt(cot_ref[...], wout_ref[0], bf16)


def expert_back(cot, expert_out):
    count, width = cot.shape
    ff = expert_out.shape[1]
    block = 1024
    return pl.pallas_call(
        back_kernel,
        grid=(ff // block,),
        in_specs=[
            pl.BlockSpec((count, width), lambda j: (0, 0)),
            pl.BlockSpec((1, block, width), lambda j: (0, j, 0)),
        ],
        out_specs=pl.BlockSpec((count, block), lambda j: (0, j)),
        out_shape=jax.ShapeDtypeStruct((count, ff), bf16),
        compiler_params=params("arbitrary"),
        cost_estimate=cost(2 * count * width * ff, 2 * count * ff + 2 * width * ff),
        name="expert_back",
    )(cot, expert_out)


def front_kernel(parts, rows_ref, gh_ref, win_ref, hidden_ref, pre_ref, out_ref, acc_ref):
    step = pl.program_id(0)
    count = rows_ref.shape[0] // parts

    @pl.when(step == 0)
    def _():
        acc_ref[...] = jnp.zeros_like(acc_ref)

    first = lambda i: matmul(rows_ref[i * count : (i + 1) * count, :], win_ref[0])
    pre = first(0)
    for i in range(parts):
        later = first(i + 1) if i + 1 < parts else None
        here = pl.ds(i * count, count)
        sig = logistic(pre)
        hidden = pre * sig
        hidden_ref[here, :] = rounded(hidden)
        grad_pre = rounded(gh_ref[here, :].astype(f32) * sig * (1.0 + pre - hidden))
        pre_ref[here, :] = grad_pre
        acc_ref[here, :] += matmul_nt(grad_pre, win_ref[0])
        pre = later

    @pl.when(step == pl.num_programs(0) - 1)
    def _():
        out_ref[...] = rounded(acc_ref[...])


def expert_front(rows, grad_hidden, expert_in):
    count, width = rows.shape
    ff = expert_in.shape[2]
    block = 1024
    whole = pl.BlockSpec((count, width), lambda j: (0, 0))
    part = pl.BlockSpec((count, block), lambda j: (0, j))
    return pl.pallas_call(
        functools.partial(front_kernel, 4),
        grid=(ff // block,),
        in_specs=[whole, part, pl.BlockSpec((1, width, block), lambda j: (0, 0, j))],
        out_specs=[part, part, whole],
        out_shape=[
            jax.ShapeDtypeStruct((count, ff), bf16),
            jax.ShapeDtypeStruct((count, ff), bf16),
            jax.ShapeDtypeStruct((count, width), bf16),
        ],
        scratch_shapes=[pltpu.VMEM((count, width), f32)],
        compiler_params=params("arbitrary"),
        cost_estimate=cost(4 * count * width * ff, 6 * count * ff + 2 * width * ff, count * ff),
        name="expert_front",
    )(rows, grad_hidden, expert_in)


def produce_kernel(hidden_ref, wout_ref, out_ref, acc_ref):
    step = pl.program_id(0)
    part = matmul(hidden_ref[...], wout_ref[0])

    @pl.when(step == 0)
    def _():
        acc_ref[...] = part

    @pl.when(step > 0)
    def _():
        acc_ref[...] += part

    @pl.when(step == pl.num_programs(0) - 1)
    def _():
        out_ref[...] = rounded(acc_ref[...])


def expert_produce(hidden, expert_out):
    count, ff = hidden.shape
    width = expert_out.shape[2]
    block = 1024
    return pl.pallas_call(
        produce_kernel,
        grid=(ff // block,),
        in_specs=[
            pl.BlockSpec((count, block), lambda j: (0, j)),
            pl.BlockSpec((1, block, width), lambda j: (0, j, 0)),
        ],
        out_specs=pl.BlockSpec((count, width), lambda j: (0, 0)),
        out_shape=jax.ShapeDtypeStruct((count, width), bf16),
        scratch_shapes=[pltpu.VMEM((count, width), f32)],
        compiler_params=params("arbitrary"),
        cost_estimate=cost(2 * count * width * ff, 2 * count * ff + 2 * width * ff),
        name="expert_produce",
    )(hidden, expert_out)


def own_kernel(_, hidden_ref, pre_ref, rows_ref, cot_ref, out_ref, in_ref):
    out_ref[...] = matmul_tn(hidden_ref[...], cot_ref[...])
    in_ref[...] = matmul_tn(rows_ref[...], pre_ref[...])


def own_sums(place, groups, hidden, grad_pre, rows, cot):
    count, ff = hidden.shape
    width = rows.shape[1]
    part = ff // groups
    block = part // 2
    whole = pl.BlockSpec((count, width), lambda j, w: (0, 0))
    columns = pl.BlockSpec((count, block), lambda j, w: (0, 2 * w[0] + j))
    return pl.pallas_call(
        own_kernel,
        grid_spec=pltpu.PrefetchScalarGridSpec(
            num_scalar_prefetch=1,
            grid=(2,),
            in_specs=[columns, columns, whole, whole],
            out_specs=[
                pl.BlockSpec((block, width), lambda j, w: (j, 0)),
                pl.BlockSpec((width, block), lambda j, w: (0, j)),
            ],
        ),
        out_shape=[
            jax.ShapeDtypeStruct((part, width), f32),
            jax.ShapeDtypeStruct((width, part), f32),
        ],
        compiler_params=params("arbitrary"),
        cost_estimate=cost(4 * count * width * part, 16e6),
        name="own_sums",
    )(place, hidden, grad_pre, rows, cot)


def shard_kernel(
    _, win_ref, wout_ref, out_acc_ref, in_acc_ref, near_rows_ref, near_ref, rows_ref, far_ref, *refs
):
    out_ref, in_ref, out_sum, in_sum = refs[-4:]
    step = pl.program_id(0)

    def shard(rows, cot):
        pre = matmul(rows, win_ref[0])
        grad_hidden = matmul_nt(cot, wout_ref[0])
        sig = logistic(pre)
        hidden = pre * sig
        out = matmul_tn(rounded(hidden), cot)
        grad_pre = rounded(grad_hidden * sig * (1.0 + pre - hidden))
        return out, matmul_tn(rows, grad_pre)

    @pl.when(step == 0)
    def _():
        rows = near_rows_ref[0]
        out, inner = shard(rows, near_ref[...].reshape(rows.shape))
        out_sum[...] = out_acc_ref[...] + out
        in_sum[...] = in_acc_ref[...] + inner

    rows = rows_ref[0]
    out, inner = shard(rows, far_ref[...].reshape(rows.shape))
    out_sum[...] += out
    in_sum[...] += inner

    @pl.when(step == pl.num_programs(0) - 1)
    def _():
        out_ref[0] = out_sum[...]
        in_ref[...] = rounded(in_sum[...]).reshape(in_ref.shape)


def shard_sums(number, half, groups, expert_in, expert_out, acc, rows, cot, earlier=None):
    _, count, width = rows.shape
    sources, _, slots, _ = cot[0].shape
    part = expert_in.shape[2] // groups
    block = part // 2
    specs = [
        pl.BlockSpec((1, width, block), lambda j, w: (0, 0, 2 * w[0] + half)),
        pl.BlockSpec((1, block, width), lambda j, w: (0, 2 * w[0] + half, 0)),
        pl.BlockSpec((block, width), lambda j, w: (half, 0)),
        pl.BlockSpec((width, block), lambda j, w: (0, half)),
        pl.BlockSpec((1, count, width), lambda j, w: (w[1], 0, 0)),
        pl.BlockSpec((sources, 1, slots, width), lambda j, w: (0, 0, 0, 0)),
        pl.BlockSpec((1, count, width), lambda j, w: (w[2 + j], 0, 0)),
        pl.BlockSpec((sources, 1, slots, width), lambda j, w: (0, 1 + j, 0, 0)),
    ]
    values = [expert_in, expert_out, *acc, rows, cot[0], rows, cot[1]]
    aliases = {}
    if earlier is not None:
        specs.append(pl.BlockSpec(memory_space=pl.ANY))
        values.append(earlier)
        aliases = {len(values): 0}
    return pl.pallas_call(
        shard_kernel,
        grid_spec=pltpu.PrefetchScalarGridSpec(
            num_scalar_prefetch=1,
            grid=(groups - 2,),
            in_specs=specs,
            out_specs=[
                pl.BlockSpec((1, block, width), lambda j, w: (0, half, 0)),
                pl.BlockSpec((groups, width // groups, block), lambda j, w: (0, 0, 0)),
            ],
            scratch_shapes=[
                pltpu.VMEM((block, width), f32),
                pltpu.VMEM((width, block), f32),
            ],
        ),
        out_shape=[
            jax.ShapeDtypeStruct((1, part, width), f32),
            jax.ShapeDtypeStruct((groups, width // groups, block), bf16),
        ],
        input_output_aliases=aliases,
        compiler_params=params("arbitrary"),
        cost_estimate=cost(8 * count * width * block * groups, 16e6, count * block * groups),
        name="shard_sums",
    )(number, *values)


def lay_kernel(*refs):
    gots, out_ref = refs[:-1], refs[-1]
    block = gots[0].shape[2]
    for i in range(gots[0].shape[0]):
        for j, ref in enumerate(gots):
            start = (i * len(gots) + j) * block
            out_ref[0, :, start : start + block] = ref[i].astype(f32)


def lay_out(gots):
    groups, rows, block = gots[0].shape
    tall = 64
    width = groups * block * len(gots)
    return pl.pallas_call(
        lay_kernel,
        grid=(rows // tall,),
        in_specs=[pl.BlockSpec((groups, tall, block), lambda j: (0, j, 0))] * len(gots),
        out_specs=pl.BlockSpec((1, tall, width), lambda j: (0, j, 0)),
        out_shape=jax.ShapeDtypeStruct((1, rows, width), f32),
        compiler_params=params("arbitrary"),
        cost_estimate=cost(rows * width, 6 * rows * width),
        name="lay_out",
    )(*gots)


def spread_kernel(first, _, ids_ref, values_ref, *refs):
    out_ref = refs[-1]
    experts, _, capacity, width = out_ref.shape

    def spread():
        rows = ids_ref.shape[2]
        ids = ids_ref[0]
        number = lax.broadcasted_iota(jnp.int32, (experts, rows), 0)
        routed = jnp.where(number == ids, f32(1.0), f32(0.0))
        square = (rows, rows)
        before = lax.broadcasted_iota(jnp.int32, square, 0) <= lax.broadcasted_iota(
            jnp.int32, square, 1
        )
        running = matmul(rounded(routed), rounded(jnp.where(before, f32(1.0), f32(0.0))))
        rank = jnp.sum(running * routed, axis=0, keepdims=True).astype(jnp.int32) - 1
        slot = ids * capacity + rank
        places = lax.broadcasted_iota(jnp.int32, (experts * capacity, rows), 0)
        onehot = rounded(jnp.where(places == slot, f32(1.0), f32(0.0)))
        out = matmul(onehot, values_ref[0, :, :width], bf16)
        out_ref[...] = out.reshape(out_ref.shape)

    if first:
        step = pl.program_id(0)

        @pl.when(step == 0)
        def _():
            out_ref[...] = refs[0][...].reshape(out_ref.shape)

        pl.when(step > 0)(spread)
    else:
        spread()


def spread_rows(numbers, ids, values, experts, first=None):
    _, rows, columns = values.shape
    width = columns - 128
    capacity = 2 * rows // experts
    start = 0 if first is None else 1
    count = numbers.shape[0] + start
    which = lambda j, w: w[jnp.maximum(j - start, 0)]
    specs = [
        pl.BlockSpec((1, 1, rows), lambda j, w: (which(j, w), 0, 0)),
        pl.BlockSpec((1, rows, columns), lambda j, w: (which(j, w), 0, 0)),
    ]
    operands = [ids, values]
    if start:
        specs.append(pl.BlockSpec(first.shape, lambda j, w: (0, 0)))
        operands.append(first)
    return pl.pallas_call(
        functools.partial(spread_kernel, start),
        grid_spec=pltpu.PrefetchScalarGridSpec(
            num_scalar_prefetch=1,
            grid=(count,),
            in_specs=specs,
            out_specs=pl.BlockSpec((experts, 1, capacity, width), lambda j, w: (0, j, 0, 0)),
        ),
        out_shape=jax.ShapeDtypeStruct((experts, count, capacity, width), bf16),
        compiler_params=params("arbitrary"),
        cost_estimate=cost(2 * count * experts * capacity * rows * width, 8e6),
        name="spread_rows",
    )(numbers, *operands)


def project_kernel(count, gain_ref, bias_ref, wq_ref, wk_ref, wv_ref, *refs):
    pieces, (in_ref, q_ref, k_ref, v_ref, scratch) = refs[:count], refs[count:]

    @pl.when(pl.program_id(0) == 0)
    def _():
        start = 0
        for ref in pieces:
            end = start + ref.shape[0]
            values = normalize(ref[...].astype(f32), gain_ref[...], bias_ref[...])[0]
            scratch[start:end, :] = rounded(values)
            start = end
        in_ref[...] = scratch[...]

    first, last = pieces[0].shape[0], pieces[-1].shape[0]
    size = scratch.shape[0]
    q_ref[:first, :] = matmul(scratch[:first, :], wq_ref[...], bf16)
    q_ref[first:, :] = matmul(scratch[size - last :, :], wq_ref[...], bf16)
    k_ref[...] = matmul(scratch[...], wk_ref[...], bf16)
    v_ref[...] = matmul(scratch[...], wv_ref[...], bf16)


def project(pieces, gain, shift, w_query, w_key, w_value):
    width = gain.shape[0]
    size = sum(p.shape[0] for p in pieces)
    own = pieces[0].shape[0] + pieces[-1].shape[0]
    block = 512
    whole = lambda rows: pl.BlockSpec((rows, width), lambda j: (0, 0))
    weights = pl.BlockSpec((width, block), lambda j: (0, j))
    columns = lambda rows: pl.BlockSpec((rows, block), lambda j: (0, j))
    return pl.pallas_call(
        functools.partial(project_kernel, len(pieces)),
        grid=(width // block,),
        in_specs=[whole(1), whole(1)] + [weights] * 3 + [whole(p.shape[0]) for p in pieces],
        out_specs=[whole(size), columns(own), columns(size), columns(size)],
        out_shape=[jax.ShapeDtypeStruct((rows, width), bf16) for rows in (size, own, size, size)],
        scratch_shapes=[pltpu.VMEM((size, width), bf16)],
        compiler_params=params("arbitrary"),
        cost_estimate=cost(4 * size * width * width, 8 * size * width + 4 * width * width),
        name="project",
    )(gain[None], shift[None], w_query, w_key, w_value, *pieces)


def weights_kernel(odd_ref, *refs):
    attended_ref, others_ref, grad_ref, dq_ref, *backs = refs[:-2]
    keep_ref, send_ref = refs[-2:]
    size = others_ref.shape[0]
    totals = [
        matmul_tn(attended_ref[...], grad_ref[...]),
        matmul_tn(others_ref[:PROMPT_DEV, :], dq_ref[:PROMPT_DEV, :])
        + matmul_tn(others_ref[size - CONT_DEV :, :], dq_ref[PROMPT_DEV:, :]),
    ]
    for i in range(2):
        total, start = None, 0
        for ref in backs:
            count = ref.shape[1]
            part = matmul_tn(others_ref[start : start + count, :], ref[i])
            total = part if total is None else total + part
            start += count
        totals.append(total)
    half, rows = keep_ref.shape[2:4]

    def put(even_ref, odd_ref):
        for i, total in enumerate(totals):
            for j in range(half):
                start = 2 * j * rows
                even_ref[i, 0, j] = rounded(total[start : start + rows])
                odd_ref[i, 0, j] = rounded(total[start + rows : start + 2 * rows])

    @pl.when(odd_ref[0] == 0)
    def _():
        put(keep_ref, send_ref)

    @pl.when(odd_ref[0] != 0)
    def _():
        put(send_ref, keep_ref)


def weight_parts(odd, attended, others_in, grad_attn, grad_queries, backs, groups, experts):
    width = attended.shape[1]
    part = width // groups
    rows = part // experts
    left = lambda m: pl.BlockSpec((m.shape[0], part), lambda j: (0, j))
    whole = lambda m: pl.BlockSpec(m.shape, lambda j: (0,) * m.ndim)
    lefts, rights = [attended, others_in], [grad_attn, grad_queries, *backs]
    shape = (4, groups, experts // 2, rows, width)
    out = pl.BlockSpec((4, 1) + shape[2:], lambda j: (0, j, 0, 0, 0))
    return pl.pallas_call(
        weights_kernel,
        grid=(groups,),
        in_specs=[pl.BlockSpec(memory_space=pltpu.SMEM)]
        + [left(m) for m in lefts]
        + [whole(m) for m in rights],
        out_specs=[out, out],
        out_shape=[jax.ShapeDtypeStruct(shape, bf16)] * 2,
        compiler_params=params("arbitrary"),
        cost_estimate=cost(10e9, 30e6),
        name="weight_parts",
    )(odd, *lefts, *rights)


def resid_back_kernel(
    got_ref, spread_ref, resid_ref, gain_ref, cot_ref, wo_ref, grad_ref, attn_ref, attended_ref, sums_ref
):
    grad = matmul_tn(spread_ref[...], got_ref[...])
    _, normed, inverse = normalize(resid_ref[...], 1.0, 0.0)
    sums = jnp.concatenate(
        [jnp.sum(grad * normed, axis=0, keepdims=True), jnp.sum(grad, axis=0, keepdims=True)]
    )

    @pl.when(pl.program_id(0) == 0)
    def _():
        sums_ref[...] = sums

    @pl.when(pl.program_id(0) > 0)
    def _():
        sums_ref[...] += sums

    total = cot_ref[...].astype(f32) + norm_back(grad, gain_ref[...], normed, inverse)
    grad_ref[...] = total
    attn_ref[...] = rounded(total)
    attended_ref[...] = matmul_nt(rounded(total), wo_ref[...], bf16)


def resid_back(got, spread, residual, gain, cotangent, w_output):
    rows, width = residual.shape
    slots = got.shape[0]
    block = 256
    whole = lambda count: pl.BlockSpec((count, width), lambda j: (0, 0))
    part = pl.BlockSpec((block, width), lambda j: (j, 0))
    return pl.pallas_call(
        resid_back_kernel,
        grid=(rows // block,),
        in_specs=[
            whole(slots),
            pl.BlockSpec((slots, block), lambda j: (0, j)),
            part,
            whole(1),
            part,
            whole(width),
        ],
        out_specs=[part, part, part, whole(2)],
        out_shape=[
            jax.ShapeDtypeStruct((rows, width), f32),
            jax.ShapeDtypeStruct((rows, width), bf16),
            jax.ShapeDtypeStruct((rows, width), bf16),
            jax.ShapeDtypeStruct((2, width), f32),
        ],
        compiler_params=params("arbitrary"),
        cost_estimate=cost(2 * rows * width * (slots + width), 16 * rows * width),
        name="resid_back",
    )(got, spread, residual, gain[None], cotangent, w_output)


def input_back_kernel(
    prompt_ref, own_ref, near_ref, dq_ref, wq_ref, wk_ref, wv_ref, x_ref, gain_ref, resid_ref,
    out_ref, sums_ref, dk_ref, dv_ref,
):
    step = pl.program_id(0)
    block = dk_ref.shape[0]
    count = prompt_ref.shape[1]

    def put(first):
        for i, ref in enumerate((dk_ref, dv_ref)):
            start, size = (0, block - count) if first else (block - count, block)
            if first:
                ref[:count, :] = prompt_ref[i]
            here = pl.ds(start, size)
            ref[block - size :, :] = rounded(added(own_ref[i, here, :], near_ref[i, here, :]))

    pl.when(step == 0)(lambda: put(True))
    pl.when(step > 0)(lambda: put(False))
    grad = matmul_nt(dq_ref[...], wq_ref[...])
    grad = grad + matmul_nt(dk_ref[...], wk_ref[...])
    grad = grad + matmul_nt(dv_ref[...], wv_ref[...])
    _, normed, inverse = normalize(x_ref[...].astype(f32), 1.0, 0.0)
    sums = jnp.concatenate(
        [jnp.sum(grad * normed, axis=0, keepdims=True), jnp.sum(grad, axis=0, keepdims=True)]
    )

    @pl.when(step == 0)
    def _():
        sums_ref[...] = sums

    @pl.when(step > 0)
    def _():
        sums_ref[...] += sums

    out_ref[...] = rounded(resid_ref[...] + norm_back(grad, gain_ref[...], normed, inverse))


def input_back(prompt, own, near, grad_queries, w_query, w_key, w_value, tokens, gain, grad_resid):
    rows, width = tokens.shape
    block = rows // 2
    whole = lambda count: pl.BlockSpec((count, width), lambda j: (0, 0))
    part = pl.BlockSpec((block, width), lambda j: (j, 0))
    pair = lambda count: pl.BlockSpec((2, count, width), lambda j: (0, 0, 0))
    return pl.pallas_call(
        input_back_kernel,
        grid=(rows // block,),
        in_specs=[
            pair(PROMPT_DEV),
            pair(CONT_DEV),
            pair(CONT_DEV),
            part,
            whole(width),
            whole(width),
            whole(width),
            part,
            whole(1),
            part,
        ],
        out_specs=[part, whole(2)],
        out_shape=[
            jax.ShapeDtypeStruct((rows, width), bf16),
            jax.ShapeDtypeStruct((2, width), f32),
        ],
        scratch_shapes=[pltpu.VMEM((block, width), bf16)] * 2,
        compiler_params=params("arbitrary"),
        cost_estimate=cost(6 * rows * width * width, 20 * rows * width),
        name="input_back",
    )(prompt, own, near, grad_queries, w_query, w_key, w_value, tokens, gain[None], grad_resid)


def head_stack(block):
    first = lax.broadcasted_iota(jnp.int32, block.shape, 1) < block.shape[1] // 2
    zero = jnp.zeros_like(block)
    return jnp.concatenate([jnp.where(first, block, zero), jnp.where(first, zero, block)])


def head_merge(turned):
    half, rows = turned.shape[0] // 2, turned.shape[1] // 2
    return jnp.concatenate([turned[:half, :rows], turned[half:, rows:]]).T


def chunk_scores(chunk, keys, stack, near_bias, bias_ref, prompt_len):
    scores = matmul_nt(keys, stack)
    if chunk == 0:
        bias = bias_ref[...]
        return scores + jnp.concatenate([bias, bias], axis=1)
    tri = (PROMPT_DEV, PROMPT_DEV)
    after = lax.broadcasted_iota(jnp.int32, tri, 0) > lax.broadcasted_iota(jnp.int32, tri, 1)
    diag = jnp.where(after, f32(masked_score), f32(0.0))
    last = keys.shape[0] - PROMPT_DEV
    near_end = prompt_len + CONT_DEV
    pieces = [scores[:prompt_len], scores[prompt_len:near_end] + near_bias]
    if last > near_end:
        pieces.append(scores[near_end:last])
    pieces.append(scores[last:] + jnp.concatenate([diag, diag], axis=1))
    return jnp.concatenate(pieces)


def chunk_keys(chunk, prompt_len):
    return prompt_len if chunk == 0 else prompt_len + CONT_DEV + PROMPT_DEV * chunk


def attend_kernel(prompt_len, near_ref, q_ref, k_ref, v_ref, bias_ref, out_ref, log_ref):
    scale = bf16(1.0 / math.sqrt(q_ref.shape[1] // 2))
    chunks = q_ref.shape[0] // PROMPT_DEV

    def scores_of(chunk):
        stack = head_stack(q_ref[pl.ds(chunk * PROMPT_DEV, PROMPT_DEV), :] * scale)
        keys = k_ref[: chunk_keys(chunk, prompt_len), :]
        return chunk_scores(chunk, keys, stack, near_ref[0], bias_ref, prompt_len)

    scores = scores_of(0)
    for chunk in range(chunks):
        rows = pl.ds(chunk * PROMPT_DEV, PROMPT_DEV)
        size = chunk_keys(chunk, prompt_len)
        later = scores_of(chunk + 1) if chunk + 1 < chunks else None
        top = jnp.max(scores, axis=0, keepdims=True)
        weights = jnp.exp(scores - top)
        total = jnp.sum(weights, axis=0, keepdims=True)
        mixed = matmul_tn(v_ref[:size, :], rounded(weights)) / total
        out_ref[rows, :] = rounded(head_merge(mixed))
        log_ref[0, chunk : chunk + 1, :] = top + jnp.log(total)
        scores = later


def attend_back_kernel(
    prompt_len,
    near_ref,
    q_ref,
    k_ref,
    v_ref,
    bias_ref,
    log_ref,
    out_ref,
    grad_ref,
    dq_ref,
    first_ref,
    second_ref,
    near_out_ref,
    own_ref,
    dk_ref,
    dv_ref,
):
    scale = 1.0 / math.sqrt(q_ref.shape[1] // 2)
    half = q_ref.shape[1] // 2
    dk_ref[...] = jnp.zeros_like(dk_ref)
    dv_ref[...] = jnp.zeros_like(dv_ref)
    for chunk in range(q_ref.shape[0] // PROMPT_DEV):
        rows = pl.ds(chunk * PROMPT_DEV, PROMPT_DEV)
        size = chunk_keys(chunk, prompt_len)
        stack = head_stack(q_ref[rows, :] * bf16(scale))
        grad = grad_ref[rows, :]
        grad_stack = head_stack(grad)
        product = (grad.astype(f32) * out_ref[rows, :].astype(f32)).T
        inner = jnp.concatenate(
            [
                jnp.sum(product[:half], axis=0, keepdims=True),
                jnp.sum(product[half:], axis=0, keepdims=True),
            ],
            axis=1,
        )
        keys = k_ref[:size, :]
        scores = chunk_scores(chunk, keys, stack, near_ref[0], bias_ref, prompt_len)
        weights = jnp.exp(scores - log_ref[0, chunk : chunk + 1, :])
        dv_ref[:size, :] += matmul(rounded(weights), grad_stack)
        grad_prob = matmul_nt(v_ref[:size, :], grad_stack)
        grad_score = rounded(weights * (grad_prob - inner))
        dk_ref[:size, :] += matmul(grad_score, stack)
        dq_ref[rows, :] = rounded(head_merge(matmul_tn(keys, grad_score)) * scale)
    start = 0
    for ref in (first_ref, second_ref, near_out_ref, own_ref):
        count = ref.shape[1]
        ref[0] = rounded(dk_ref[start : start + count, :])
        ref[1] = rounded(dv_ref[start : start + count, :])
        start += count


def attend(near_bias, queries, keys, values, bias):
    rows, width = queries.shape
    size = keys.shape[0]
    prompt_len = bias.shape[0]
    lanes = 2 * width // HEADS
    pairs = HEADS // 2
    chunks = rows // PROMPT_DEV
    block = lambda count: pl.BlockSpec((count, lanes), lambda j: (0, j))
    return pl.pallas_call(
        functools.partial(attend_kernel, prompt_len),
        grid=(pairs,),
        in_specs=[
            pl.BlockSpec(memory_space=pltpu.SMEM),
            block(rows),
            block(size),
            block(size),
            pl.BlockSpec((prompt_len, PROMPT_DEV), lambda j: (0, 0)),
        ],
        out_specs=[
            block(rows),
            pl.BlockSpec((1, chunks, 2 * PROMPT_DEV), lambda j: (j, 0, 0)),
        ],
        out_shape=[
            jax.ShapeDtypeStruct((rows, width), bf16),
            jax.ShapeDtypeStruct((pairs, chunks, 2 * PROMPT_DEV), f32),
        ],
        compiler_params=params("arbitrary"),
        cost_estimate=cost(16 * rows * size * width, 4 * (rows + size) * width, rows * size * HEADS),
        name="attend",
    )(near_bias, queries, keys, values, bias)


def attend_back(near_bias, queries, keys, values, bias, log_total, attended, grad):
    rows, width = queries.shape
    size = keys.shape[0]
    prompt_len = bias.shape[0]
    lanes = 2 * width // HEADS
    pairs = HEADS // 2
    chunks = rows // PROMPT_DEV
    block = lambda count: pl.BlockSpec((count, lanes), lambda j: (0, j))
    counts = (prompt_len // 2, prompt_len // 2, CONT_DEV, CONT_DEV)
    return pl.pallas_call(
        functools.partial(attend_back_kernel, prompt_len),
        grid=(pairs,),
        in_specs=[
            pl.BlockSpec(memory_space=pltpu.SMEM),
            block(rows),
            block(size),
            block(size),
            pl.BlockSpec((prompt_len, PROMPT_DEV), lambda j: (0, 0)),
            pl.BlockSpec((1, chunks, 2 * PROMPT_DEV), lambda j: (j, 0, 0)),
            block(rows),
            block(rows),
        ],
        out_specs=[block(rows)]
        + [pl.BlockSpec((2, count, lanes), lambda j: (0, 0, j)) for count in counts],
        out_shape=[jax.ShapeDtypeStruct((rows, width), bf16)]
        + [jax.ShapeDtypeStruct((2, count, width), bf16) for count in counts],
        scratch_shapes=[pltpu.VMEM((size, lanes), f32), pltpu.VMEM((size, lanes), f32)],
        compiler_params=params("arbitrary"),
        cost_estimate=cost(40 * rows * size * width, 8 * (rows + size) * width, rows * size * HEADS),
        name="attend_back",
    )(near_bias, queries, keys, values, bias, log_total, attended, grad)


def local(
    tokens_in,
    cotangent,
    hash_ids,
    norm1_gain,
    norm1_bias,
    w_query,
    w_key,
    w_value,
    w_output,
    norm2_gain,
    norm2_bias,
    expert_in,
    expert_out,
):
    row_count, width = tokens_in.shape
    experts = lax.axis_size("expert")
    groups = lax.axis_size("group")
    position = lax.axis_index("expert")
    group = lax.axis_index("group")
    capacity = 2 * row_count // experts
    slots = experts * capacity
    tied = lax.optimization_barrier

    def all_exchanged(values):
        return lax.all_to_all(values, "expert", split_axis=0, concat_axis=0, tiled=True)

    def exchanged(values):
        got = all_exchanged(values.reshape(experts, capacity, width))
        return got.reshape(slots, width)

    near_tokens = lax.ppermute(
        tokens_in[PROMPT_DEV:], "expert", [(i, i + 1) for i in range(0, experts, 2)]
    )
    prompts, prompt_ids, near_tokens, last_tokens = gather_relative(
        tokens_in[:PROMPT_DEV], "expert", near_tokens
    )
    ids = jnp.broadcast_to(rounded(hash_ids), (row_count, 128))
    all_cot = lax.all_gather(jnp.concatenate([cotangent, ids], axis=1), "group")

    row_index = jnp.arange(row_count, dtype=jnp.int32)
    lower = rounded(row_index[:, None] >= row_index[None, :])

    routed = rounded(hash_ids == jnp.arange(experts, dtype=jnp.int32)[None, :])
    running = matmul(lower, routed)
    rank = (jnp.sum(running * routed.astype(f32), axis=-1) - 1.0).astype(jnp.int32)
    slot = hash_ids[:, 0] * capacity + rank
    spread = rounded(slot[None, :] == jnp.arange(slots, dtype=jnp.int32)[:, None])

    cot_sent, _ = tied((matmul(spread, cotangent, bf16), last_tokens))
    cot = {0: exchanged(cot_sent)}
    others_in, queries, keys, values = project(
        prompts + [near_tokens, tokens_in[PROMPT_DEV:]],
        norm1_gain,
        norm1_bias,
        w_query,
        w_key,
        w_value,
    )
    block_pos = jnp.stack([(position ^ r) * PROMPT_DEV for r in prompt_ids])
    prompt_pos = jnp.arange(PROMPT_DEV, dtype=jnp.int32)
    key_pos = (block_pos[:, None] + prompt_pos[None, :]).reshape(-1)
    query_pos = position * PROMPT_DEV + row_index[:PROMPT_DEV]
    bias = jnp.where(key_pos[:, None] <= query_pos[None, :], f32(0.0), f32(masked_score))
    near_bias = jnp.where(position % 2 == 1, f32(0.0), f32(masked_score))[None]
    cot[0], keys = tied((cot[0], keys))
    attended, log_total = attend(near_bias, queries, keys, values, bias)

    residual = tokens_in.astype(f32) + matmul(attended, w_output)
    ffn_in = rounded(normalize(residual, norm2_gain, norm2_bias)[0])
    rows = exchanged(matmul(spread, ffn_in, bf16))
    all_numbers = all_cot[:, :, width].astype(jnp.int32)[:, None]
    numbers = lambda masks: jnp.stack([group ^ mask for mask in masks])
    near_sent = spread_rows(numbers([1]), all_numbers, all_cot, experts)
    grad_hidden = expert_back(cot[0], expert_out)
    rows, grad_hidden, near_sent = tied((rows, grad_hidden, near_sent))
    all_rows = lax.all_gather(rows, "group")
    cot[1] = all_exchanged(near_sent)
    hidden, grad_pre, grad_rows = expert_front(rows, grad_hidden, expert_in)
    grad_rows, hidden, cot[1] = tied((grad_rows, hidden, cot[1]))
    grad_got = exchanged(grad_rows)
    produced = expert_produce(hidden, expert_out)
    far_sent = spread_rows(numbers(range(2, groups)), all_numbers, all_cot, experts, produced)
    far_sent, grad_got = tied((far_sent, grad_got))
    far_got = all_exchanged(far_sent)

    grad_resid, grad_attn, grad_attended, sums2 = resid_back(
        grad_got, spread, residual, norm2_gain, cotangent, w_output
    )
    grad_queries, back_first, back_second, back_near, back_own = attend_back(
        near_bias, queries, keys, values, bias, log_total, attended, grad_attended
    )
    backs = (back_first, back_second, back_near, back_own, grad_queries)
    prompt_sums = scatter_relative(back_first, back_second, "expert")
    prompt_sent = next(prompt_sums)
    near_back = lax.ppermute(
        back_near, "expert", [(i + 1, i) for i in range(0, experts, 2)]
    )
    weights = weight_parts(
        (position & 1)[None],
        attended,
        others_in,
        grad_attn,
        grad_queries,
        (back_first, back_second, back_near, back_own),
        groups,
        experts,
    )
    weights, prompt_sent, near_back, far_got = tied((weights, prompt_sent, near_back, far_got))
    weight_sums = weight_chain(*weights)
    weight_sent = next(weight_sums)
    place, _ = tied((group[None], weights))
    sums = own_sums(place, groups, hidden, grad_pre, rows, cot[0])
    prompt_sent, prompt_back = moved_on(prompt_sums, prompt_sent)
    sums, weight_sent, prompt_sent = tied((sums, weight_sent, prompt_sent))
    weight_sent, _ = moved_on(weight_sums, weight_sent)
    prompt_sent, prompt_back = moved_on(prompt_sums, prompt_sent)
    others = list(range(1, groups))
    number = jnp.stack([group] + [group ^ mask for mask in others])
    grad_expert_out, in_first = shard_sums(
        number, 0, groups, expert_in, expert_out, sums, all_rows, (cot[1], far_got)
    )
    in_first, weight_sent, prompt_sent = tied((in_first, weight_sent, prompt_sent))
    result_got = far_got[:, 0].reshape(slots, width)
    result = rounded(residual + matmul_tn(spread, result_got))
    over_group = lambda values: lax.all_to_all(
        values, "group", split_axis=0, concat_axis=0, tiled=True
    )
    got_first = over_group(in_first)
    weight_sent, _ = moved_on(weight_sums, weight_sent)
    number, _ = tied((number, in_first))
    grad_expert_out, in_second = shard_sums(
        number, 1, groups, expert_in, expert_out, sums, all_rows, (cot[1], far_got), grad_expert_out
    )
    got_first, in_second, weight_sent, prompt_sent = tied(
        (got_first, in_second, weight_sent, prompt_sent)
    )
    got_second = over_group(in_second)
    while prompt_sent is not None:
        prompt_sent, prompt_back = moved_on(prompt_sums, prompt_sent)
    grad_tokens, sums1 = input_back(
        prompt_back,
        back_own,
        near_back,
        grad_queries,
        w_query,
        w_key,
        w_value,
        tokens_in,
        norm1_gain,
        grad_resid,
    )
    got_second, weight_sent, vectors = tied(
        (got_second, weight_sent, jnp.concatenate([sums1, sums2]))
    )
    vectors = vector_sums(vectors)
    while weight_sent is not None:
        weight_sent, weight_grads = moved_on(weight_sums, weight_sent)
    grad_expert_in = lay_out([got_first, got_second])
    grad_w_output, grad_w_query, grad_w_key, grad_w_value = weight_grads
    return (
        result,
        grad_tokens,
        vectors[0],
        vectors[1],
        grad_w_query,
        grad_w_key,
        grad_w_value,
        grad_w_output,
        vectors[2],
        vectors[3],
        grad_expert_in,
        grad_expert_out,
    )


def solution(mesh):
    both = ("group", "expert")
    return jax.shard_map(
        local,
        mesh=mesh,
        in_specs=(
            P(both, None),
            P(both, None),
            P(both, None),
            P(),
            P(),
            P(),
            P(),
            P(),
            P(),
            P(),
            P(),
            P("expert", None, None),
            P("expert", None, None),
        ),
        out_specs=(
            P(both, None),
            P(both, None),
            P(both),
            P(both),
            P(both, None),
            P(both, None),
            P(both, None),
            P(both, None),
            P(both),
            P(both),
            P("expert", "group", None),
            P("expert", "group", None),
        ),
        check_vma=False,
    )
```

```python
import functools
import math

import jax
import jax.numpy as jnp
from jax import lax
from jax.experimental import pallas as pl
from jax.experimental.pallas import tpu as pltpu
from jax.sharding import PartitionSpec as P

HEADS = 16
PROMPT_DEV = 128
CONT_DEV = 384


norm_eps = 1e-05
masked_score = -1e30
bf16 = jnp.bfloat16
f32 = jnp.float32
MIB = 1 << 20
share = 0.05


def swapped(block, axis, mask):
    return lax.ppermute(block, axis, [(i, i ^ mask) for i in range(lax.axis_size(axis))])


def rounded(values):
    return values.astype(bf16)


def normalize(values, gain, shift):
    average = jnp.mean(values, axis=-1, keepdims=True)
    centered = values - average
    variance = jnp.mean(centered * centered, axis=-1, keepdims=True)
    inverse = lax.rsqrt(variance + norm_eps)
    normed = centered * inverse
    return (normed * gain + shift, normed, inverse)


def norm_back(grad_out, gain, normed, inverse):
    scaled = grad_out * gain
    first_mean = jnp.mean(scaled, axis=-1, keepdims=True)
    second = jnp.mean(scaled * normed, axis=-1, keepdims=True)
    return inverse * (scaled - first_mean - normed * second)


def matmul(a, b, kind=f32):
    return jnp.dot(a, b, preferred_element_type=f32).astype(kind)


def matmul_nt(a, b, kind=f32):
    return lax.dot_general(a, b, (((1,), (1,)), ((), ())), preferred_element_type=f32).astype(kind)


def matmul_tn(a, b, kind=f32):
    return lax.dot_general(a, b, (((0,), (0,)), ((), ())), preferred_element_type=f32).astype(kind)


def outer_bits(size):
    return range(size.bit_length() - 2, 0, -1)


def gather_relative(block, axis, more):
    size = lax.axis_size(axis)
    pieces = {0: block}
    ready, last = [0], []
    while ready:
        fresh = {}
        for r in ready:
            for bit in outer_bits(size):
                if r ^ (1 << bit) not in pieces and r ^ (1 << bit) not in fresh:
                    fresh[r ^ (1 << bit)] = swapped(pieces[r], axis, 1 << bit)
        fresh, more = lax.optimization_barrier((fresh, more))
        pieces.update(fresh)
        ready, last = list(fresh), list(fresh.values()) or last
    near = sorted(pieces)
    for r in near:
        pieces[r ^ 1] = swapped(pieces[r], axis, 1)
    order = near + [r ^ 1 for r in near]
    return [pieces[r] for r in order], order, more, last


def scatter_relative(near, far, axis):
    size = lax.axis_size(axis)
    got = yield swapped(far, axis, 1)
    both = added(near, got)
    count = size // 2
    rows = both.shape[1] // count
    pieces = {2 * i: rounded(both[:, i * rows : (i + 1) * rows]) for i in range(count)}
    bits = list(outer_bits(size))
    for level in range(len(bits), 0, -1):
        sent, spans = [], []
        for r in [r for r in sorted(pieces) if bin(r).count("1") == level]:
            ways = [bit for bit in bits if r >> bit & 1]
            if rows % (16 * len(ways)):
                ways = ways[:1]
            part = rows // len(ways)
            piece = pieces.pop(r)
            for i, bit in enumerate(ways):
                span = (i * part, (i + 1) * part)
                sent.append(swapped(piece[:, span[0] : span[1]], axis, 1 << bit))
                spans.append((r ^ (1 << bit), span))
        gots = yield sent
        for r in sorted(pieces):
            total = pieces[r].astype(f32)
            for got, (target, span) in zip(gots, spans):
                if target == r:
                    outside = ((0, 0), (span[0], rows - span[1]), (0, 0))
                    total = total + jnp.pad(got.astype(f32), outside)
            pieces[r] = rounded(total)
    return pieces[0]


def halved(blocks, place, axis, bit):
    own = (lax.axis_index(axis) >> bit) & 1
    return (
        lax.dynamic_index_in_dim(blocks, own, place, keepdims=False),
        lax.dynamic_index_in_dim(blocks, 1 - own, place, keepdims=False),
    )


def added(keep, got):
    return keep.astype(f32) + got.astype(f32)


def places_of(bits, bit, value):
    rest = [other for other in bits if other != bit]
    weight = {other: 1 << (len(bits) - 1 - i) for i, other in enumerate(bits)}
    places = []
    for number in range(1 << len(rest)):
        place = value * weight[bit]
        for i, other in enumerate(rest):
            place = place + (number >> (len(rest) - 1 - i) & 1) * weight[other]
        places.append(place)
    return places


def halve_kernel(lefts, bits, own_ref, *refs):
    sets = len(lefts)
    for k, (left, bit) in enumerate(zip(lefts, bits)):
        keep_ref, got_ref = refs[2 * k : 2 * k + 2]
        outs = refs[2 * sets + 2 * k : 2 * sets + 2 * k + 2]
        own = (own_ref[0] >> bit) & 1
        for ref, value in zip(outs, (own, 1 - own)):
            for i, place in enumerate(places_of(left, bit, value)):
                for j in range(ref.shape[1]):
                    ref[0, j, i] = rounded(added(keep_ref[0, j, place], got_ref[0, j, place]))


def halve(number, states, bits):
    _, groups, count, rows, width = states[0][0].shape
    shape = (2, groups, count // 2, rows, width)
    came = lambda first: pl.BlockSpec(
        (1, groups, count, rows, width), lambda i: (first + i if first else i, 0, 0, 0, 0)
    )
    out = pl.BlockSpec((1, groups, count // 2, rows, width), lambda i: (i, 0, 0, 0, 0))
    size = 2 * math.prod(shape)
    outs = pl.pallas_call(
        functools.partial(halve_kernel, [state[3] for state in states], bits),
        grid=(2,),
        in_specs=[pl.BlockSpec(memory_space=pltpu.SMEM)]
        + [came(state[2]) for state in states for _ in range(2)],
        out_specs=[out] * (2 * len(states)),
        out_shape=[jax.ShapeDtypeStruct(shape, bf16)] * (2 * len(states)),
        compiler_params=params("arbitrary"),
        cost_estimate=cost(2 * size, 12 * size),
        name="halve",
    )(number, *[value for state in states for value in state[:2]])
    return list(zip(outs[::2], outs[1::2]))


def turn_kernel(own_ref, *refs):
    (*sets, own_out_ref, send_ref) = refs
    own = own_ref[0] & 1
    start = 0
    for keep_ref, got_ref in zip(sets[::2], sets[1::2]):
        for i in range(keep_ref.shape[0]):
            for j in range(keep_ref.shape[1] // 2):
                for ref, value in ((own_out_ref, own), (send_ref, 1 - own)):
                    place = 2 * j + value
                    ref[start + i, j] = rounded(added(keep_ref[i, place, 0], got_ref[i, place, 0]))
        start += keep_ref.shape[0]


def turn(number, sets):
    _, groups, _, rows, width = sets[0].shape
    shape = (4, groups // 2, rows, width)
    return pl.pallas_call(
        turn_kernel,
        in_specs=[pl.BlockSpec(memory_space=pltpu.SMEM)]
        + [pl.BlockSpec(memory_space=pltpu.VMEM)] * len(sets),
        out_specs=[pl.BlockSpec(memory_space=pltpu.VMEM)] * 2,
        out_shape=[jax.ShapeDtypeStruct(shape, bf16)] * 2,
        compiler_params=params(),
        cost_estimate=cost(8 * sets[0].size, 8 * sets[0].size),
        name="turn",
    )(number, *sets)


def weight_chain(keep, send, marks):
    bits = list(range(1, lax.axis_size("expert").bit_length() - 1))
    number = lax.axis_index("expert")[None]
    got = yield swapped(send, "expert", 1)
    states = [(keep, got, 0, bits[::-1]), (keep, got, 2, bits[::-1])]
    for pair in zip(bits, bits[::-1]):
        halves = halve(number, states, pair)
        marks.append(halves[0][0])
        gots = yield [swapped(send, "expert", 1 << bit) for bit, (_, send) in zip(pair, halves)]
        states = [
            (keep, got, 0, [other for other in state[3] if other != bit])
            for state, bit, (keep, _), got in zip(states, pair, halves, gots)
        ]
    keep, send = turn(
        lax.axis_index("group")[None], [value for state in states for value in state[:2]]
    )
    marks.append(keep)
    got = yield swapped(send, "group", 1)
    both = added(keep, got)
    bits = list(range(1, lax.axis_size("group").bit_length() - 1))
    both = both.reshape((4,) + (2,) * len(bits) + both.shape[-2:])
    left = bits[::-1]
    for bit in bits:
        keep, send = halved(rounded(both), 1 + left.index(bit), "group", bit)
        left.remove(bit)
        got = yield swapped(send, "group", 1 << bit)
        both = added(keep, got)
    return [both[i] for i in range(both.shape[0])]


def moved_on(chain, came):
    try:
        return chain.send(came), None
    except StopIteration as stop:
        return None, stop.value


def vector_sums(vectors):
    for axis in ("expert", "group"):
        for bit in range(lax.axis_size(axis).bit_length() - 1):
            got = yield swapped(vectors, axis, 1 << bit)
            vectors = vectors + got
    part = vectors.shape[1] // (lax.axis_size("group") * lax.axis_size("expert"))
    place = lax.axis_index("group") * lax.axis_size("expert") + lax.axis_index("expert")
    return lax.dynamic_slice_in_dim(vectors, place * part, part, axis=1)


def params(*semantics):
    return pltpu.CompilerParams(dimension_semantics=semantics, vmem_limit_bytes=60 * MIB)


def cost(flops, total_bytes, exps=0):
    return pl.CostEstimate(
        flops=int(flops * share), bytes_accessed=int(total_bytes * share), transcendentals=int(exps * share)
    )


def logistic(values):
    return 0.5 * jnp.tanh(0.5 * values) + 0.5


def back_kernel(cot_ref, wout_ref, out_ref):
    out_ref[...] = matmul_nt(cot_ref[...], wout_ref[0], bf16)


def expert_back(cot, expert_out):
    count, width = cot.shape
    ff = expert_out.shape[1]
    block = 1024
    return pl.pallas_call(
        back_kernel,
        grid=(ff // block,),
        in_specs=[
            pl.BlockSpec((count, width), lambda j: (0, 0)),
            pl.BlockSpec((1, block, width), lambda j: (0, j, 0)),
        ],
        out_specs=pl.BlockSpec((count, block), lambda j: (0, j)),
        out_shape=jax.ShapeDtypeStruct((count, ff), bf16),
        compiler_params=params("arbitrary"),
        cost_estimate=cost(2 * count * width * ff, 2 * count * ff + 2 * width * ff),
        name="expert_back",
    )(cot, expert_out)


def front_kernel(parts, rows_ref, gh_ref, win_ref, hidden_ref, pre_ref, out_ref, acc_ref):
    step = pl.program_id(0)
    count = rows_ref.shape[0] // parts

    @pl.when(step == 0)
    def _():
        acc_ref[...] = jnp.zeros_like(acc_ref)

    first = lambda i: matmul(rows_ref[i * count : (i + 1) * count, :], win_ref[0])
    pre = first(0)
    for i in range(parts):
        later = first(i + 1) if i + 1 < parts else None
        here = pl.ds(i * count, count)
        sig = logistic(pre)
        hidden = pre * sig
        hidden_ref[here, :] = rounded(hidden)
        grad_pre = rounded(gh_ref[here, :].astype(f32) * sig * (1.0 + pre - hidden))
        pre_ref[here, :] = grad_pre
        acc_ref[here, :] += matmul_nt(grad_pre, win_ref[0])
        pre = later

    @pl.when(step == pl.num_programs(0) - 1)
    def _():
        out_ref[...] = rounded(acc_ref[...])


def expert_front(rows, grad_hidden, expert_in):
    count, width = rows.shape
    ff = expert_in.shape[2]
    block = 1024
    whole = pl.BlockSpec((count, width), lambda j: (0, 0))
    part = pl.BlockSpec((count, block), lambda j: (0, j))
    return pl.pallas_call(
        functools.partial(front_kernel, 4),
        grid=(ff // block,),
        in_specs=[whole, part, pl.BlockSpec((1, width, block), lambda j: (0, 0, j))],
        out_specs=[part, part, whole],
        out_shape=[
            jax.ShapeDtypeStruct((count, ff), bf16),
            jax.ShapeDtypeStruct((count, ff), bf16),
            jax.ShapeDtypeStruct((count, width), bf16),
        ],
        scratch_shapes=[pltpu.VMEM((count, width), f32)],
        compiler_params=params("arbitrary"),
        cost_estimate=cost(4 * count * width * ff, 6 * count * ff + 2 * width * ff, count * ff),
        name="expert_front",
    )(rows, grad_hidden, expert_in)


def produce_kernel(hidden_ref, wout_ref, out_ref, acc_ref):
    step = pl.program_id(0)
    part = matmul(hidden_ref[...], wout_ref[0])

    @pl.when(step == 0)
    def _():
        acc_ref[...] = part

    @pl.when(step > 0)
    def _():
        acc_ref[...] += part

    @pl.when(step == pl.num_programs(0) - 1)
    def _():
        out_ref[...] = rounded(acc_ref[...])


def expert_produce(hidden, expert_out):
    count, ff = hidden.shape
    width = expert_out.shape[2]
    block = 1024
    return pl.pallas_call(
        produce_kernel,
        grid=(ff // block,),
        in_specs=[
            pl.BlockSpec((count, block), lambda j: (0, j)),
            pl.BlockSpec((1, block, width), lambda j: (0, j, 0)),
        ],
        out_specs=pl.BlockSpec((count, width), lambda j: (0, 0)),
        out_shape=jax.ShapeDtypeStruct((count, width), bf16),
        scratch_shapes=[pltpu.VMEM((count, width), f32)],
        compiler_params=params("arbitrary"),
        cost_estimate=cost(2 * count * width * ff, 2 * count * ff + 2 * width * ff),
        name="expert_produce",
    )(hidden, expert_out)


def in_kernel(
    _, win_ref, wout_ref, own_rows_ref, own_pre_ref, near_rows_ref, near_ref, rows_ref, far_ref,
    in_ref, near_hidden_ref, hidden_ref, in_sum,
):
    step = pl.program_id(0)

    def shard(rows, cot):
        pre = matmul(rows, win_ref[0])
        grad_hidden = matmul_nt(cot, wout_ref[0])
        sig = logistic(pre)
        hidden = pre * sig
        grad_pre = rounded(grad_hidden * sig * (1.0 + pre - hidden))
        return rounded(hidden), matmul_tn(rows, grad_pre)

    @pl.when(step == 0)
    def _():
        rows = near_rows_ref[0]
        near_hidden_ref[...], inner = shard(rows, near_ref[...].reshape(rows.shape))
        in_sum[...] = matmul_tn(own_rows_ref[...], own_pre_ref[...]) + inner

    rows = rows_ref[0]
    hidden_ref[0], inner = shard(rows, far_ref[...].reshape(rows.shape))
    in_sum[...] += inner

    @pl.when(step == pl.num_programs(0) - 1)
    def _():
        in_ref[...] = rounded(in_sum[...]).reshape(in_ref.shape)


def in_sums(number, half, expert_in, expert_out, own, rows, near, far):
    groups, count, width = rows.shape
    sources, _, slots, _ = near.shape
    part = expert_in.shape[2] // groups
    block = part // 2
    column = lambda j, w: 2 * w[0] + half
    return pl.pallas_call(
        in_kernel,
        grid_spec=pltpu.PrefetchScalarGridSpec(
            num_scalar_prefetch=1,
            grid=(groups - 2,),
            in_specs=[
                pl.BlockSpec((1, width, block), lambda j, w: (0, 0, column(j, w))),
                pl.BlockSpec((1, block, width), lambda j, w: (0, column(j, w), 0)),
                pl.BlockSpec((count, width), lambda j, w: (0, 0)),
                pl.BlockSpec((count, block), lambda j, w: (0, column(j, w))),
                pl.BlockSpec((1, count, width), lambda j, w: (w[1], 0, 0)),
                pl.BlockSpec((sources, 1, slots, width), lambda j, w: (0, 0, 0, 0)),
                pl.BlockSpec((1, count, width), lambda j, w: (w[2 + j], 0, 0)),
                pl.BlockSpec((sources, 1, slots, width), lambda j, w: (0, 1 + j, 0, 0)),
            ],
            out_specs=[
                pl.BlockSpec((groups, width // groups, block), lambda j, w: (0, 0, 0)),
                pl.BlockSpec((count, block), lambda j, w: (0, 0)),
                pl.BlockSpec((1, count, block), lambda j, w: (j, 0, 0)),
            ],
            scratch_shapes=[pltpu.VMEM((width, block), f32)],
        ),
        out_shape=[
            jax.ShapeDtypeStruct((groups, width // groups, block), bf16),
            jax.ShapeDtypeStruct((count, block), bf16),
            jax.ShapeDtypeStruct((groups - 2, count, block), bf16),
        ],
        compiler_params=params("arbitrary"),
        cost_estimate=cost(6 * count * width * block * groups, 16e6, count * block * groups),
        name="in_sums",
    )(number, expert_in, expert_out, *own, rows, near, rows, far)


def out_kernel(_, hidden_ref, cot_ref, near_ref, far_ref, *refs):
    out_ref, total = refs[-2:]
    hiddens = refs[:-2]
    block = total.shape[0] // 2
    step = pl.program_id(0)
    cot = cot_ref[...]

    @pl.when(step == 0)
    def _():
        total[...] = matmul_tn(hidden_ref[...], cot)
        near = near_ref[...].reshape(cot.shape)
        for half in range(2):
            here = pl.ds(half * block, block)
            total[here, :] += matmul_tn(hiddens[2 * half][...], near)

    far = far_ref[...].reshape(cot.shape)
    for half in range(2):
        here = pl.ds(half * block, block)
        total[here, :] += matmul_tn(hiddens[2 * half + 1][0], far)

    @pl.when(step == pl.num_programs(0) - 1)
    def _():
        out_ref[0] = total[...]


def out_sums(number, own, near, far, hiddens):
    hidden, cot = own
    count, width = cot.shape
    sources, _, slots, _ = near.shape
    groups = number.shape[0]
    part = hidden.shape[1] // groups
    near_hidden = pl.BlockSpec((count, part // 2), lambda j, w: (0, 0))
    far_hidden = pl.BlockSpec((1, count, part // 2), lambda j, w: (j, 0, 0))
    return pl.pallas_call(
        out_kernel,
        grid_spec=pltpu.PrefetchScalarGridSpec(
            num_scalar_prefetch=1,
            grid=(groups - 2,),
            in_specs=[
                pl.BlockSpec((count, part), lambda j, w: (0, w[0])),
                pl.BlockSpec((count, width), lambda j, w: (0, 0)),
                pl.BlockSpec((sources, 1, slots, width), lambda j, w: (0, 0, 0, 0)),
                pl.BlockSpec((sources, 1, slots, width), lambda j, w: (0, 1 + j, 0, 0)),
            ]
            + [near_hidden, far_hidden] * 2,
            out_specs=pl.BlockSpec((1, part, width), lambda j, w: (0, 0, 0)),
            scratch_shapes=[pltpu.VMEM((part, width), f32)],
        ),
        out_shape=jax.ShapeDtypeStruct((1, part, width), f32),
        compiler_params=params("arbitrary"),
        cost_estimate=cost(2 * count * width * part * groups, 16e6),
        name="out_sums",
    )(number, hidden, cot, near, far, *hiddens)


def lay_kernel(*refs):
    gots, out_ref = refs[:-1], refs[-1]
    block = gots[0].shape[2]
    for i in range(gots[0].shape[0]):
        for j, ref in enumerate(gots):
            start = (i * len(gots) + j) * block
            out_ref[0, :, start : start + block] = ref[i].astype(f32)


def lay_out(gots):
    groups, rows, block = gots[0].shape
    tall = 64
    width = groups * block * len(gots)
    return pl.pallas_call(
        lay_kernel,
        grid=(rows // tall,),
        in_specs=[pl.BlockSpec((groups, tall, block), lambda j: (0, j, 0))] * len(gots),
        out_specs=pl.BlockSpec((1, tall, width), lambda j: (0, j, 0)),
        out_shape=jax.ShapeDtypeStruct((1, rows, width), f32),
        compiler_params=params("arbitrary"),
        cost_estimate=cost(rows * width, 6 * rows * width),
        name="lay_out",
    )(*gots)


def spread_kernel(first, _, ids_ref, values_ref, *refs):
    out_ref = refs[-1]
    experts, _, capacity, width = out_ref.shape

    def spread():
        rows = ids_ref.shape[2]
        ids = ids_ref[0]
        number = lax.broadcasted_iota(jnp.int32, (experts, rows), 0)
        routed = jnp.where(number == ids, f32(1.0), f32(0.0))
        square = (rows, rows)
        before = lax.broadcasted_iota(jnp.int32, square, 0) <= lax.broadcasted_iota(
            jnp.int32, square, 1
        )
        running = matmul(rounded(routed), rounded(jnp.where(before, f32(1.0), f32(0.0))))
        rank = jnp.sum(running * routed, axis=0, keepdims=True).astype(jnp.int32) - 1
        slot = ids * capacity + rank
        places = lax.broadcasted_iota(jnp.int32, (experts * capacity, rows), 0)
        onehot = rounded(jnp.where(places == slot, f32(1.0), f32(0.0)))
        out = matmul(onehot, values_ref[0, :, :width], bf16)
        out_ref[...] = out.reshape(out_ref.shape)

    if first:
        step = pl.program_id(0)

        @pl.when(step == 0)
        def _():
            out_ref[...] = refs[0][...].reshape(out_ref.shape)

        pl.when(step > 0)(spread)
    else:
        spread()


def spread_rows(numbers, ids, values, experts, first=None):
    _, rows, columns = values.shape
    width = columns - 128
    capacity = 2 * rows // experts
    start = 0 if first is None else 1
    count = numbers.shape[0] + start
    which = lambda j, w: w[jnp.maximum(j - start, 0)]
    specs = [
        pl.BlockSpec((1, 1, rows), lambda j, w: (which(j, w), 0, 0)),
        pl.BlockSpec((1, rows, columns), lambda j, w: (which(j, w), 0, 0)),
    ]
    operands = [ids, values]
    if start:
        specs.append(pl.BlockSpec(first.shape, lambda j, w: (0, 0)))
        operands.append(first)
    return pl.pallas_call(
        functools.partial(spread_kernel, start),
        grid_spec=pltpu.PrefetchScalarGridSpec(
            num_scalar_prefetch=1,
            grid=(count,),
            in_specs=specs,
            out_specs=pl.BlockSpec((experts, 1, capacity, width), lambda j, w: (0, j, 0, 0)),
        ),
        out_shape=jax.ShapeDtypeStruct((experts, count, capacity, width), bf16),
        compiler_params=params("arbitrary"),
        cost_estimate=cost(2 * count * experts * capacity * rows * width, 8e6),
        name="spread_rows",
    )(numbers, *operands)


def project_kernel(count, gain_ref, bias_ref, wq_ref, wk_ref, wv_ref, *refs):
    pieces, (in_ref, q_ref, k_ref, v_ref, scratch) = refs[:count], refs[count:]

    @pl.when(pl.program_id(0) == 0)
    def _():
        start = 0
        for ref in pieces:
            end = start + ref.shape[0]
            values = normalize(ref[...].astype(f32), gain_ref[...], bias_ref[...])[0]
            scratch[start:end, :] = rounded(values)
            start = end
        in_ref[...] = scratch[...]

    first, last = pieces[0].shape[0], pieces[-1].shape[0]
    size = scratch.shape[0]
    q_ref[:first, :] = matmul(scratch[:first, :], wq_ref[...], bf16)
    q_ref[first:, :] = matmul(scratch[size - last :, :], wq_ref[...], bf16)
    k_ref[...] = matmul(scratch[...], wk_ref[...], bf16)
    v_ref[...] = matmul(scratch[...], wv_ref[...], bf16)


def project(pieces, gain, shift, w_query, w_key, w_value):
    width = gain.shape[0]
    size = sum(p.shape[0] for p in pieces)
    own = pieces[0].shape[0] + pieces[-1].shape[0]
    block = 512
    whole = lambda rows: pl.BlockSpec((rows, width), lambda j: (0, 0))
    weights = pl.BlockSpec((width, block), lambda j: (0, j))
    columns = lambda rows: pl.BlockSpec((rows, block), lambda j: (0, j))
    return pl.pallas_call(
        functools.partial(project_kernel, len(pieces)),
        grid=(width // block,),
        in_specs=[whole(1), whole(1)] + [weights] * 3 + [whole(p.shape[0]) for p in pieces],
        out_specs=[whole(size), columns(own), columns(size), columns(size)],
        out_shape=[jax.ShapeDtypeStruct((rows, width), bf16) for rows in (size, own, size, size)],
        scratch_shapes=[pltpu.VMEM((size, width), bf16)],
        compiler_params=params("arbitrary"),
        cost_estimate=cost(4 * size * width * width, 8 * size * width + 4 * width * width),
        name="project",
    )(gain[None], shift[None], w_query, w_key, w_value, *pieces)


def weights_kernel(odd_ref, *refs):
    attended_ref, others_ref, grad_ref, dq_ref, *backs = refs[:-2]
    keep_ref, send_ref = refs[-2:]
    size = others_ref.shape[0]
    totals = [
        matmul_tn(attended_ref[...], grad_ref[...]),
        matmul_tn(others_ref[:PROMPT_DEV, :], dq_ref[:PROMPT_DEV, :])
        + matmul_tn(others_ref[size - CONT_DEV :, :], dq_ref[PROMPT_DEV:, :]),
    ]
    for i in range(2):
        total, start = None, 0
        for ref in backs:
            count = ref.shape[1]
            part = matmul_tn(others_ref[start : start + count, :], ref[i])
            total = part if total is None else total + part
            start += count
        totals.append(total)
    half, rows = keep_ref.shape[2:4]

    def put(even_ref, odd_ref):
        for i, total in enumerate(totals):
            for j in range(half):
                start = 2 * j * rows
                even_ref[i, 0, j] = rounded(total[start : start + rows])
                odd_ref[i, 0, j] = rounded(total[start + rows : start + 2 * rows])

    @pl.when(odd_ref[0] == 0)
    def _():
        put(keep_ref, send_ref)

    @pl.when(odd_ref[0] != 0)
    def _():
        put(send_ref, keep_ref)


def weight_parts(odd, attended, others_in, grad_attn, grad_queries, backs, groups, experts):
    width = attended.shape[1]
    part = width // groups
    rows = part // experts
    left = lambda m: pl.BlockSpec((m.shape[0], part), lambda j: (0, j))
    whole = lambda m: pl.BlockSpec(m.shape, lambda j: (0,) * m.ndim)
    lefts, rights = [attended, others_in], [grad_attn, grad_queries, *backs]
    shape = (4, groups, experts // 2, rows, width)
    out = pl.BlockSpec((4, 1) + shape[2:], lambda j: (0, j, 0, 0, 0))
    return pl.pallas_call(
        weights_kernel,
        grid=(groups,),
        in_specs=[pl.BlockSpec(memory_space=pltpu.SMEM)]
        + [left(m) for m in lefts]
        + [whole(m) for m in rights],
        out_specs=[out, out],
        out_shape=[jax.ShapeDtypeStruct(shape, bf16)] * 2,
        compiler_params=params("arbitrary"),
        cost_estimate=cost(10e9, 30e6),
        name="weight_parts",
    )(odd, *lefts, *rights)


def resid_back_kernel(
    got_ref, spread_ref, resid_ref, gain_ref, cot_ref, wo_ref, grad_ref, attn_ref, attended_ref, sums_ref
):
    grad = matmul_tn(spread_ref[...], got_ref[...])
    _, normed, inverse = normalize(resid_ref[...], 1.0, 0.0)
    sums = jnp.concatenate(
        [jnp.sum(grad * normed, axis=0, keepdims=True), jnp.sum(grad, axis=0, keepdims=True)]
    )

    @pl.when(pl.program_id(0) == 0)
    def _():
        sums_ref[...] = sums

    @pl.when(pl.program_id(0) > 0)
    def _():
        sums_ref[...] += sums

    total = cot_ref[...].astype(f32) + norm_back(grad, gain_ref[...], normed, inverse)
    grad_ref[...] = total
    attn_ref[...] = rounded(total)
    attended_ref[...] = matmul_nt(rounded(total), wo_ref[...], bf16)


def resid_back(got, spread, residual, gain, cotangent, w_output):
    rows, width = residual.shape
    slots = got.shape[0]
    block = 256
    whole = lambda count: pl.BlockSpec((count, width), lambda j: (0, 0))
    part = pl.BlockSpec((block, width), lambda j: (j, 0))
    return pl.pallas_call(
        resid_back_kernel,
        grid=(rows // block,),
        in_specs=[
            whole(slots),
            pl.BlockSpec((slots, block), lambda j: (0, j)),
            part,
            whole(1),
            part,
            whole(width),
        ],
        out_specs=[part, part, part, whole(2)],
        out_shape=[
            jax.ShapeDtypeStruct((rows, width), f32),
            jax.ShapeDtypeStruct((rows, width), bf16),
            jax.ShapeDtypeStruct((rows, width), bf16),
            jax.ShapeDtypeStruct((2, width), f32),
        ],
        compiler_params=params("arbitrary"),
        cost_estimate=cost(2 * rows * width * (slots + width), 16 * rows * width),
        name="resid_back",
    )(got, spread, residual, gain[None], cotangent, w_output)


def input_back_kernel(
    prompt_ref, own_ref, near_ref, dq_ref, wq_ref, wk_ref, wv_ref, x_ref, gain_ref, resid_ref,
    out_ref, sums_ref, dk_ref, dv_ref,
):
    step = pl.program_id(0)
    block = dk_ref.shape[0]
    count = prompt_ref.shape[1]

    def put(first):
        for i, ref in enumerate((dk_ref, dv_ref)):
            start, size = (0, block - count) if first else (block - count, block)
            if first:
                ref[:count, :] = prompt_ref[i]
            here = pl.ds(start, size)
            ref[block - size :, :] = rounded(added(own_ref[i, here, :], near_ref[i, here, :]))

    pl.when(step == 0)(lambda: put(True))
    pl.when(step > 0)(lambda: put(False))
    grad = matmul_nt(dq_ref[...], wq_ref[...])
    grad = grad + matmul_nt(dk_ref[...], wk_ref[...])
    grad = grad + matmul_nt(dv_ref[...], wv_ref[...])
    _, normed, inverse = normalize(x_ref[...].astype(f32), 1.0, 0.0)
    sums = jnp.concatenate(
        [jnp.sum(grad * normed, axis=0, keepdims=True), jnp.sum(grad, axis=0, keepdims=True)]
    )

    @pl.when(step == 0)
    def _():
        sums_ref[...] = sums

    @pl.when(step > 0)
    def _():
        sums_ref[...] += sums

    out_ref[...] = rounded(resid_ref[...] + norm_back(grad, gain_ref[...], normed, inverse))


def input_back(prompt, own, near, grad_queries, w_query, w_key, w_value, tokens, gain, grad_resid):
    rows, width = tokens.shape
    block = rows // 2
    whole = lambda count: pl.BlockSpec((count, width), lambda j: (0, 0))
    part = pl.BlockSpec((block, width), lambda j: (j, 0))
    pair = lambda count: pl.BlockSpec((2, count, width), lambda j: (0, 0, 0))
    return pl.pallas_call(
        input_back_kernel,
        grid=(rows // block,),
        in_specs=[
            pair(PROMPT_DEV),
            pair(CONT_DEV),
            pair(CONT_DEV),
            part,
            whole(width),
            whole(width),
            whole(width),
            part,
            whole(1),
            part,
        ],
        out_specs=[part, whole(2)],
        out_shape=[
            jax.ShapeDtypeStruct((rows, width), bf16),
            jax.ShapeDtypeStruct((2, width), f32),
        ],
        scratch_shapes=[pltpu.VMEM((block, width), bf16)] * 2,
        compiler_params=params("arbitrary"),
        cost_estimate=cost(6 * rows * width * width, 20 * rows * width),
        name="input_back",
    )(prompt, own, near, grad_queries, w_query, w_key, w_value, tokens, gain[None], grad_resid)


def head_stack(block):
    first = lax.broadcasted_iota(jnp.int32, block.shape, 1) < block.shape[1] // 2
    zero = jnp.zeros_like(block)
    return jnp.concatenate([jnp.where(first, block, zero), jnp.where(first, zero, block)])


def head_merge(turned):
    half, rows = turned.shape[0] // 2, turned.shape[1] // 2
    return jnp.concatenate([turned[:half, :rows], turned[half:, rows:]]).T


def chunk_scores(chunk, keys, stack, near_bias, bias_ref, prompt_len):
    scores = matmul_nt(keys, stack)
    if chunk == 0:
        bias = bias_ref[...]
        return scores + jnp.concatenate([bias, bias], axis=1)
    tri = (PROMPT_DEV, PROMPT_DEV)
    after = lax.broadcasted_iota(jnp.int32, tri, 0) > lax.broadcasted_iota(jnp.int32, tri, 1)
    diag = jnp.where(after, f32(masked_score), f32(0.0))
    last = keys.shape[0] - PROMPT_DEV
    near_end = prompt_len + CONT_DEV
    pieces = [scores[:prompt_len], scores[prompt_len:near_end] + near_bias]
    if last > near_end:
        pieces.append(scores[near_end:last])
    pieces.append(scores[last:] + jnp.concatenate([diag, diag], axis=1))
    return jnp.concatenate(pieces)


def chunk_keys(chunk, prompt_len):
    return prompt_len if chunk == 0 else prompt_len + CONT_DEV + PROMPT_DEV * chunk


def attend_kernel(prompt_len, near_ref, q_ref, k_ref, v_ref, bias_ref, out_ref, log_ref):
    scale = bf16(1.0 / math.sqrt(q_ref.shape[1] // 2))
    chunks = q_ref.shape[0] // PROMPT_DEV

    def scores_of(chunk):
        stack = head_stack(q_ref[pl.ds(chunk * PROMPT_DEV, PROMPT_DEV), :] * scale)
        keys = k_ref[: chunk_keys(chunk, prompt_len), :]
        return chunk_scores(chunk, keys, stack, near_ref[0], bias_ref, prompt_len)

    scores = scores_of(0)
    for chunk in range(chunks):
        rows = pl.ds(chunk * PROMPT_DEV, PROMPT_DEV)
        size = chunk_keys(chunk, prompt_len)
        later = scores_of(chunk + 1) if chunk + 1 < chunks else None
        top = jnp.max(scores, axis=0, keepdims=True)
        weights = jnp.exp(scores - top)
        total = jnp.sum(weights, axis=0, keepdims=True)
        mixed = matmul_tn(v_ref[:size, :], rounded(weights)) / total
        out_ref[rows, :] = rounded(head_merge(mixed))
        log_ref[0, chunk : chunk + 1, :] = top + jnp.log(total)
        scores = later


def attend_back_kernel(
    prompt_len,
    near_ref,
    q_ref,
    k_ref,
    v_ref,
    bias_ref,
    log_ref,
    out_ref,
    grad_ref,
    dq_ref,
    first_ref,
    second_ref,
    near_out_ref,
    own_ref,
    dk_ref,
    dv_ref,
):
    scale = 1.0 / math.sqrt(q_ref.shape[1] // 2)
    half = q_ref.shape[1] // 2
    dk_ref[...] = jnp.zeros_like(dk_ref)
    dv_ref[...] = jnp.zeros_like(dv_ref)
    for chunk in range(q_ref.shape[0] // PROMPT_DEV):
        rows = pl.ds(chunk * PROMPT_DEV, PROMPT_DEV)
        size = chunk_keys(chunk, prompt_len)
        stack = head_stack(q_ref[rows, :] * bf16(scale))
        grad = grad_ref[rows, :]
        grad_stack = head_stack(grad)
        product = (grad.astype(f32) * out_ref[rows, :].astype(f32)).T
        inner = jnp.concatenate(
            [
                jnp.sum(product[:half], axis=0, keepdims=True),
                jnp.sum(product[half:], axis=0, keepdims=True),
            ],
            axis=1,
        )
        keys = k_ref[:size, :]
        scores = chunk_scores(chunk, keys, stack, near_ref[0], bias_ref, prompt_len)
        weights = jnp.exp(scores - log_ref[0, chunk : chunk + 1, :])
        dv_ref[:size, :] += matmul(rounded(weights), grad_stack)
        grad_prob = matmul_nt(v_ref[:size, :], grad_stack)
        grad_score = rounded(weights * (grad_prob - inner))
        dk_ref[:size, :] += matmul(grad_score, stack)
        dq_ref[rows, :] = rounded(head_merge(matmul_tn(keys, grad_score)) * scale)
    start = 0
    for ref in (first_ref, second_ref, near_out_ref, own_ref):
        count = ref.shape[1]
        ref[0] = rounded(dk_ref[start : start + count, :])
        ref[1] = rounded(dv_ref[start : start + count, :])
        start += count


def attend(near_bias, queries, keys, values, bias):
    rows, width = queries.shape
    size = keys.shape[0]
    prompt_len = bias.shape[0]
    lanes = 2 * width // HEADS
    pairs = HEADS // 2
    chunks = rows // PROMPT_DEV
    block = lambda count: pl.BlockSpec((count, lanes), lambda j: (0, j))
    return pl.pallas_call(
        functools.partial(attend_kernel, prompt_len),
        grid=(pairs,),
        in_specs=[
            pl.BlockSpec(memory_space=pltpu.SMEM),
            block(rows),
            block(size),
            block(size),
            pl.BlockSpec((prompt_len, PROMPT_DEV), lambda j: (0, 0)),
        ],
        out_specs=[
            block(rows),
            pl.BlockSpec((1, chunks, 2 * PROMPT_DEV), lambda j: (j, 0, 0)),
        ],
        out_shape=[
            jax.ShapeDtypeStruct((rows, width), bf16),
            jax.ShapeDtypeStruct((pairs, chunks, 2 * PROMPT_DEV), f32),
        ],
        compiler_params=params("arbitrary"),
        cost_estimate=cost(16 * rows * size * width, 4 * (rows + size) * width, rows * size * HEADS),
        name="attend",
    )(near_bias, queries, keys, values, bias)


def attend_back(near_bias, queries, keys, values, bias, log_total, attended, grad):
    rows, width = queries.shape
    size = keys.shape[0]
    prompt_len = bias.shape[0]
    lanes = 2 * width // HEADS
    pairs = HEADS // 2
    chunks = rows // PROMPT_DEV
    block = lambda count: pl.BlockSpec((count, lanes), lambda j: (0, j))
    counts = (prompt_len // 2, prompt_len // 2, CONT_DEV, CONT_DEV)
    return pl.pallas_call(
        functools.partial(attend_back_kernel, prompt_len),
        grid=(pairs,),
        in_specs=[
            pl.BlockSpec(memory_space=pltpu.SMEM),
            block(rows),
            block(size),
            block(size),
            pl.BlockSpec((prompt_len, PROMPT_DEV), lambda j: (0, 0)),
            pl.BlockSpec((1, chunks, 2 * PROMPT_DEV), lambda j: (j, 0, 0)),
            block(rows),
            block(rows),
        ],
        out_specs=[block(rows)]
        + [pl.BlockSpec((2, count, lanes), lambda j: (0, 0, j)) for count in counts],
        out_shape=[jax.ShapeDtypeStruct((rows, width), bf16)]
        + [jax.ShapeDtypeStruct((2, count, width), bf16) for count in counts],
        scratch_shapes=[pltpu.VMEM((size, lanes), f32), pltpu.VMEM((size, lanes), f32)],
        compiler_params=params("arbitrary"),
        cost_estimate=cost(40 * rows * size * width, 8 * (rows + size) * width, rows * size * HEADS),
        name="attend_back",
    )(near_bias, queries, keys, values, bias, log_total, attended, grad)


def local(
    tokens_in,
    cotangent,
    hash_ids,
    norm1_gain,
    norm1_bias,
    w_query,
    w_key,
    w_value,
    w_output,
    norm2_gain,
    norm2_bias,
    expert_in,
    expert_out,
):
    row_count, width = tokens_in.shape
    experts = lax.axis_size("expert")
    groups = lax.axis_size("group")
    position = lax.axis_index("expert")
    group = lax.axis_index("group")
    capacity = 2 * row_count // experts
    slots = experts * capacity
    tied = lax.optimization_barrier

    def all_exchanged(values):
        return lax.all_to_all(values, "expert", split_axis=0, concat_axis=0, tiled=True)

    def exchanged(values):
        got = all_exchanged(values.reshape(experts, capacity, width))
        return got.reshape(slots, width)

    near_tokens = lax.ppermute(
        tokens_in[PROMPT_DEV:], "expert", [(i, i + 1) for i in range(0, experts, 2)]
    )
    prompts, prompt_ids, near_tokens, last_tokens = gather_relative(
        tokens_in[:PROMPT_DEV], "expert", near_tokens
    )
    ids = jnp.broadcast_to(rounded(hash_ids), (row_count, 128))
    all_cot = lax.all_gather(jnp.concatenate([cotangent, ids], axis=1), "group")

    row_index = jnp.arange(row_count, dtype=jnp.int32)
    lower = rounded(row_index[:, None] >= row_index[None, :])

    routed = rounded(hash_ids == jnp.arange(experts, dtype=jnp.int32)[None, :])
    running = matmul(lower, routed)
    rank = (jnp.sum(running * routed.astype(f32), axis=-1) - 1.0).astype(jnp.int32)
    slot = hash_ids[:, 0] * capacity + rank
    spread = rounded(slot[None, :] == jnp.arange(slots, dtype=jnp.int32)[:, None])

    cot_sent, _ = tied((matmul(spread, cotangent, bf16), last_tokens))
    cot = {0: exchanged(cot_sent)}
    others_in, queries, keys, values = project(
        prompts + [near_tokens, tokens_in[PROMPT_DEV:]],
        norm1_gain,
        norm1_bias,
        w_query,
        w_key,
        w_value,
    )
    block_pos = jnp.stack([(position ^ r) * PROMPT_DEV for r in prompt_ids])
    prompt_pos = jnp.arange(PROMPT_DEV, dtype=jnp.int32)
    key_pos = (block_pos[:, None] + prompt_pos[None, :]).reshape(-1)
    query_pos = position * PROMPT_DEV + row_index[:PROMPT_DEV]
    bias = jnp.where(key_pos[:, None] <= query_pos[None, :], f32(0.0), f32(masked_score))
    near_bias = jnp.where(position % 2 == 1, f32(0.0), f32(masked_score))[None]
    attended, log_total = attend(near_bias, queries, keys, values, bias)

    residual = tokens_in.astype(f32) + matmul(attended, w_output)
    ffn_in = rounded(normalize(residual, norm2_gain, norm2_bias)[0])
    rows = exchanged(matmul(spread, ffn_in, bf16))
    all_numbers = all_cot[:, :, width].astype(jnp.int32)[:, None]
    numbers = lambda masks: jnp.stack([group ^ mask for mask in masks])
    near_sent = spread_rows(numbers([1]), all_numbers, all_cot, experts)
    grad_hidden = expert_back(cot[0], expert_out)
    rows, grad_hidden, near_sent = tied((rows, grad_hidden, near_sent))
    all_rows = lax.all_gather(rows, "group")
    cot[1] = all_exchanged(near_sent)
    hidden, grad_pre, grad_rows = expert_front(rows, grad_hidden, expert_in)
    grad_rows, hidden, cot[1] = tied((grad_rows, hidden, cot[1]))
    grad_got = exchanged(grad_rows)
    produced = expert_produce(hidden, expert_out)
    far_sent = spread_rows(numbers(range(2, groups)), all_numbers, all_cot, experts, produced)
    far_sent, grad_got = tied((far_sent, grad_got))
    far_got = all_exchanged(far_sent)

    grad_resid, grad_attn, grad_attended, sums2 = resid_back(
        grad_got, spread, residual, norm2_gain, cotangent, w_output
    )
    grad_queries, back_first, back_second, back_near, back_own = attend_back(
        near_bias, queries, keys, values, bias, log_total, attended, grad_attended
    )
    backs = (back_first, back_second, back_near, back_own, grad_queries)
    prompt_sums = scatter_relative(back_first, back_second, "expert")
    prompt_sent = next(prompt_sums)
    near_back = lax.ppermute(
        back_near, "expert", [(i + 1, i) for i in range(0, experts, 2)]
    )
    weights = weight_parts(
        (position & 1)[None],
        attended,
        others_in,
        grad_attn,
        grad_queries,
        (back_first, back_second, back_near, back_own),
        groups,
        experts,
    )
    weights, prompt_sent, near_back, far_got = tied((weights, prompt_sent, near_back, far_got))
    marks = []
    weight_sums = weight_chain(*weights, marks)
    weight_sent = next(weight_sums)
    prompt_sent, prompt_back = moved_on(prompt_sums, prompt_sent)
    weight_sent, prompt_sent = tied((weight_sent, prompt_sent))
    weight_sent, _ = moved_on(weight_sums, weight_sent)
    prompt_sent, prompt_back = moved_on(prompt_sums, prompt_sent)
    number, _ = tied((numbers(range(groups)), marks[-1]))
    operands = (expert_in, expert_out, (rows, grad_pre), all_rows, cot[1], far_got)
    in_first, *hidden_first = in_sums(number, 0, *operands)
    over_group = lambda values: lax.all_to_all(
        values, "group", split_axis=0, concat_axis=0, tiled=True
    )
    weight_sent, in_first = tied((weight_sent, in_first))
    got_first = over_group(in_first)
    weight_sent, _ = moved_on(weight_sums, weight_sent)
    number, _ = tied((number, marks[-1]))
    in_second, *hidden_second = in_sums(number, 1, *operands)
    got_first, in_second = tied((got_first, in_second))
    got_second = over_group(in_second)
    prompt_sent, weight_sent, number, _ = tied((prompt_sent, weight_sent, number, in_second))
    while prompt_sent is not None:
        prompt_sent, prompt_back = moved_on(prompt_sums, prompt_sent)
    grad_tokens, sums1 = input_back(
        prompt_back,
        back_own,
        near_back,
        grad_queries,
        w_query,
        w_key,
        w_value,
        tokens_in,
        norm1_gain,
        grad_resid,
    )
    number, _ = tied((number, sums1))
    grad_expert_out = out_sums(
        number, (hidden, cot[0]), cot[1], far_got, hidden_first + hidden_second
    )
    vector_steps = vector_sums(jnp.concatenate([sums1, sums2]))
    vectors = next(vector_steps)
    vectors = vector_steps.send(vectors)
    vectors, got_second, grad_expert_out = tied((vectors, got_second, grad_expert_out))
    vectors, _ = moved_on(vector_steps, vectors)
    while vectors is not None:
        vectors, vector_parts = moved_on(vector_steps, vectors)
    vectors = vector_parts
    while weight_sent is not None:
        weight_sent, weight_grads = moved_on(weight_sums, weight_sent)
    far_late, _ = tied((far_got, in_second))
    result_got = far_late[:, 0].reshape(slots, width)
    result = rounded(residual + matmul_tn(spread, result_got))
    grad_expert_in = lay_out([got_first, got_second])
    grad_w_output, grad_w_query, grad_w_key, grad_w_value = weight_grads
    return (
        result,
        grad_tokens,
        vectors[0],
        vectors[1],
        grad_w_query,
        grad_w_key,
        grad_w_value,
        grad_w_output,
        vectors[2],
        vectors[3],
        grad_expert_in,
        grad_expert_out,
    )


def solution(mesh):
    both = ("group", "expert")
    return jax.shard_map(
        local,
        mesh=mesh,
        in_specs=(
            P(both, None),
            P(both, None),
            P(both, None),
            P(),
            P(),
            P(),
            P(),
            P(),
            P(),
            P(),
            P(),
            P("expert", None, None),
            P("expert", None, None),
        ),
        out_specs=(
            P(both, None),
            P(both, None),
            P(both),
            P(both),
            P(both, None),
            P(both, None),
            P(both, None),
            P(both, None),
            P(both),
            P(both),
            P("expert", "group", None),
            P("expert", "group", None),
        ),
        check_vma=False,
    )
```

```python
import functools
import math

import jax
import jax.numpy as jnp
from jax import lax
from jax.experimental import pallas as pl
from jax.experimental.pallas import tpu as pltpu
from jax.sharding import PartitionSpec as P

HEADS = 16
PROMPT_DEV = 128
CONT_DEV = 384


norm_eps = 1e-05
masked_score = -1e30
bf16 = jnp.bfloat16
f32 = jnp.float32
MIB = 1 << 20
share = 0.05


def swapped(block, axis, mask):
    return lax.ppermute(block, axis, [(i, i ^ mask) for i in range(lax.axis_size(axis))])


def rounded(values):
    return values.astype(bf16)


def normalize(values, gain, shift):
    average = jnp.mean(values, axis=-1, keepdims=True)
    centered = values - average
    variance = jnp.mean(centered * centered, axis=-1, keepdims=True)
    inverse = lax.rsqrt(variance + norm_eps)
    normed = centered * inverse
    return (normed * gain + shift, normed, inverse)


def norm_back(grad_out, gain, normed, inverse):
    scaled = grad_out * gain
    first_mean = jnp.mean(scaled, axis=-1, keepdims=True)
    second = jnp.mean(scaled * normed, axis=-1, keepdims=True)
    return inverse * (scaled - first_mean - normed * second)


def matmul(a, b, kind=f32):
    return jnp.dot(a, b, preferred_element_type=f32).astype(kind)


def matmul_nt(a, b, kind=f32):
    return lax.dot_general(a, b, (((1,), (1,)), ((), ())), preferred_element_type=f32).astype(kind)


def matmul_tn(a, b, kind=f32):
    return lax.dot_general(a, b, (((0,), (0,)), ((), ())), preferred_element_type=f32).astype(kind)


def outer_bits(size):
    return range(size.bit_length() - 2, 0, -1)


def gather_relative(block, axis, more):
    size = lax.axis_size(axis)
    pieces = {0: block}
    ready, last = [0], []
    while ready:
        fresh = {}
        for r in ready:
            for bit in outer_bits(size):
                if r ^ (1 << bit) not in pieces and r ^ (1 << bit) not in fresh:
                    fresh[r ^ (1 << bit)] = swapped(pieces[r], axis, 1 << bit)
        fresh, more = lax.optimization_barrier((fresh, more))
        pieces.update(fresh)
        ready, last = list(fresh), list(fresh.values()) or last
    near = sorted(pieces)
    for r in near:
        pieces[r ^ 1] = swapped(pieces[r], axis, 1)
    order = near + [r ^ 1 for r in near]
    return [pieces[r] for r in order], order, more, last


def scatter_relative(near, far, axis):
    size = lax.axis_size(axis)
    got = yield swapped(far, axis, 1)
    both = added(near, got)
    count = size // 2
    rows = both.shape[1] // count
    pieces = {2 * i: rounded(both[:, i * rows : (i + 1) * rows]) for i in range(count)}
    bits = list(outer_bits(size))
    for level in range(len(bits), 0, -1):
        sent, spans = [], []
        for r in [r for r in sorted(pieces) if bin(r).count("1") == level]:
            ways = [bit for bit in bits if r >> bit & 1]
            if rows % (16 * len(ways)):
                ways = ways[:1]
            part = rows // len(ways)
            piece = pieces.pop(r)
            for i, bit in enumerate(ways):
                span = (i * part, (i + 1) * part)
                sent.append(swapped(piece[:, span[0] : span[1]], axis, 1 << bit))
                spans.append((r ^ (1 << bit), span))
        gots = yield sent
        for r in sorted(pieces):
            total = pieces[r].astype(f32)
            for got, (target, span) in zip(gots, spans):
                if target == r:
                    outside = ((0, 0), (span[0], rows - span[1]), (0, 0))
                    total = total + jnp.pad(got.astype(f32), outside)
            pieces[r] = rounded(total)
    return pieces[0]


def halved(blocks, place, axis, bit):
    own = (lax.axis_index(axis) >> bit) & 1
    return (
        lax.dynamic_index_in_dim(blocks, own, place, keepdims=False),
        lax.dynamic_index_in_dim(blocks, 1 - own, place, keepdims=False),
    )


def added(keep, got):
    return keep.astype(f32) + got.astype(f32)


def places_of(bits, bit, value):
    rest = [other for other in bits if other != bit]
    weight = {other: 1 << (len(bits) - 1 - i) for i, other in enumerate(bits)}
    places = []
    for number in range(1 << len(rest)):
        place = value * weight[bit]
        for i, other in enumerate(rest):
            place = place + (number >> (len(rest) - 1 - i) & 1) * weight[other]
        places.append(place)
    return places


def halve_kernel(lefts, bits, own_ref, *refs):
    sets = len(lefts)
    for k, (left, bit) in enumerate(zip(lefts, bits)):
        keep_ref, got_ref = refs[2 * k : 2 * k + 2]
        outs = refs[2 * sets + 2 * k : 2 * sets + 2 * k + 2]
        own = (own_ref[0] >> bit) & 1
        for ref, value in zip(outs, (own, 1 - own)):
            for i, place in enumerate(places_of(left, bit, value)):
                for j in range(ref.shape[1]):
                    ref[0, j, i] = rounded(added(keep_ref[0, j, place], got_ref[0, j, place]))


def halve(number, states, bits):
    _, groups, count, rows, width = states[0][0].shape
    shape = (2, groups, count // 2, rows, width)
    came = lambda first: pl.BlockSpec(
        (1, groups, count, rows, width), lambda i: (first + i if first else i, 0, 0, 0, 0)
    )
    out = pl.BlockSpec((1, groups, count // 2, rows, width), lambda i: (i, 0, 0, 0, 0))
    size = 2 * math.prod(shape)
    outs = pl.pallas_call(
        functools.partial(halve_kernel, [state[3] for state in states], bits),
        grid=(2,),
        in_specs=[pl.BlockSpec(memory_space=pltpu.SMEM)]
        + [came(state[2]) for state in states for _ in range(2)],
        out_specs=[out] * (2 * len(states)),
        out_shape=[jax.ShapeDtypeStruct(shape, bf16)] * (2 * len(states)),
        compiler_params=params("arbitrary"),
        cost_estimate=cost(2 * size, 12 * size),
        name="halve",
    )(number, *[value for state in states for value in state[:2]])
    return list(zip(outs[::2], outs[1::2]))


def turn_kernel(own_ref, *refs):
    (*sets, own_out_ref, send_ref) = refs
    own = own_ref[0] & 1
    start = 0
    for keep_ref, got_ref in zip(sets[::2], sets[1::2]):
        for i in range(keep_ref.shape[0]):
            for j in range(keep_ref.shape[1] // 2):
                for ref, value in ((own_out_ref, own), (send_ref, 1 - own)):
                    place = 2 * j + value
                    ref[start + i, j] = rounded(added(keep_ref[i, place, 0], got_ref[i, place, 0]))
        start += keep_ref.shape[0]


def turn(number, sets):
    _, groups, _, rows, width = sets[0].shape
    shape = (4, groups // 2, rows, width)
    return pl.pallas_call(
        turn_kernel,
        in_specs=[pl.BlockSpec(memory_space=pltpu.SMEM)]
        + [pl.BlockSpec(memory_space=pltpu.VMEM)] * len(sets),
        out_specs=[pl.BlockSpec(memory_space=pltpu.VMEM)] * 2,
        out_shape=[jax.ShapeDtypeStruct(shape, bf16)] * 2,
        compiler_params=params(),
        cost_estimate=cost(8 * sets[0].size, 8 * sets[0].size),
        name="turn",
    )(number, *sets)


def weight_chain(keep, send, marks):
    bits = list(range(1, lax.axis_size("expert").bit_length() - 1))
    number = lax.axis_index("expert")[None]
    got = yield swapped(send, "expert", 1)
    states = [(keep, got, 0, bits[::-1]), (keep, got, 2, bits[::-1])]
    for pair in zip(bits, bits[::-1]):
        halves = halve(number, states, pair)
        marks.append(halves[0][0])
        gots = yield [swapped(send, "expert", 1 << bit) for bit, (_, send) in zip(pair, halves)]
        states = [
            (keep, got, 0, [other for other in state[3] if other != bit])
            for state, bit, (keep, _), got in zip(states, pair, halves, gots)
        ]
    keep, send = turn(
        lax.axis_index("group")[None], [value for state in states for value in state[:2]]
    )
    marks.append(keep)
    got = yield swapped(send, "group", 1)
    both = added(keep, got)
    bits = list(range(1, lax.axis_size("group").bit_length() - 1))
    both = both.reshape((4,) + (2,) * len(bits) + both.shape[-2:])
    left = bits[::-1]
    for bit in bits:
        keep, send = halved(rounded(both), 1 + left.index(bit), "group", bit)
        left.remove(bit)
        got = yield swapped(send, "group", 1 << bit)
        both = added(keep, got)
    return [both[i] for i in range(both.shape[0])]


def moved_on(chain, came):
    try:
        return chain.send(came), None
    except StopIteration as stop:
        return None, stop.value


def vector_sums(vectors):
    axes = ("group", "expert")
    devices = lax.axis_size("group") * lax.axis_size("expert")
    count, width = vectors.shape
    pieces = vectors.reshape(count, devices, width // devices).swapaxes(0, 1)
    got = lax.all_to_all(pieces, axes, split_axis=0, concat_axis=0, tiled=True)
    return jnp.sum(got, axis=0)


def params(*semantics):
    return pltpu.CompilerParams(dimension_semantics=semantics, vmem_limit_bytes=60 * MIB)


def cost(flops, total_bytes, exps=0):
    return pl.CostEstimate(
        flops=int(flops * share), bytes_accessed=int(total_bytes * share), transcendentals=int(exps * share)
    )


def logistic(values):
    return 0.5 * jnp.tanh(0.5 * values) + 0.5


def back_kernel(cot_ref, wout_ref, out_ref):
    out_ref[...] = matmul_nt(cot_ref[...], wout_ref[0], bf16)


def expert_back(cot, expert_out):
    count, width = cot.shape
    ff = expert_out.shape[1]
    block = 1024
    return pl.pallas_call(
        back_kernel,
        grid=(ff // block,),
        in_specs=[
            pl.BlockSpec((count, width), lambda j: (0, 0)),
            pl.BlockSpec((1, block, width), lambda j: (0, j, 0)),
        ],
        out_specs=pl.BlockSpec((count, block), lambda j: (0, j)),
        out_shape=jax.ShapeDtypeStruct((count, ff), bf16),
        compiler_params=params("arbitrary"),
        cost_estimate=cost(2 * count * width * ff, 2 * count * ff + 2 * width * ff),
        name="expert_back",
    )(cot, expert_out)


def front_kernel(parts, rows_ref, gh_ref, win_ref, hidden_ref, pre_ref, out_ref, acc_ref):
    step = pl.program_id(0)
    count = rows_ref.shape[0] // parts

    @pl.when(step == 0)
    def _():
        acc_ref[...] = jnp.zeros_like(acc_ref)

    first = lambda i: matmul(rows_ref[i * count : (i + 1) * count, :], win_ref[0])
    pre = first(0)
    for i in range(parts):
        later = first(i + 1) if i + 1 < parts else None
        here = pl.ds(i * count, count)
        sig = logistic(pre)
        hidden = pre * sig
        hidden_ref[here, :] = rounded(hidden)
        grad_pre = rounded(gh_ref[here, :].astype(f32) * sig * (1.0 + pre - hidden))
        pre_ref[here, :] = grad_pre
        acc_ref[here, :] += matmul_nt(grad_pre, win_ref[0])
        pre = later

    @pl.when(step == pl.num_programs(0) - 1)
    def _():
        out_ref[...] = rounded(acc_ref[...])


def expert_front(rows, grad_hidden, expert_in):
    count, width = rows.shape
    ff = expert_in.shape[2]
    block = 1024
    whole = pl.BlockSpec((count, width), lambda j: (0, 0))
    part = pl.BlockSpec((count, block), lambda j: (0, j))
    return pl.pallas_call(
        functools.partial(front_kernel, 4),
        grid=(ff // block,),
        in_specs=[whole, part, pl.BlockSpec((1, width, block), lambda j: (0, 0, j))],
        out_specs=[part, part, whole],
        out_shape=[
            jax.ShapeDtypeStruct((count, ff), bf16),
            jax.ShapeDtypeStruct((count, ff), bf16),
            jax.ShapeDtypeStruct((count, width), bf16),
        ],
        scratch_shapes=[pltpu.VMEM((count, width), f32)],
        compiler_params=params("arbitrary"),
        cost_estimate=cost(4 * count * width * ff, 6 * count * ff + 2 * width * ff, count * ff),
        name="expert_front",
    )(rows, grad_hidden, expert_in)


def produce_kernel(hidden_ref, wout_ref, out_ref, acc_ref):
    step = pl.program_id(0)
    part = matmul(hidden_ref[...], wout_ref[0])

    @pl.when(step == 0)
    def _():
        acc_ref[...] = part

    @pl.when(step > 0)
    def _():
        acc_ref[...] += part

    @pl.when(step == pl.num_programs(0) - 1)
    def _():
        out_ref[...] = rounded(acc_ref[...])


def expert_produce(hidden, expert_out):
    count, ff = hidden.shape
    width = expert_out.shape[2]
    block = 1024
    return pl.pallas_call(
        produce_kernel,
        grid=(ff // block,),
        in_specs=[
            pl.BlockSpec((count, block), lambda j: (0, j)),
            pl.BlockSpec((1, block, width), lambda j: (0, j, 0)),
        ],
        out_specs=pl.BlockSpec((count, width), lambda j: (0, 0)),
        out_shape=jax.ShapeDtypeStruct((count, width), bf16),
        scratch_shapes=[pltpu.VMEM((count, width), f32)],
        compiler_params=params("arbitrary"),
        cost_estimate=cost(2 * count * width * ff, 2 * count * ff + 2 * width * ff),
        name="expert_produce",
    )(hidden, expert_out)


def in_kernel(
    _, win_ref, wout_ref, own_rows_ref, own_pre_ref, near_rows_ref, near_ref, rows_ref, far_ref,
    in_ref, near_hidden_ref, hidden_ref, in_sum,
):
    step = pl.program_id(0)

    def shard(rows, cot):
        pre = matmul(rows, win_ref[0])
        grad_hidden = matmul_nt(cot, wout_ref[0])
        sig = logistic(pre)
        hidden = pre * sig
        grad_pre = rounded(grad_hidden * sig * (1.0 + pre - hidden))
        return rounded(hidden), matmul_tn(rows, grad_pre)

    @pl.when(step == 0)
    def _():
        rows = near_rows_ref[0]
        near_hidden_ref[...], inner = shard(rows, near_ref[...].reshape(rows.shape))
        in_sum[...] = matmul_tn(own_rows_ref[...], own_pre_ref[...]) + inner

    rows = rows_ref[0]
    hidden_ref[0], inner = shard(rows, far_ref[...].reshape(rows.shape))
    in_sum[...] += inner

    @pl.when(step == pl.num_programs(0) - 1)
    def _():
        in_ref[...] = rounded(in_sum[...]).reshape(in_ref.shape)


def in_sums(number, half, expert_in, expert_out, own, rows, near, far):
    groups, count, width = rows.shape
    sources, _, slots, _ = near.shape
    part = expert_in.shape[2] // groups
    block = part // 2
    column = lambda j, w: 2 * w[0] + half
    return pl.pallas_call(
        in_kernel,
        grid_spec=pltpu.PrefetchScalarGridSpec(
            num_scalar_prefetch=1,
            grid=(groups - 2,),
            in_specs=[
                pl.BlockSpec((1, width, block), lambda j, w: (0, 0, column(j, w))),
                pl.BlockSpec((1, block, width), lambda j, w: (0, column(j, w), 0)),
                pl.BlockSpec((count, width), lambda j, w: (0, 0)),
                pl.BlockSpec((count, block), lambda j, w: (0, column(j, w))),
                pl.BlockSpec((1, count, width), lambda j, w: (w[1], 0, 0)),
                pl.BlockSpec((sources, 1, slots, width), lambda j, w: (0, 0, 0, 0)),
                pl.BlockSpec((1, count, width), lambda j, w: (w[2 + j], 0, 0)),
                pl.BlockSpec((sources, 1, slots, width), lambda j, w: (0, 1 + j, 0, 0)),
            ],
            out_specs=[
                pl.BlockSpec((groups, width // groups, block), lambda j, w: (0, 0, 0)),
                pl.BlockSpec((count, block), lambda j, w: (0, 0)),
                pl.BlockSpec((1, count, block), lambda j, w: (j, 0, 0)),
            ],
            scratch_shapes=[pltpu.VMEM((width, block), f32)],
        ),
        out_shape=[
            jax.ShapeDtypeStruct((groups, width // groups, block), bf16),
            jax.ShapeDtypeStruct((count, block), bf16),
            jax.ShapeDtypeStruct((groups - 2, count, block), bf16),
        ],
        compiler_params=params("arbitrary"),
        cost_estimate=cost(6 * count * width * block * groups, 16e6, count * block * groups),
        name="in_sums",
    )(number, expert_in, expert_out, *own, rows, near, rows, far)


def out_kernel(_, hidden_ref, cot_ref, near_ref, far_ref, *refs):
    out_ref, total = refs[-2:]
    hiddens = refs[:-2]
    block = total.shape[0] // 2
    step = pl.program_id(0)
    cot = cot_ref[...]

    @pl.when(step == 0)
    def _():
        total[...] = matmul_tn(hidden_ref[...], cot)
        near = near_ref[...].reshape(cot.shape)
        for half in range(2):
            here = pl.ds(half * block, block)
            total[here, :] += matmul_tn(hiddens[2 * half][...], near)

    far = far_ref[...].reshape(cot.shape)
    for half in range(2):
        here = pl.ds(half * block, block)
        total[here, :] += matmul_tn(hiddens[2 * half + 1][0], far)

    @pl.when(step == pl.num_programs(0) - 1)
    def _():
        out_ref[0] = total[...]


def out_sums(number, own, near, far, hiddens):
    hidden, cot = own
    count, width = cot.shape
    sources, _, slots, _ = near.shape
    groups = number.shape[0]
    part = hidden.shape[1] // groups
    near_hidden = pl.BlockSpec((count, part // 2), lambda j, w: (0, 0))
    far_hidden = pl.BlockSpec((1, count, part // 2), lambda j, w: (j, 0, 0))
    return pl.pallas_call(
        out_kernel,
        grid_spec=pltpu.PrefetchScalarGridSpec(
            num_scalar_prefetch=1,
            grid=(groups - 2,),
            in_specs=[
                pl.BlockSpec((count, part), lambda j, w: (0, w[0])),
                pl.BlockSpec((count, width), lambda j, w: (0, 0)),
                pl.BlockSpec((sources, 1, slots, width), lambda j, w: (0, 0, 0, 0)),
                pl.BlockSpec((sources, 1, slots, width), lambda j, w: (0, 1 + j, 0, 0)),
            ]
            + [near_hidden, far_hidden] * 2,
            out_specs=pl.BlockSpec((1, part, width), lambda j, w: (0, 0, 0)),
            scratch_shapes=[pltpu.VMEM((part, width), f32)],
        ),
        out_shape=jax.ShapeDtypeStruct((1, part, width), f32),
        compiler_params=params("arbitrary"),
        cost_estimate=cost(2 * count * width * part * groups, 16e6),
        name="out_sums",
    )(number, hidden, cot, near, far, *hiddens)


def lay_kernel(*refs):
    gots, out_ref = refs[:-1], refs[-1]
    block = gots[0].shape[2]
    for i in range(gots[0].shape[0]):
        for j, ref in enumerate(gots):
            start = (i * len(gots) + j) * block
            out_ref[0, :, start : start + block] = ref[i].astype(f32)


def lay_out(gots):
    groups, rows, block = gots[0].shape
    tall = 64
    width = groups * block * len(gots)
    return pl.pallas_call(
        lay_kernel,
        grid=(rows // tall,),
        in_specs=[pl.BlockSpec((groups, tall, block), lambda j: (0, j, 0))] * len(gots),
        out_specs=pl.BlockSpec((1, tall, width), lambda j: (0, j, 0)),
        out_shape=jax.ShapeDtypeStruct((1, rows, width), f32),
        compiler_params=params("arbitrary"),
        cost_estimate=cost(rows * width, 6 * rows * width),
        name="lay_out",
    )(*gots)


def spread_kernel(first, _, ids_ref, values_ref, *refs):
    out_ref = refs[-1]
    experts, _, capacity, width = out_ref.shape

    def spread():
        rows = ids_ref.shape[2]
        ids = ids_ref[0]
        number = lax.broadcasted_iota(jnp.int32, (experts, rows), 0)
        routed = jnp.where(number == ids, f32(1.0), f32(0.0))
        square = (rows, rows)
        before = lax.broadcasted_iota(jnp.int32, square, 0) <= lax.broadcasted_iota(
            jnp.int32, square, 1
        )
        running = matmul(rounded(routed), rounded(jnp.where(before, f32(1.0), f32(0.0))))
        rank = jnp.sum(running * routed, axis=0, keepdims=True).astype(jnp.int32) - 1
        slot = ids * capacity + rank
        places = lax.broadcasted_iota(jnp.int32, (experts * capacity, rows), 0)
        onehot = rounded(jnp.where(places == slot, f32(1.0), f32(0.0)))
        out = matmul(onehot, values_ref[0, :, :width], bf16)
        out_ref[...] = out.reshape(out_ref.shape)

    if first:
        step = pl.program_id(0)

        @pl.when(step == 0)
        def _():
            out_ref[...] = refs[0][...].reshape(out_ref.shape)

        pl.when(step > 0)(spread)
    else:
        spread()


def spread_rows(numbers, ids, values, experts, first=None):
    _, rows, columns = values.shape
    width = columns - 128
    capacity = 2 * rows // experts
    start = 0 if first is None else 1
    count = numbers.shape[0] + start
    which = lambda j, w: w[jnp.maximum(j - start, 0)]
    specs = [
        pl.BlockSpec((1, 1, rows), lambda j, w: (which(j, w), 0, 0)),
        pl.BlockSpec((1, rows, columns), lambda j, w: (which(j, w), 0, 0)),
    ]
    operands = [ids, values]
    if start:
        specs.append(pl.BlockSpec(first.shape, lambda j, w: (0, 0)))
        operands.append(first)
    return pl.pallas_call(
        functools.partial(spread_kernel, start),
        grid_spec=pltpu.PrefetchScalarGridSpec(
            num_scalar_prefetch=1,
            grid=(count,),
            in_specs=specs,
            out_specs=pl.BlockSpec((experts, 1, capacity, width), lambda j, w: (0, j, 0, 0)),
        ),
        out_shape=jax.ShapeDtypeStruct((experts, count, capacity, width), bf16),
        compiler_params=params("arbitrary"),
        cost_estimate=cost(2 * count * experts * capacity * rows * width, 8e6),
        name="spread_rows",
    )(numbers, *operands)


def project_kernel(count, gain_ref, bias_ref, wq_ref, wk_ref, wv_ref, *refs):
    pieces, (in_ref, q_ref, k_ref, v_ref, scratch) = refs[:count], refs[count:]

    @pl.when(pl.program_id(0) == 0)
    def _():
        start = 0
        for ref in pieces:
            end = start + ref.shape[0]
            values = normalize(ref[...].astype(f32), gain_ref[...], bias_ref[...])[0]
            scratch[start:end, :] = rounded(values)
            start = end
        in_ref[...] = scratch[...]

    first, last = pieces[0].shape[0], pieces[-1].shape[0]
    size = scratch.shape[0]
    q_ref[:first, :] = matmul(scratch[:first, :], wq_ref[...], bf16)
    q_ref[first:, :] = matmul(scratch[size - last :, :], wq_ref[...], bf16)
    k_ref[...] = matmul(scratch[...], wk_ref[...], bf16)
    v_ref[...] = matmul(scratch[...], wv_ref[...], bf16)


def project(pieces, gain, shift, w_query, w_key, w_value):
    width = gain.shape[0]
    size = sum(p.shape[0] for p in pieces)
    own = pieces[0].shape[0] + pieces[-1].shape[0]
    block = 512
    whole = lambda rows: pl.BlockSpec((rows, width), lambda j: (0, 0))
    weights = pl.BlockSpec((width, block), lambda j: (0, j))
    columns = lambda rows: pl.BlockSpec((rows, block), lambda j: (0, j))
    return pl.pallas_call(
        functools.partial(project_kernel, len(pieces)),
        grid=(width // block,),
        in_specs=[whole(1), whole(1)] + [weights] * 3 + [whole(p.shape[0]) for p in pieces],
        out_specs=[whole(size), columns(own), columns(size), columns(size)],
        out_shape=[jax.ShapeDtypeStruct((rows, width), bf16) for rows in (size, own, size, size)],
        scratch_shapes=[pltpu.VMEM((size, width), bf16)],
        compiler_params=params("arbitrary"),
        cost_estimate=cost(4 * size * width * width, 8 * size * width + 4 * width * width),
        name="project",
    )(gain[None], shift[None], w_query, w_key, w_value, *pieces)


def weights_kernel(odd_ref, *refs):
    attended_ref, others_ref, grad_ref, dq_ref, *backs = refs[:-2]
    keep_ref, send_ref = refs[-2:]
    size = others_ref.shape[0]
    totals = [
        matmul_tn(attended_ref[...], grad_ref[...]),
        matmul_tn(others_ref[:PROMPT_DEV, :], dq_ref[:PROMPT_DEV, :])
        + matmul_tn(others_ref[size - CONT_DEV :, :], dq_ref[PROMPT_DEV:, :]),
    ]
    for i in range(2):
        total, start = None, 0
        for ref in backs:
            count = ref.shape[1]
            part = matmul_tn(others_ref[start : start + count, :], ref[i])
            total = part if total is None else total + part
            start += count
        totals.append(total)
    half, rows = keep_ref.shape[2:4]

    def put(even_ref, odd_ref):
        for i, total in enumerate(totals):
            for j in range(half):
                start = 2 * j * rows
                even_ref[i, 0, j] = rounded(total[start : start + rows])
                odd_ref[i, 0, j] = rounded(total[start + rows : start + 2 * rows])

    @pl.when(odd_ref[0] == 0)
    def _():
        put(keep_ref, send_ref)

    @pl.when(odd_ref[0] != 0)
    def _():
        put(send_ref, keep_ref)


def weight_parts(odd, attended, others_in, grad_attn, grad_queries, backs, groups, experts):
    width = attended.shape[1]
    part = width // groups
    rows = part // experts
    left = lambda m: pl.BlockSpec((m.shape[0], part), lambda j: (0, j))
    whole = lambda m: pl.BlockSpec(m.shape, lambda j: (0,) * m.ndim)
    lefts, rights = [attended, others_in], [grad_attn, grad_queries, *backs]
    shape = (4, groups, experts // 2, rows, width)
    out = pl.BlockSpec((4, 1) + shape[2:], lambda j: (0, j, 0, 0, 0))
    return pl.pallas_call(
        weights_kernel,
        grid=(groups,),
        in_specs=[pl.BlockSpec(memory_space=pltpu.SMEM)]
        + [left(m) for m in lefts]
        + [whole(m) for m in rights],
        out_specs=[out, out],
        out_shape=[jax.ShapeDtypeStruct(shape, bf16)] * 2,
        compiler_params=params("arbitrary"),
        cost_estimate=cost(10e9, 30e6),
        name="weight_parts",
    )(odd, *lefts, *rights)


def resid_back_kernel(
    got_ref, spread_ref, resid_ref, gain_ref, cot_ref, wo_ref, grad_ref, attn_ref, attended_ref, sums_ref
):
    grad = matmul_tn(spread_ref[...], got_ref[...])
    _, normed, inverse = normalize(resid_ref[...], 1.0, 0.0)
    sums = jnp.concatenate(
        [jnp.sum(grad * normed, axis=0, keepdims=True), jnp.sum(grad, axis=0, keepdims=True)]
    )

    @pl.when(pl.program_id(0) == 0)
    def _():
        sums_ref[...] = sums

    @pl.when(pl.program_id(0) > 0)
    def _():
        sums_ref[...] += sums

    total = cot_ref[...].astype(f32) + norm_back(grad, gain_ref[...], normed, inverse)
    grad_ref[...] = total
    attn_ref[...] = rounded(total)
    attended_ref[...] = matmul_nt(rounded(total), wo_ref[...], bf16)


def resid_back(got, spread, residual, gain, cotangent, w_output):
    rows, width = residual.shape
    slots = got.shape[0]
    block = 256
    whole = lambda count: pl.BlockSpec((count, width), lambda j: (0, 0))
    part = pl.BlockSpec((block, width), lambda j: (j, 0))
    return pl.pallas_call(
        resid_back_kernel,
        grid=(rows // block,),
        in_specs=[
            whole(slots),
            pl.BlockSpec((slots, block), lambda j: (0, j)),
            part,
            whole(1),
            part,
            whole(width),
        ],
        out_specs=[part, part, part, whole(2)],
        out_shape=[
            jax.ShapeDtypeStruct((rows, width), f32),
            jax.ShapeDtypeStruct((rows, width), bf16),
            jax.ShapeDtypeStruct((rows, width), bf16),
            jax.ShapeDtypeStruct((2, width), f32),
        ],
        compiler_params=params("arbitrary"),
        cost_estimate=cost(2 * rows * width * (slots + width), 16 * rows * width),
        name="resid_back",
    )(got, spread, residual, gain[None], cotangent, w_output)


def input_back_kernel(
    prompt_ref, own_ref, near_ref, dq_ref, wq_ref, wk_ref, wv_ref, x_ref, gain_ref, resid_ref,
    out_ref, sums_ref, dk_ref, dv_ref,
):
    step = pl.program_id(0)
    block = dk_ref.shape[0]
    count = prompt_ref.shape[1]

    def put(first):
        for i, ref in enumerate((dk_ref, dv_ref)):
            start, size = (0, block - count) if first else (block - count, block)
            if first:
                ref[:count, :] = prompt_ref[i]
            here = pl.ds(start, size)
            ref[block - size :, :] = rounded(added(own_ref[i, here, :], near_ref[i, here, :]))

    pl.when(step == 0)(lambda: put(True))
    pl.when(step > 0)(lambda: put(False))
    grad = matmul_nt(dq_ref[...], wq_ref[...])
    grad = grad + matmul_nt(dk_ref[...], wk_ref[...])
    grad = grad + matmul_nt(dv_ref[...], wv_ref[...])
    _, normed, inverse = normalize(x_ref[...].astype(f32), 1.0, 0.0)
    sums = jnp.concatenate(
        [jnp.sum(grad * normed, axis=0, keepdims=True), jnp.sum(grad, axis=0, keepdims=True)]
    )

    @pl.when(step == 0)
    def _():
        sums_ref[...] = sums

    @pl.when(step > 0)
    def _():
        sums_ref[...] += sums

    out_ref[...] = rounded(resid_ref[...] + norm_back(grad, gain_ref[...], normed, inverse))


def input_back(prompt, own, near, grad_queries, w_query, w_key, w_value, tokens, gain, grad_resid):
    rows, width = tokens.shape
    block = rows // 2
    whole = lambda count: pl.BlockSpec((count, width), lambda j: (0, 0))
    part = pl.BlockSpec((block, width), lambda j: (j, 0))
    pair = lambda count: pl.BlockSpec((2, count, width), lambda j: (0, 0, 0))
    return pl.pallas_call(
        input_back_kernel,
        grid=(rows // block,),
        in_specs=[
            pair(PROMPT_DEV),
            pair(CONT_DEV),
            pair(CONT_DEV),
            part,
            whole(width),
            whole(width),
            whole(width),
            part,
            whole(1),
            part,
        ],
        out_specs=[part, whole(2)],
        out_shape=[
            jax.ShapeDtypeStruct((rows, width), bf16),
            jax.ShapeDtypeStruct((2, width), f32),
        ],
        scratch_shapes=[pltpu.VMEM((block, width), bf16)] * 2,
        compiler_params=params("arbitrary"),
        cost_estimate=cost(6 * rows * width * width, 20 * rows * width),
        name="input_back",
    )(prompt, own, near, grad_queries, w_query, w_key, w_value, tokens, gain[None], grad_resid)


def head_stack(block):
    first = lax.broadcasted_iota(jnp.int32, block.shape, 1) < block.shape[1] // 2
    zero = jnp.zeros_like(block)
    return jnp.concatenate([jnp.where(first, block, zero), jnp.where(first, zero, block)])


def head_merge(turned):
    half, rows = turned.shape[0] // 2, turned.shape[1] // 2
    return jnp.concatenate([turned[:half, :rows], turned[half:, rows:]]).T


def chunk_scores(chunk, keys, stack, near_bias, bias_ref, prompt_len):
    scores = matmul_nt(keys, stack)
    if chunk == 0:
        bias = bias_ref[...]
        return scores + jnp.concatenate([bias, bias], axis=1)
    tri = (PROMPT_DEV, PROMPT_DEV)
    after = lax.broadcasted_iota(jnp.int32, tri, 0) > lax.broadcasted_iota(jnp.int32, tri, 1)
    diag = jnp.where(after, f32(masked_score), f32(0.0))
    last = keys.shape[0] - PROMPT_DEV
    near_end = prompt_len + CONT_DEV
    pieces = [scores[:prompt_len], scores[prompt_len:near_end] + near_bias]
    if last > near_end:
        pieces.append(scores[near_end:last])
    pieces.append(scores[last:] + jnp.concatenate([diag, diag], axis=1))
    return jnp.concatenate(pieces)


def chunk_keys(chunk, prompt_len):
    return prompt_len if chunk == 0 else prompt_len + CONT_DEV + PROMPT_DEV * chunk


def attend_kernel(prompt_len, near_ref, q_ref, k_ref, v_ref, bias_ref, out_ref, log_ref):
    scale = bf16(1.0 / math.sqrt(q_ref.shape[1] // 2))
    chunks = q_ref.shape[0] // PROMPT_DEV

    def scores_of(chunk):
        stack = head_stack(q_ref[pl.ds(chunk * PROMPT_DEV, PROMPT_DEV), :] * scale)
        keys = k_ref[: chunk_keys(chunk, prompt_len), :]
        return chunk_scores(chunk, keys, stack, near_ref[0], bias_ref, prompt_len)

    scores = scores_of(0)
    for chunk in range(chunks):
        rows = pl.ds(chunk * PROMPT_DEV, PROMPT_DEV)
        size = chunk_keys(chunk, prompt_len)
        later = scores_of(chunk + 1) if chunk + 1 < chunks else None
        top = jnp.max(scores, axis=0, keepdims=True)
        weights = jnp.exp(scores - top)
        total = jnp.sum(weights, axis=0, keepdims=True)
        mixed = matmul_tn(v_ref[:size, :], rounded(weights)) / total
        out_ref[rows, :] = rounded(head_merge(mixed))
        log_ref[0, chunk : chunk + 1, :] = top + jnp.log(total)
        scores = later


def attend_back_kernel(
    prompt_len,
    near_ref,
    q_ref,
    k_ref,
    v_ref,
    bias_ref,
    log_ref,
    out_ref,
    grad_ref,
    dq_ref,
    first_ref,
    second_ref,
    near_out_ref,
    own_ref,
    dk_ref,
    dv_ref,
):
    scale = 1.0 / math.sqrt(q_ref.shape[1] // 2)
    half = q_ref.shape[1] // 2
    dk_ref[...] = jnp.zeros_like(dk_ref)
    dv_ref[...] = jnp.zeros_like(dv_ref)
    for chunk in range(q_ref.shape[0] // PROMPT_DEV):
        rows = pl.ds(chunk * PROMPT_DEV, PROMPT_DEV)
        size = chunk_keys(chunk, prompt_len)
        stack = head_stack(q_ref[rows, :] * bf16(scale))
        grad = grad_ref[rows, :]
        grad_stack = head_stack(grad)
        product = (grad.astype(f32) * out_ref[rows, :].astype(f32)).T
        inner = jnp.concatenate(
            [
                jnp.sum(product[:half], axis=0, keepdims=True),
                jnp.sum(product[half:], axis=0, keepdims=True),
            ],
            axis=1,
        )
        keys = k_ref[:size, :]
        scores = chunk_scores(chunk, keys, stack, near_ref[0], bias_ref, prompt_len)
        weights = jnp.exp(scores - log_ref[0, chunk : chunk + 1, :])
        dv_ref[:size, :] += matmul(rounded(weights), grad_stack)
        grad_prob = matmul_nt(v_ref[:size, :], grad_stack)
        grad_score = rounded(weights * (grad_prob - inner))
        dk_ref[:size, :] += matmul(grad_score, stack)
        dq_ref[rows, :] = rounded(head_merge(matmul_tn(keys, grad_score)) * scale)
    start = 0
    for ref in (first_ref, second_ref, near_out_ref, own_ref):
        count = ref.shape[1]
        ref[0] = rounded(dk_ref[start : start + count, :])
        ref[1] = rounded(dv_ref[start : start + count, :])
        start += count


def attend(near_bias, queries, keys, values, bias):
    rows, width = queries.shape
    size = keys.shape[0]
    prompt_len = bias.shape[0]
    lanes = 2 * width // HEADS
    pairs = HEADS // 2
    chunks = rows // PROMPT_DEV
    block = lambda count: pl.BlockSpec((count, lanes), lambda j: (0, j))
    return pl.pallas_call(
        functools.partial(attend_kernel, prompt_len),
        grid=(pairs,),
        in_specs=[
            pl.BlockSpec(memory_space=pltpu.SMEM),
            block(rows),
            block(size),
            block(size),
            pl.BlockSpec((prompt_len, PROMPT_DEV), lambda j: (0, 0)),
        ],
        out_specs=[
            block(rows),
            pl.BlockSpec((1, chunks, 2 * PROMPT_DEV), lambda j: (j, 0, 0)),
        ],
        out_shape=[
            jax.ShapeDtypeStruct((rows, width), bf16),
            jax.ShapeDtypeStruct((pairs, chunks, 2 * PROMPT_DEV), f32),
        ],
        compiler_params=params("arbitrary"),
        cost_estimate=cost(16 * rows * size * width, 4 * (rows + size) * width, rows * size * HEADS),
        name="attend",
    )(near_bias, queries, keys, values, bias)


def attend_back(near_bias, queries, keys, values, bias, log_total, attended, grad):
    rows, width = queries.shape
    size = keys.shape[0]
    prompt_len = bias.shape[0]
    lanes = 2 * width // HEADS
    pairs = HEADS // 2
    chunks = rows // PROMPT_DEV
    block = lambda count: pl.BlockSpec((count, lanes), lambda j: (0, j))
    counts = (prompt_len // 2, prompt_len // 2, CONT_DEV, CONT_DEV)
    return pl.pallas_call(
        functools.partial(attend_back_kernel, prompt_len),
        grid=(pairs,),
        in_specs=[
            pl.BlockSpec(memory_space=pltpu.SMEM),
            block(rows),
            block(size),
            block(size),
            pl.BlockSpec((prompt_len, PROMPT_DEV), lambda j: (0, 0)),
            pl.BlockSpec((1, chunks, 2 * PROMPT_DEV), lambda j: (j, 0, 0)),
            block(rows),
            block(rows),
        ],
        out_specs=[block(rows)]
        + [pl.BlockSpec((2, count, lanes), lambda j: (0, 0, j)) for count in counts],
        out_shape=[jax.ShapeDtypeStruct((rows, width), bf16)]
        + [jax.ShapeDtypeStruct((2, count, width), bf16) for count in counts],
        scratch_shapes=[pltpu.VMEM((size, lanes), f32), pltpu.VMEM((size, lanes), f32)],
        compiler_params=params("arbitrary"),
        cost_estimate=cost(40 * rows * size * width, 8 * (rows + size) * width, rows * size * HEADS),
        name="attend_back",
    )(near_bias, queries, keys, values, bias, log_total, attended, grad)


def local(
    tokens_in,
    cotangent,
    hash_ids,
    norm1_gain,
    norm1_bias,
    w_query,
    w_key,
    w_value,
    w_output,
    norm2_gain,
    norm2_bias,
    expert_in,
    expert_out,
):
    row_count, width = tokens_in.shape
    experts = lax.axis_size("expert")
    groups = lax.axis_size("group")
    position = lax.axis_index("expert")
    group = lax.axis_index("group")
    capacity = 2 * row_count // experts
    slots = experts * capacity
    tied = lax.optimization_barrier

    def all_exchanged(values):
        return lax.all_to_all(values, "expert", split_axis=0, concat_axis=0, tiled=True)

    def exchanged(values):
        got = all_exchanged(values.reshape(experts, capacity, width))
        return got.reshape(slots, width)

    near_tokens = lax.ppermute(
        tokens_in[PROMPT_DEV:], "expert", [(i, i + 1) for i in range(0, experts, 2)]
    )
    prompts, prompt_ids, near_tokens, last_tokens = gather_relative(
        tokens_in[:PROMPT_DEV], "expert", near_tokens
    )
    ids = jnp.broadcast_to(rounded(hash_ids), (row_count, 128))
    all_cot = lax.all_gather(jnp.concatenate([cotangent, ids], axis=1), "group")

    row_index = jnp.arange(row_count, dtype=jnp.int32)
    lower = rounded(row_index[:, None] >= row_index[None, :])

    routed = rounded(hash_ids == jnp.arange(experts, dtype=jnp.int32)[None, :])
    running = matmul(lower, routed)
    rank = (jnp.sum(running * routed.astype(f32), axis=-1) - 1.0).astype(jnp.int32)
    slot = hash_ids[:, 0] * capacity + rank
    spread = rounded(slot[None, :] == jnp.arange(slots, dtype=jnp.int32)[:, None])

    cot_sent, _ = tied((matmul(spread, cotangent, bf16), last_tokens))
    cot = {0: exchanged(cot_sent)}
    others_in, queries, keys, values = project(
        prompts + [near_tokens, tokens_in[PROMPT_DEV:]],
        norm1_gain,
        norm1_bias,
        w_query,
        w_key,
        w_value,
    )
    block_pos = jnp.stack([(position ^ r) * PROMPT_DEV for r in prompt_ids])
    prompt_pos = jnp.arange(PROMPT_DEV, dtype=jnp.int32)
    key_pos = (block_pos[:, None] + prompt_pos[None, :]).reshape(-1)
    query_pos = position * PROMPT_DEV + row_index[:PROMPT_DEV]
    bias = jnp.where(key_pos[:, None] <= query_pos[None, :], f32(0.0), f32(masked_score))
    near_bias = jnp.where(position % 2 == 1, f32(0.0), f32(masked_score))[None]
    attended, log_total = attend(near_bias, queries, keys, values, bias)

    residual = tokens_in.astype(f32) + matmul(attended, w_output)
    ffn_in = rounded(normalize(residual, norm2_gain, norm2_bias)[0])
    rows = exchanged(matmul(spread, ffn_in, bf16))
    all_numbers = all_cot[:, :, width].astype(jnp.int32)[:, None]
    numbers = lambda masks: jnp.stack([group ^ mask for mask in masks])
    near_sent = spread_rows(numbers([1]), all_numbers, all_cot, experts)
    grad_hidden = expert_back(cot[0], expert_out)
    rows, grad_hidden, near_sent = tied((rows, grad_hidden, near_sent))
    all_rows = lax.all_gather(rows, "group")
    cot[1] = all_exchanged(near_sent)
    hidden, grad_pre, grad_rows = expert_front(rows, grad_hidden, expert_in)
    grad_rows, hidden, cot[1] = tied((grad_rows, hidden, cot[1]))
    grad_got = exchanged(grad_rows)
    produced = expert_produce(hidden, expert_out)
    far_sent = spread_rows(numbers(range(2, groups)), all_numbers, all_cot, experts, produced)
    far_sent, grad_got = tied((far_sent, grad_got))
    far_got = all_exchanged(far_sent)

    grad_resid, grad_attn, grad_attended, sums2 = resid_back(
        grad_got, spread, residual, norm2_gain, cotangent, w_output
    )
    grad_queries, back_first, back_second, back_near, back_own = attend_back(
        near_bias, queries, keys, values, bias, log_total, attended, grad_attended
    )
    backs = (back_first, back_second, back_near, back_own, grad_queries)
    prompt_sums = scatter_relative(back_first, back_second, "expert")
    prompt_sent = next(prompt_sums)
    near_back = lax.ppermute(
        back_near, "expert", [(i + 1, i) for i in range(0, experts, 2)]
    )
    weights = weight_parts(
        (position & 1)[None],
        attended,
        others_in,
        grad_attn,
        grad_queries,
        (back_first, back_second, back_near, back_own),
        groups,
        experts,
    )
    weights, prompt_sent, near_back, far_got = tied((weights, prompt_sent, near_back, far_got))
    marks = []
    weight_sums = weight_chain(*weights, marks)
    weight_sent = next(weight_sums)
    prompt_sent, prompt_back = moved_on(prompt_sums, prompt_sent)
    result_got = far_got[:, 0].reshape(slots, width)
    result = rounded(residual + matmul_tn(spread, result_got))
    weight_sent, prompt_sent, result = tied((weight_sent, prompt_sent, result))
    weight_sent, _ = moved_on(weight_sums, weight_sent)
    prompt_sent, prompt_back = moved_on(prompt_sums, prompt_sent)
    number, _ = tied((numbers(range(groups)), marks[-1]))
    operands = (expert_in, expert_out, (rows, grad_pre), all_rows, cot[1], far_got)
    in_first, *hidden_first = in_sums(number, 0, *operands)
    over_group = lambda values: lax.all_to_all(
        values, "group", split_axis=0, concat_axis=0, tiled=True
    )
    weight_sent, in_first = tied((weight_sent, in_first))
    got_first = over_group(in_first)
    weight_sent, _ = moved_on(weight_sums, weight_sent)
    number, _ = tied((number, marks[-1]))
    in_second, *hidden_second = in_sums(number, 1, *operands)
    got_first, in_second, prompt_sent, weight_sent = tied(
        (got_first, in_second, prompt_sent, weight_sent)
    )
    got_second = over_group(in_second)
    prompt_sent, weight_sent, number, _ = tied((prompt_sent, weight_sent, number, in_second))
    while prompt_sent is not None:
        prompt_sent, prompt_back = moved_on(prompt_sums, prompt_sent)
    grad_tokens, sums1 = input_back(
        prompt_back,
        back_own,
        near_back,
        grad_queries,
        w_query,
        w_key,
        w_value,
        tokens_in,
        norm1_gain,
        grad_resid,
    )
    weight_sent, number, sums1 = tied((weight_sent, number, sums1))
    weight_sent, weight_grads = moved_on(weight_sums, weight_sent)
    grad_expert_out = out_sums(
        number, (hidden, cot[0]), cot[1], far_got, hidden_first + hidden_second
    )
    vectors = jnp.concatenate([sums1, sums2])
    vectors, got_second, grad_expert_out, weight_sent = tied(
        (vectors, got_second, grad_expert_out, weight_sent)
    )
    vectors = vector_sums(vectors)
    while weight_sent is not None:
        weight_sent, weight_grads = moved_on(weight_sums, weight_sent)
    grad_expert_in = lay_out([got_first, got_second])
    grad_w_output, grad_w_query, grad_w_key, grad_w_value = weight_grads
    return (
        result,
        grad_tokens,
        vectors[0],
        vectors[1],
        grad_w_query,
        grad_w_key,
        grad_w_value,
        grad_w_output,
        vectors[2],
        vectors[3],
        grad_expert_in,
        grad_expert_out,
    )


def solution(mesh):
    both = ("group", "expert")
    return jax.shard_map(
        local,
        mesh=mesh,
        in_specs=(
            P(both, None),
            P(both, None),
            P(both, None),
            P(),
            P(),
            P(),
            P(),
            P(),
            P(),
            P(),
            P(),
            P("expert", None, None),
            P("expert", None, None),
        ),
        out_specs=(
            P(both, None),
            P(both, None),
            P(both),
            P(both),
            P(both, None),
            P(both, None),
            P(both, None),
            P(both, None),
            P(both),
            P(both),
            P("expert", "group", None),
            P("expert", "group", None),
        ),
        check_vma=False,
    )
```

```python
import functools
import math

import jax
import jax.numpy as jnp
from jax import lax
from jax.experimental import pallas as pl
from jax.experimental.pallas import tpu as pltpu
from jax.sharding import PartitionSpec as P

HEADS = 16
PROMPT_DEV = 128
CONT_DEV = 384


norm_eps = 1e-05
masked_score = -1e30
bf16 = jnp.bfloat16
f32 = jnp.float32
MIB = 1 << 20
share = 0.05


def swapped(block, axis, mask):
    return lax.ppermute(block, axis, [(i, i ^ mask) for i in range(lax.axis_size(axis))])


def rounded(values):
    return values.astype(bf16)


def normalize(values, gain, shift):
    average = jnp.mean(values, axis=-1, keepdims=True)
    centered = values - average
    variance = jnp.mean(centered * centered, axis=-1, keepdims=True)
    inverse = lax.rsqrt(variance + norm_eps)
    normed = centered * inverse
    return (normed * gain + shift, normed, inverse)


def norm_back(grad_out, gain, normed, inverse):
    scaled = grad_out * gain
    first_mean = jnp.mean(scaled, axis=-1, keepdims=True)
    second = jnp.mean(scaled * normed, axis=-1, keepdims=True)
    return inverse * (scaled - first_mean - normed * second)


def matmul(a, b, kind=f32):
    return jnp.dot(a, b, preferred_element_type=f32).astype(kind)


def matmul_nt(a, b, kind=f32):
    return lax.dot_general(a, b, (((1,), (1,)), ((), ())), preferred_element_type=f32).astype(kind)


def matmul_tn(a, b, kind=f32):
    return lax.dot_general(a, b, (((0,), (0,)), ((), ())), preferred_element_type=f32).astype(kind)


def outer_bits(size):
    return range(size.bit_length() - 2, 0, -1)


def gather_relative(block, axis, more):
    size = lax.axis_size(axis)
    pieces = {0: block}
    ready, last = [0], []
    while ready:
        fresh = {}
        for r in ready:
            for bit in outer_bits(size):
                if r ^ (1 << bit) not in pieces and r ^ (1 << bit) not in fresh:
                    fresh[r ^ (1 << bit)] = swapped(pieces[r], axis, 1 << bit)
        fresh, more = lax.optimization_barrier((fresh, more))
        pieces.update(fresh)
        ready, last = list(fresh), list(fresh.values()) or last
    near = sorted(pieces)
    for r in near:
        pieces[r ^ 1] = swapped(pieces[r], axis, 1)
    order = near + [r ^ 1 for r in near]
    return [pieces[r] for r in order], order, more, last


def scatter_relative(near, far, axis):
    size = lax.axis_size(axis)
    got = yield swapped(far, axis, 1)
    both = added(near, got)
    count = size // 2
    rows = both.shape[1] // count
    pieces = {2 * i: rounded(both[:, i * rows : (i + 1) * rows]) for i in range(count)}
    bits = list(outer_bits(size))
    for level in range(len(bits), 0, -1):
        sent, spans = [], []
        for r in [r for r in sorted(pieces) if bin(r).count("1") == level]:
            ways = [bit for bit in bits if r >> bit & 1]
            if rows % (16 * len(ways)):
                ways = ways[:1]
            part = rows // len(ways)
            piece = pieces.pop(r)
            for i, bit in enumerate(ways):
                span = (i * part, (i + 1) * part)
                sent.append(swapped(piece[:, span[0] : span[1]], axis, 1 << bit))
                spans.append((r ^ (1 << bit), span))
        gots = yield sent
        for r in sorted(pieces):
            total = pieces[r].astype(f32)
            for got, (target, span) in zip(gots, spans):
                if target == r:
                    outside = ((0, 0), (span[0], rows - span[1]), (0, 0))
                    total = total + jnp.pad(got.astype(f32), outside)
            pieces[r] = rounded(total)
    return pieces[0]


def halved(blocks, place, axis, bit):
    own = (lax.axis_index(axis) >> bit) & 1
    return (
        lax.dynamic_index_in_dim(blocks, own, place, keepdims=False),
        lax.dynamic_index_in_dim(blocks, 1 - own, place, keepdims=False),
    )


def added(keep, got):
    return keep.astype(f32) + got.astype(f32)


def places_of(bits, bit, value):
    rest = [other for other in bits if other != bit]
    weight = {other: 1 << (len(bits) - 1 - i) for i, other in enumerate(bits)}
    places = []
    for number in range(1 << len(rest)):
        place = value * weight[bit]
        for i, other in enumerate(rest):
            place = place + (number >> (len(rest) - 1 - i) & 1) * weight[other]
        places.append(place)
    return places


def halve_kernel(lefts, bits, own_ref, *refs):
    sets = len(lefts)
    for k, (left, bit) in enumerate(zip(lefts, bits)):
        keep_ref, got_ref = refs[2 * k : 2 * k + 2]
        outs = refs[2 * sets + 2 * k : 2 * sets + 2 * k + 2]
        own = (own_ref[0] >> bit) & 1
        for ref, value in zip(outs, (own, 1 - own)):
            for i, place in enumerate(places_of(left, bit, value)):
                for j in range(ref.shape[1]):
                    ref[0, j, i] = rounded(added(keep_ref[0, j, place], got_ref[0, j, place]))


def halve(number, states, bits):
    _, groups, count, rows, width = states[0][0].shape
    shape = (2, groups, count // 2, rows, width)
    came = lambda first: pl.BlockSpec(
        (1, groups, count, rows, width), lambda i: (first + i if first else i, 0, 0, 0, 0)
    )
    out = pl.BlockSpec((1, groups, count // 2, rows, width), lambda i: (i, 0, 0, 0, 0))
    size = 2 * math.prod(shape)
    outs = pl.pallas_call(
        functools.partial(halve_kernel, [state[3] for state in states], bits),
        grid=(2,),
        in_specs=[pl.BlockSpec(memory_space=pltpu.SMEM)]
        + [came(state[2]) for state in states for _ in range(2)],
        out_specs=[out] * (2 * len(states)),
        out_shape=[jax.ShapeDtypeStruct(shape, bf16)] * (2 * len(states)),
        compiler_params=params("arbitrary"),
        cost_estimate=cost(2 * size, 12 * size),
        name="halve",
    )(number, *[value for state in states for value in state[:2]])
    return list(zip(outs[::2], outs[1::2]))


def turn_kernel(own_ref, *refs):
    (*sets, own_out_ref, send_ref) = refs
    own = own_ref[0] & 1
    start = 0
    for keep_ref, got_ref in zip(sets[::2], sets[1::2]):
        for i in range(keep_ref.shape[0]):
            for j in range(keep_ref.shape[1] // 2):
                for ref, value in ((own_out_ref, own), (send_ref, 1 - own)):
                    place = 2 * j + value
                    ref[start + i, j] = rounded(added(keep_ref[i, place, 0], got_ref[i, place, 0]))
        start += keep_ref.shape[0]


def turn(number, sets):
    _, groups, _, rows, width = sets[0].shape
    shape = (4, groups // 2, rows, width)
    return pl.pallas_call(
        turn_kernel,
        in_specs=[pl.BlockSpec(memory_space=pltpu.SMEM)]
        + [pl.BlockSpec(memory_space=pltpu.VMEM)] * len(sets),
        out_specs=[pl.BlockSpec(memory_space=pltpu.VMEM)] * 2,
        out_shape=[jax.ShapeDtypeStruct(shape, bf16)] * 2,
        compiler_params=params(),
        cost_estimate=cost(8 * sets[0].size, 8 * sets[0].size),
        name="turn",
    )(number, *sets)


def weight_chain(keep, send, marks):
    bits = list(range(1, lax.axis_size("expert").bit_length() - 1))
    number = lax.axis_index("expert")[None]
    got = yield swapped(send, "expert", 1)
    states = [(keep, got, 0, bits[::-1]), (keep, got, 2, bits[::-1])]
    for pair in zip(bits, bits[::-1]):
        halves = halve(number, states, pair)
        marks.append(halves[0][0])
        gots = yield [swapped(send, "expert", 1 << bit) for bit, (_, send) in zip(pair, halves)]
        states = [
            (keep, got, 0, [other for other in state[3] if other != bit])
            for state, bit, (keep, _), got in zip(states, pair, halves, gots)
        ]
    keep, send = turn(
        lax.axis_index("group")[None], [value for state in states for value in state[:2]]
    )
    marks.append(keep)
    got = yield swapped(send, "group", 1)
    both = added(keep, got)
    bits = list(range(1, lax.axis_size("group").bit_length() - 1))
    both = both.reshape((4,) + (2,) * len(bits) + both.shape[-2:])
    left = bits[::-1]
    for bit in bits:
        keep, send = halved(rounded(both), 1 + left.index(bit), "group", bit)
        left.remove(bit)
        got = yield swapped(send, "group", 1 << bit)
        both = added(keep, got)
    return [both[i] for i in range(both.shape[0])]


def moved_on(chain, came):
    try:
        return chain.send(came), None
    except StopIteration as stop:
        return None, stop.value


def vector_sums(vectors):
    axes = ("group", "expert")
    devices = lax.axis_size("group") * lax.axis_size("expert")
    count, width = vectors.shape
    pieces = vectors.reshape(count, devices, width // devices).swapaxes(0, 1)
    got = lax.all_to_all(pieces, axes, split_axis=0, concat_axis=0, tiled=True)
    return jnp.sum(got, axis=0)


def params(*semantics):
    return pltpu.CompilerParams(dimension_semantics=semantics, vmem_limit_bytes=60 * MIB)


def cost(flops, total_bytes, exps=0):
    return pl.CostEstimate(
        flops=int(flops * share), bytes_accessed=int(total_bytes * share), transcendentals=int(exps * share)
    )


def logistic(values):
    return 0.5 * jnp.tanh(0.5 * values) + 0.5


def back_kernel(cot_ref, wout_ref, out_ref):
    out_ref[...] = matmul_nt(cot_ref[...], wout_ref[0], bf16)


def expert_back(cot, expert_out):
    count, width = cot.shape
    ff = expert_out.shape[1]
    block = 1024
    return pl.pallas_call(
        back_kernel,
        grid=(ff // block,),
        in_specs=[
            pl.BlockSpec((count, width), lambda j: (0, 0)),
            pl.BlockSpec((1, block, width), lambda j: (0, j, 0)),
        ],
        out_specs=pl.BlockSpec((count, block), lambda j: (0, j)),
        out_shape=jax.ShapeDtypeStruct((count, ff), bf16),
        compiler_params=params("arbitrary"),
        cost_estimate=cost(2 * count * width * ff, 2 * count * ff + 2 * width * ff),
        name="expert_back",
    )(cot, expert_out)


def front_kernel(parts, rows_ref, gh_ref, win_ref, hidden_ref, pre_ref, out_ref, acc_ref):
    step = pl.program_id(0)
    count = rows_ref.shape[0] // parts

    @pl.when(step == 0)
    def _():
        acc_ref[...] = jnp.zeros_like(acc_ref)

    first = lambda i: matmul(rows_ref[i * count : (i + 1) * count, :], win_ref[0])
    pre = first(0)
    for i in range(parts):
        later = first(i + 1) if i + 1 < parts else None
        here = pl.ds(i * count, count)
        sig = logistic(pre)
        hidden = pre * sig
        hidden_ref[here, :] = rounded(hidden)
        grad_pre = rounded(gh_ref[here, :].astype(f32) * sig * (1.0 + pre - hidden))
        pre_ref[here, :] = grad_pre
        acc_ref[here, :] += matmul_nt(grad_pre, win_ref[0])
        pre = later

    @pl.when(step == pl.num_programs(0) - 1)
    def _():
        out_ref[...] = rounded(acc_ref[...])


def expert_front(rows, grad_hidden, expert_in):
    count, width = rows.shape
    ff = expert_in.shape[2]
    block = 1024
    whole = pl.BlockSpec((count, width), lambda j: (0, 0))
    part = pl.BlockSpec((count, block), lambda j: (0, j))
    return pl.pallas_call(
        functools.partial(front_kernel, 4),
        grid=(ff // block,),
        in_specs=[whole, part, pl.BlockSpec((1, width, block), lambda j: (0, 0, j))],
        out_specs=[part, part, whole],
        out_shape=[
            jax.ShapeDtypeStruct((count, ff), bf16),
            jax.ShapeDtypeStruct((count, ff), bf16),
            jax.ShapeDtypeStruct((count, width), bf16),
        ],
        scratch_shapes=[pltpu.VMEM((count, width), f32)],
        compiler_params=params("arbitrary"),
        cost_estimate=cost(4 * count * width * ff, 6 * count * ff + 2 * width * ff, count * ff),
        name="expert_front",
    )(rows, grad_hidden, expert_in)


def produce_kernel(hidden_ref, wout_ref, out_ref, acc_ref):
    step = pl.program_id(0)
    part = matmul(hidden_ref[...], wout_ref[0])

    @pl.when(step == 0)
    def _():
        acc_ref[...] = part

    @pl.when(step > 0)
    def _():
        acc_ref[...] += part

    @pl.when(step == pl.num_programs(0) - 1)
    def _():
        out_ref[...] = rounded(acc_ref[...])


def expert_produce(hidden, expert_out):
    count, ff = hidden.shape
    width = expert_out.shape[2]
    block = 1024
    return pl.pallas_call(
        produce_kernel,
        grid=(ff // block,),
        in_specs=[
            pl.BlockSpec((count, block), lambda j: (0, j)),
            pl.BlockSpec((1, block, width), lambda j: (0, j, 0)),
        ],
        out_specs=pl.BlockSpec((count, width), lambda j: (0, 0)),
        out_shape=jax.ShapeDtypeStruct((count, width), bf16),
        scratch_shapes=[pltpu.VMEM((count, width), f32)],
        compiler_params=params("arbitrary"),
        cost_estimate=cost(2 * count * width * ff, 2 * count * ff + 2 * width * ff),
        name="expert_produce",
    )(hidden, expert_out)


def in_kernel(
    half, number_ref, own_rows_ref, own_pre_ref, win_hbm, wout_hbm, rows_hbm, near_hbm, far_hbm,
    in_ref, near_out, far_out, in_sum, win_ref, wout_ref, rows_ref, cot_ref, hidden_ref,
    weight_sems, shard_sems, out_sems,
):
    shards, count, _ = rows_ref.shape
    block = win_ref.shape[1]
    place = pl.multiple_of((2 * number_ref[0] + half) * block, block)
    weights = [
        pltpu.make_async_copy(win_hbm.at[0, :, pl.ds(place, block)], win_ref, weight_sems.at[0]),
        pltpu.make_async_copy(wout_hbm.at[0, pl.ds(place, block), :], wout_ref, weight_sems.at[1]),
    ]
    copies, outs = [], []
    for i in range(shards):
        cot = near_hbm.at[:, 0] if i == 0 else far_hbm.at[:, i]
        rows = rows_hbm.at[number_ref[1 + i]]
        copies.append(
            [
                pltpu.make_async_copy(rows, rows_ref.at[i], shard_sems.at[i, 0]),
                pltpu.make_async_copy(cot, cot_ref.at[i], shard_sems.at[i, 1]),
            ]
        )
        out = near_out if i == 0 else far_out.at[i - 1]
        outs.append(pltpu.make_async_copy(hidden_ref.at[i], out, out_sems.at[i]))
    for copy in weights + [copy for pair in copies for copy in pair]:
        copy.start()
    in_sum[...] = matmul_tn(own_rows_ref[...], own_pre_ref[...])
    for copy in weights:
        copy.wait()
    for i in range(shards):
        for copy in copies[i]:
            copy.wait()
        rows = rows_ref[i]
        pre = matmul(rows, win_ref[...])
        grad_hidden = matmul_nt(cot_ref[i].reshape(rows.shape), wout_ref[...])
        sig = logistic(pre)
        hidden = pre * sig
        hidden_ref[i] = rounded(hidden)
        outs[i].start()
        grad_pre = rounded(grad_hidden * sig * (1.0 + pre - hidden))
        in_sum[...] += matmul_tn(rows, grad_pre)
    in_ref[...] = rounded(in_sum[...]).reshape(in_ref.shape)
    for copy in outs:
        copy.wait()


def in_sums(number, half, expert_in, expert_out, own, rows, near, far):
    groups, count, width = rows.shape
    sources, _, slots, _ = near.shape
    part = expert_in.shape[2] // groups
    block = part // 2
    shards = groups - 1
    there = pl.BlockSpec(memory_space=pl.ANY)
    return pl.pallas_call(
        functools.partial(in_kernel, half),
        grid_spec=pltpu.PrefetchScalarGridSpec(
            num_scalar_prefetch=1,
            grid=(1,),
            in_specs=[
                pl.BlockSpec((count, width), lambda j, w: (0, 0)),
                pl.BlockSpec((count, block), lambda j, w: (0, 2 * w[0] + half)),
            ]
            + [there] * 5,
            out_specs=[
                pl.BlockSpec((groups, width // groups, block), lambda j, w: (0, 0, 0)),
                there,
                there,
            ],
            scratch_shapes=[
                pltpu.VMEM((width, block), f32),
                pltpu.VMEM((width, block), bf16),
                pltpu.VMEM((block, width), bf16),
                pltpu.VMEM((shards, count, width), bf16),
                pltpu.VMEM((shards, sources, slots, width), bf16),
                pltpu.VMEM((shards, count, block), bf16),
                pltpu.SemaphoreType.DMA((2,)),
                pltpu.SemaphoreType.DMA((shards, 2)),
                pltpu.SemaphoreType.DMA((shards,)),
            ],
        ),
        out_shape=[
            jax.ShapeDtypeStruct((groups, width // groups, block), bf16),
            jax.ShapeDtypeStruct((count, block), bf16),
            jax.ShapeDtypeStruct((groups - 2, count, block), bf16),
        ],
        compiler_params=params("arbitrary"),
        cost_estimate=cost(6 * count * width * block * groups, 16e6, count * block * groups),
        name="in_sums",
    )(number, *own, expert_in, expert_out, rows, near, far)


def own_kernel(_, hidden_ref, cot_ref, out_ref):
    out_ref[...] = matmul_tn(hidden_ref[...], cot_ref[...])


def own_out(number, groups, hidden, cot):
    count, width = cot.shape
    part = hidden.shape[1] // groups
    block = part // 2
    return pl.pallas_call(
        own_kernel,
        grid_spec=pltpu.PrefetchScalarGridSpec(
            num_scalar_prefetch=1,
            grid=(2,),
            in_specs=[
                pl.BlockSpec((count, block), lambda j, w: (0, 2 * w[0] + j)),
                pl.BlockSpec((count, width), lambda j, w: (0, 0)),
            ],
            out_specs=pl.BlockSpec((block, width), lambda j, w: (j, 0)),
        ),
        out_shape=jax.ShapeDtypeStruct((part, width), f32),
        compiler_params=params("arbitrary"),
        cost_estimate=cost(2 * count * width * part, 8e6),
        name="own_out",
    )(number, hidden, cot)


def out_kernel(own_ref, near_ref, far_ref, *refs):
    out_ref, total = refs[-2:]
    hiddens = refs[:-2]
    block = total.shape[0] // 2
    count = hiddens[0].shape[0]
    step = pl.program_id(0)

    @pl.when(step == 0)
    def _():
        near = near_ref[...].reshape(count, -1)
        for half in range(2):
            here = pl.ds(half * block, block)
            total[here, :] = own_ref[here, :] + matmul_tn(hiddens[2 * half][...], near)

    far = far_ref[...].reshape(count, -1)
    for half in range(2):
        here = pl.ds(half * block, block)
        total[here, :] += matmul_tn(hiddens[2 * half + 1][0], far)

    @pl.when(step == pl.num_programs(0) - 1)
    def _():
        out_ref[0] = total[...]


def out_sums(own, near, far, hiddens):
    part, width = own.shape
    count = hiddens[0].shape[0]
    sources, _, slots, _ = near.shape
    steps = hiddens[1].shape[0]
    near_hidden = pl.BlockSpec((count, part // 2), lambda j: (0, 0))
    far_hidden = pl.BlockSpec((1, count, part // 2), lambda j: (j, 0, 0))
    return pl.pallas_call(
        out_kernel,
        grid=(steps,),
        in_specs=[
            pl.BlockSpec((part, width), lambda j: (0, 0)),
            pl.BlockSpec((sources, 1, slots, width), lambda j: (0, 0, 0, 0)),
            pl.BlockSpec((sources, 1, slots, width), lambda j: (0, 1 + j, 0, 0)),
        ]
        + [near_hidden, far_hidden] * 2,
        out_specs=pl.BlockSpec((1, part, width), lambda j: (0, 0, 0)),
        out_shape=jax.ShapeDtypeStruct((1, part, width), f32),
        scratch_shapes=[pltpu.VMEM((part, width), f32)],
        compiler_params=params("arbitrary"),
        cost_estimate=cost(2 * count * width * part * (steps + 1), 16e6),
        name="out_sums",
    )(own, near, far, *hiddens)


def lay_kernel(*refs):
    gots, out_ref = refs[:-1], refs[-1]
    block = gots[0].shape[2]
    for i in range(gots[0].shape[0]):
        for j, ref in enumerate(gots):
            start = (i * len(gots) + j) * block
            out_ref[0, :, start : start + block] = ref[i].astype(f32)


def lay_out(gots):
    groups, rows, block = gots[0].shape
    tall = 64
    width = groups * block * len(gots)
    return pl.pallas_call(
        lay_kernel,
        grid=(rows // tall,),
        in_specs=[pl.BlockSpec((groups, tall, block), lambda j: (0, j, 0))] * len(gots),
        out_specs=pl.BlockSpec((1, tall, width), lambda j: (0, j, 0)),
        out_shape=jax.ShapeDtypeStruct((1, rows, width), f32),
        compiler_params=params("arbitrary"),
        cost_estimate=cost(rows * width, 6 * rows * width),
        name="lay_out",
    )(*gots)


def spread_kernel(first, _, ids_ref, values_ref, *refs):
    out_ref = refs[-1]
    experts, _, capacity, width = out_ref.shape

    def spread():
        rows = ids_ref.shape[2]
        ids = ids_ref[0]
        number = lax.broadcasted_iota(jnp.int32, (experts, rows), 0)
        routed = jnp.where(number == ids, f32(1.0), f32(0.0))
        square = (rows, rows)
        before = lax.broadcasted_iota(jnp.int32, square, 0) <= lax.broadcasted_iota(
            jnp.int32, square, 1
        )
        running = matmul(rounded(routed), rounded(jnp.where(before, f32(1.0), f32(0.0))))
        rank = jnp.sum(running * routed, axis=0, keepdims=True).astype(jnp.int32) - 1
        slot = ids * capacity + rank
        places = lax.broadcasted_iota(jnp.int32, (experts * capacity, rows), 0)
        onehot = rounded(jnp.where(places == slot, f32(1.0), f32(0.0)))
        out = matmul(onehot, values_ref[0, :, :width], bf16)
        out_ref[...] = out.reshape(out_ref.shape)

    if first:
        step = pl.program_id(0)

        @pl.when(step == 0)
        def _():
            out_ref[...] = refs[0][...].reshape(out_ref.shape)

        pl.when(step > 0)(spread)
    else:
        spread()


def spread_rows(numbers, ids, values, experts, first=None):
    _, rows, columns = values.shape
    width = columns - 128
    capacity = 2 * rows // experts
    start = 0 if first is None else 1
    count = numbers.shape[0] + start
    which = lambda j, w: w[jnp.maximum(j - start, 0)]
    specs = [
        pl.BlockSpec((1, 1, rows), lambda j, w: (which(j, w), 0, 0)),
        pl.BlockSpec((1, rows, columns), lambda j, w: (which(j, w), 0, 0)),
    ]
    operands = [ids, values]
    if start:
        specs.append(pl.BlockSpec(first.shape, lambda j, w: (0, 0)))
        operands.append(first)
    return pl.pallas_call(
        functools.partial(spread_kernel, start),
        grid_spec=pltpu.PrefetchScalarGridSpec(
            num_scalar_prefetch=1,
            grid=(count,),
            in_specs=specs,
            out_specs=pl.BlockSpec((experts, 1, capacity, width), lambda j, w: (0, j, 0, 0)),
        ),
        out_shape=jax.ShapeDtypeStruct((experts, count, capacity, width), bf16),
        compiler_params=params("arbitrary"),
        cost_estimate=cost(2 * count * experts * capacity * rows * width, 8e6),
        name="spread_rows",
    )(numbers, *operands)


def project_kernel(count, gain_ref, bias_ref, wq_ref, wk_ref, wv_ref, *refs):
    pieces, (in_ref, q_ref, k_ref, v_ref, scratch) = refs[:count], refs[count:]

    @pl.when(pl.program_id(0) == 0)
    def _():
        start = 0
        for ref in pieces:
            end = start + ref.shape[0]
            values = normalize(ref[...].astype(f32), gain_ref[...], bias_ref[...])[0]
            scratch[start:end, :] = rounded(values)
            start = end
        in_ref[...] = scratch[...]

    first, last = pieces[0].shape[0], pieces[-1].shape[0]
    size = scratch.shape[0]
    q_ref[:first, :] = matmul(scratch[:first, :], wq_ref[...], bf16)
    q_ref[first:, :] = matmul(scratch[size - last :, :], wq_ref[...], bf16)
    k_ref[...] = matmul(scratch[...], wk_ref[...], bf16)
    v_ref[...] = matmul(scratch[...], wv_ref[...], bf16)


def project(pieces, gain, shift, w_query, w_key, w_value):
    width = gain.shape[0]
    size = sum(p.shape[0] for p in pieces)
    own = pieces[0].shape[0] + pieces[-1].shape[0]
    block = 512
    whole = lambda rows: pl.BlockSpec((rows, width), lambda j: (0, 0))
    weights = pl.BlockSpec((width, block), lambda j: (0, j))
    columns = lambda rows: pl.BlockSpec((rows, block), lambda j: (0, j))
    return pl.pallas_call(
        functools.partial(project_kernel, len(pieces)),
        grid=(width // block,),
        in_specs=[whole(1), whole(1)] + [weights] * 3 + [whole(p.shape[0]) for p in pieces],
        out_specs=[whole(size), columns(own), columns(size), columns(size)],
        out_shape=[jax.ShapeDtypeStruct((rows, width), bf16) for rows in (size, own, size, size)],
        scratch_shapes=[pltpu.VMEM((size, width), bf16)],
        compiler_params=params("arbitrary"),
        cost_estimate=cost(4 * size * width * width, 8 * size * width + 4 * width * width),
        name="project",
    )(gain[None], shift[None], w_query, w_key, w_value, *pieces)


def weights_kernel(odd_ref, *refs):
    attended_ref, others_ref, grad_ref, dq_ref, *backs = refs[:-2]
    keep_ref, send_ref = refs[-2:]
    size = others_ref.shape[0]
    totals = [
        matmul_tn(attended_ref[...], grad_ref[...]),
        matmul_tn(others_ref[:PROMPT_DEV, :], dq_ref[:PROMPT_DEV, :])
        + matmul_tn(others_ref[size - CONT_DEV :, :], dq_ref[PROMPT_DEV:, :]),
    ]
    for i in range(2):
        total, start = None, 0
        for ref in backs:
            count = ref.shape[1]
            part = matmul_tn(others_ref[start : start + count, :], ref[i])
            total = part if total is None else total + part
            start += count
        totals.append(total)
    half, rows = keep_ref.shape[2:4]

    def put(even_ref, odd_ref):
        for i, total in enumerate(totals):
            for j in range(half):
                start = 2 * j * rows
                even_ref[i, 0, j] = rounded(total[start : start + rows])
                odd_ref[i, 0, j] = rounded(total[start + rows : start + 2 * rows])

    @pl.when(odd_ref[0] == 0)
    def _():
        put(keep_ref, send_ref)

    @pl.when(odd_ref[0] != 0)
    def _():
        put(send_ref, keep_ref)


def weight_parts(odd, attended, others_in, grad_attn, grad_queries, backs, groups, experts):
    width = attended.shape[1]
    part = width // groups
    rows = part // experts
    left = lambda m: pl.BlockSpec((m.shape[0], part), lambda j: (0, j))
    whole = lambda m: pl.BlockSpec(m.shape, lambda j: (0,) * m.ndim)
    lefts, rights = [attended, others_in], [grad_attn, grad_queries, *backs]
    shape = (4, groups, experts // 2, rows, width)
    out = pl.BlockSpec((4, 1) + shape[2:], lambda j: (0, j, 0, 0, 0))
    return pl.pallas_call(
        weights_kernel,
        grid=(groups,),
        in_specs=[pl.BlockSpec(memory_space=pltpu.SMEM)]
        + [left(m) for m in lefts]
        + [whole(m) for m in rights],
        out_specs=[out, out],
        out_shape=[jax.ShapeDtypeStruct(shape, bf16)] * 2,
        compiler_params=params("arbitrary"),
        cost_estimate=cost(10e9, 30e6),
        name="weight_parts",
    )(odd, *lefts, *rights)


def resid_back_kernel(
    got_ref, spread_ref, resid_ref, gain_ref, cot_ref, wo_ref, grad_ref, attn_ref, attended_ref, sums_ref
):
    grad = matmul_tn(spread_ref[...], got_ref[...])
    _, normed, inverse = normalize(resid_ref[...], 1.0, 0.0)
    sums = jnp.concatenate(
        [jnp.sum(grad * normed, axis=0, keepdims=True), jnp.sum(grad, axis=0, keepdims=True)]
    )

    @pl.when(pl.program_id(0) == 0)
    def _():
        sums_ref[...] = sums

    @pl.when(pl.program_id(0) > 0)
    def _():
        sums_ref[...] += sums

    total = cot_ref[...].astype(f32) + norm_back(grad, gain_ref[...], normed, inverse)
    grad_ref[...] = total
    attn_ref[...] = rounded(total)
    attended_ref[...] = matmul_nt(rounded(total), wo_ref[...], bf16)


def resid_back(got, spread, residual, gain, cotangent, w_output):
    rows, width = residual.shape
    slots = got.shape[0]
    block = 256
    whole = lambda count: pl.BlockSpec((count, width), lambda j: (0, 0))
    part = pl.BlockSpec((block, width), lambda j: (j, 0))
    return pl.pallas_call(
        resid_back_kernel,
        grid=(rows // block,),
        in_specs=[
            whole(slots),
            pl.BlockSpec((slots, block), lambda j: (0, j)),
            part,
            whole(1),
            part,
            whole(width),
        ],
        out_specs=[part, part, part, whole(2)],
        out_shape=[
            jax.ShapeDtypeStruct((rows, width), f32),
            jax.ShapeDtypeStruct((rows, width), bf16),
            jax.ShapeDtypeStruct((rows, width), bf16),
            jax.ShapeDtypeStruct((2, width), f32),
        ],
        compiler_params=params("arbitrary"),
        cost_estimate=cost(2 * rows * width * (slots + width), 16 * rows * width),
        name="resid_back",
    )(got, spread, residual, gain[None], cotangent, w_output)


def input_back_kernel(
    prompt_ref, own_ref, near_ref, dq_ref, wq_ref, wk_ref, wv_ref, x_ref, gain_ref, resid_ref,
    out_ref, sums_ref, dk_ref, dv_ref,
):
    step = pl.program_id(0)
    block = dk_ref.shape[0]
    count = prompt_ref.shape[1]

    def put(first):
        for i, ref in enumerate((dk_ref, dv_ref)):
            start, size = (0, block - count) if first else (block - count, block)
            if first:
                ref[:count, :] = prompt_ref[i]
            here = pl.ds(start, size)
            ref[block - size :, :] = rounded(added(own_ref[i, here, :], near_ref[i, here, :]))

    pl.when(step == 0)(lambda: put(True))
    pl.when(step > 0)(lambda: put(False))
    grad = matmul_nt(dq_ref[...], wq_ref[...])
    grad = grad + matmul_nt(dk_ref[...], wk_ref[...])
    grad = grad + matmul_nt(dv_ref[...], wv_ref[...])
    _, normed, inverse = normalize(x_ref[...].astype(f32), 1.0, 0.0)
    sums = jnp.concatenate(
        [jnp.sum(grad * normed, axis=0, keepdims=True), jnp.sum(grad, axis=0, keepdims=True)]
    )

    @pl.when(step == 0)
    def _():
        sums_ref[...] = sums

    @pl.when(step > 0)
    def _():
        sums_ref[...] += sums

    out_ref[...] = rounded(resid_ref[...] + norm_back(grad, gain_ref[...], normed, inverse))


def input_back(prompt, own, near, grad_queries, w_query, w_key, w_value, tokens, gain, grad_resid):
    rows, width = tokens.shape
    block = rows // 2
    whole = lambda count: pl.BlockSpec((count, width), lambda j: (0, 0))
    part = pl.BlockSpec((block, width), lambda j: (j, 0))
    pair = lambda count: pl.BlockSpec((2, count, width), lambda j: (0, 0, 0))
    return pl.pallas_call(
        input_back_kernel,
        grid=(rows // block,),
        in_specs=[
            pair(PROMPT_DEV),
            pair(CONT_DEV),
            pair(CONT_DEV),
            part,
            whole(width),
            whole(width),
            whole(width),
            part,
            whole(1),
            part,
        ],
        out_specs=[part, whole(2)],
        out_shape=[
            jax.ShapeDtypeStruct((rows, width), bf16),
            jax.ShapeDtypeStruct((2, width), f32),
        ],
        scratch_shapes=[pltpu.VMEM((block, width), bf16)] * 2,
        compiler_params=params("arbitrary"),
        cost_estimate=cost(6 * rows * width * width, 20 * rows * width),
        name="input_back",
    )(prompt, own, near, grad_queries, w_query, w_key, w_value, tokens, gain[None], grad_resid)


def head_stack(block):
    first = lax.broadcasted_iota(jnp.int32, block.shape, 1) < block.shape[1] // 2
    zero = jnp.zeros_like(block)
    return jnp.concatenate([jnp.where(first, block, zero), jnp.where(first, zero, block)])


def head_merge(turned):
    half, rows = turned.shape[0] // 2, turned.shape[1] // 2
    return jnp.concatenate([turned[:half, :rows], turned[half:, rows:]]).T


def chunk_scores(chunk, keys, stack, near_bias, bias_ref, prompt_len):
    scores = matmul_nt(keys, stack)
    if chunk == 0:
        bias = bias_ref[...]
        return scores + jnp.concatenate([bias, bias], axis=1)
    tri = (PROMPT_DEV, PROMPT_DEV)
    after = lax.broadcasted_iota(jnp.int32, tri, 0) > lax.broadcasted_iota(jnp.int32, tri, 1)
    diag = jnp.where(after, f32(masked_score), f32(0.0))
    last = keys.shape[0] - PROMPT_DEV
    near_end = prompt_len + CONT_DEV
    pieces = [scores[:prompt_len], scores[prompt_len:near_end] + near_bias]
    if last > near_end:
        pieces.append(scores[near_end:last])
    pieces.append(scores[last:] + jnp.concatenate([diag, diag], axis=1))
    return jnp.concatenate(pieces)


def chunk_keys(chunk, prompt_len):
    return prompt_len if chunk == 0 else prompt_len + CONT_DEV + PROMPT_DEV * chunk


def attend_kernel(prompt_len, near_ref, q_ref, k_ref, v_ref, bias_ref, out_ref, log_ref):
    scale = bf16(1.0 / math.sqrt(q_ref.shape[1] // 2))
    chunks = q_ref.shape[0] // PROMPT_DEV

    def scores_of(chunk):
        stack = head_stack(q_ref[pl.ds(chunk * PROMPT_DEV, PROMPT_DEV), :] * scale)
        keys = k_ref[: chunk_keys(chunk, prompt_len), :]
        return chunk_scores(chunk, keys, stack, near_ref[0], bias_ref, prompt_len)

    scores = scores_of(0)
    for chunk in range(chunks):
        rows = pl.ds(chunk * PROMPT_DEV, PROMPT_DEV)
        size = chunk_keys(chunk, prompt_len)
        later = scores_of(chunk + 1) if chunk + 1 < chunks else None
        top = jnp.max(scores, axis=0, keepdims=True)
        weights = jnp.exp(scores - top)
        total = jnp.sum(weights, axis=0, keepdims=True)
        mixed = matmul_tn(v_ref[:size, :], rounded(weights)) / total
        out_ref[rows, :] = rounded(head_merge(mixed))
        log_ref[0, chunk : chunk + 1, :] = top + jnp.log(total)
        scores = later


def attend_back_kernel(
    prompt_len,
    near_ref,
    q_ref,
    k_ref,
    v_ref,
    bias_ref,
    log_ref,
    out_ref,
    grad_ref,
    dq_ref,
    first_ref,
    second_ref,
    near_out_ref,
    own_ref,
    dk_ref,
    dv_ref,
):
    scale = 1.0 / math.sqrt(q_ref.shape[1] // 2)
    half = q_ref.shape[1] // 2
    dk_ref[...] = jnp.zeros_like(dk_ref)
    dv_ref[...] = jnp.zeros_like(dv_ref)
    for chunk in range(q_ref.shape[0] // PROMPT_DEV):
        rows = pl.ds(chunk * PROMPT_DEV, PROMPT_DEV)
        size = chunk_keys(chunk, prompt_len)
        stack = head_stack(q_ref[rows, :] * bf16(scale))
        grad = grad_ref[rows, :]
        grad_stack = head_stack(grad)
        product = (grad.astype(f32) * out_ref[rows, :].astype(f32)).T
        inner = jnp.concatenate(
            [
                jnp.sum(product[:half], axis=0, keepdims=True),
                jnp.sum(product[half:], axis=0, keepdims=True),
            ],
            axis=1,
        )
        keys = k_ref[:size, :]
        scores = chunk_scores(chunk, keys, stack, near_ref[0], bias_ref, prompt_len)
        weights = jnp.exp(scores - log_ref[0, chunk : chunk + 1, :])
        dv_ref[:size, :] += matmul(rounded(weights), grad_stack)
        grad_prob = matmul_nt(v_ref[:size, :], grad_stack)
        grad_score = rounded(weights * (grad_prob - inner))
        dk_ref[:size, :] += matmul(grad_score, stack)
        dq_ref[rows, :] = rounded(head_merge(matmul_tn(keys, grad_score)) * scale)
    start = 0
    for ref in (first_ref, second_ref, near_out_ref, own_ref):
        count = ref.shape[1]
        ref[0] = rounded(dk_ref[start : start + count, :])
        ref[1] = rounded(dv_ref[start : start + count, :])
        start += count


def attend(near_bias, queries, keys, values, bias):
    rows, width = queries.shape
    size = keys.shape[0]
    prompt_len = bias.shape[0]
    lanes = 2 * width // HEADS
    pairs = HEADS // 2
    chunks = rows // PROMPT_DEV
    block = lambda count: pl.BlockSpec((count, lanes), lambda j: (0, j))
    return pl.pallas_call(
        functools.partial(attend_kernel, prompt_len),
        grid=(pairs,),
        in_specs=[
            pl.BlockSpec(memory_space=pltpu.SMEM),
            block(rows),
            block(size),
            block(size),
            pl.BlockSpec((prompt_len, PROMPT_DEV), lambda j: (0, 0)),
        ],
        out_specs=[
            block(rows),
            pl.BlockSpec((1, chunks, 2 * PROMPT_DEV), lambda j: (j, 0, 0)),
        ],
        out_shape=[
            jax.ShapeDtypeStruct((rows, width), bf16),
            jax.ShapeDtypeStruct((pairs, chunks, 2 * PROMPT_DEV), f32),
        ],
        compiler_params=params("arbitrary"),
        cost_estimate=cost(16 * rows * size * width, 4 * (rows + size) * width, rows * size * HEADS),
        name="attend",
    )(near_bias, queries, keys, values, bias)


def attend_back(near_bias, queries, keys, values, bias, log_total, attended, grad):
    rows, width = queries.shape
    size = keys.shape[0]
    prompt_len = bias.shape[0]
    lanes = 2 * width // HEADS
    pairs = HEADS // 2
    chunks = rows // PROMPT_DEV
    block = lambda count: pl.BlockSpec((count, lanes), lambda j: (0, j))
    counts = (prompt_len // 2, prompt_len // 2, CONT_DEV, CONT_DEV)
    return pl.pallas_call(
        functools.partial(attend_back_kernel, prompt_len),
        grid=(pairs,),
        in_specs=[
            pl.BlockSpec(memory_space=pltpu.SMEM),
            block(rows),
            block(size),
            block(size),
            pl.BlockSpec((prompt_len, PROMPT_DEV), lambda j: (0, 0)),
            pl.BlockSpec((1, chunks, 2 * PROMPT_DEV), lambda j: (j, 0, 0)),
            block(rows),
            block(rows),
        ],
        out_specs=[block(rows)]
        + [pl.BlockSpec((2, count, lanes), lambda j: (0, 0, j)) for count in counts],
        out_shape=[jax.ShapeDtypeStruct((rows, width), bf16)]
        + [jax.ShapeDtypeStruct((2, count, width), bf16) for count in counts],
        scratch_shapes=[pltpu.VMEM((size, lanes), f32), pltpu.VMEM((size, lanes), f32)],
        compiler_params=params("arbitrary"),
        cost_estimate=cost(40 * rows * size * width, 8 * (rows + size) * width, rows * size * HEADS),
        name="attend_back",
    )(near_bias, queries, keys, values, bias, log_total, attended, grad)


def local(
    tokens_in,
    cotangent,
    hash_ids,
    norm1_gain,
    norm1_bias,
    w_query,
    w_key,
    w_value,
    w_output,
    norm2_gain,
    norm2_bias,
    expert_in,
    expert_out,
):
    row_count, width = tokens_in.shape
    experts = lax.axis_size("expert")
    groups = lax.axis_size("group")
    position = lax.axis_index("expert")
    group = lax.axis_index("group")
    capacity = 2 * row_count // experts
    slots = experts * capacity
    tied = lax.optimization_barrier

    def all_exchanged(values):
        return lax.all_to_all(values, "expert", split_axis=0, concat_axis=0, tiled=True)

    def exchanged(values):
        got = all_exchanged(values.reshape(experts, capacity, width))
        return got.reshape(slots, width)

    near_tokens = lax.ppermute(
        tokens_in[PROMPT_DEV:], "expert", [(i, i + 1) for i in range(0, experts, 2)]
    )
    prompts, prompt_ids, near_tokens, last_tokens = gather_relative(
        tokens_in[:PROMPT_DEV], "expert", near_tokens
    )
    ids = jnp.broadcast_to(rounded(hash_ids), (row_count, 128))
    all_cot = lax.all_gather(jnp.concatenate([cotangent, ids], axis=1), "group")

    row_index = jnp.arange(row_count, dtype=jnp.int32)
    lower = rounded(row_index[:, None] >= row_index[None, :])

    routed = rounded(hash_ids == jnp.arange(experts, dtype=jnp.int32)[None, :])
    running = matmul(lower, routed)
    rank = (jnp.sum(running * routed.astype(f32), axis=-1) - 1.0).astype(jnp.int32)
    slot = hash_ids[:, 0] * capacity + rank
    spread = rounded(slot[None, :] == jnp.arange(slots, dtype=jnp.int32)[:, None])

    cot_sent, _ = tied((matmul(spread, cotangent, bf16), last_tokens))
    cot = {0: exchanged(cot_sent)}
    others_in, queries, keys, values = project(
        prompts + [near_tokens, tokens_in[PROMPT_DEV:]],
        norm1_gain,
        norm1_bias,
        w_query,
        w_key,
        w_value,
    )
    block_pos = jnp.stack([(position ^ r) * PROMPT_DEV for r in prompt_ids])
    prompt_pos = jnp.arange(PROMPT_DEV, dtype=jnp.int32)
    key_pos = (block_pos[:, None] + prompt_pos[None, :]).reshape(-1)
    query_pos = position * PROMPT_DEV + row_index[:PROMPT_DEV]
    bias = jnp.where(key_pos[:, None] <= query_pos[None, :], f32(0.0), f32(masked_score))
    near_bias = jnp.where(position % 2 == 1, f32(0.0), f32(masked_score))[None]
    attended, log_total = attend(near_bias, queries, keys, values, bias)

    residual = tokens_in.astype(f32) + matmul(attended, w_output)
    ffn_in = rounded(normalize(residual, norm2_gain, norm2_bias)[0])
    rows = exchanged(matmul(spread, ffn_in, bf16))
    all_numbers = all_cot[:, :, width].astype(jnp.int32)[:, None]
    numbers = lambda masks: jnp.stack([group ^ mask for mask in masks])
    near_sent = spread_rows(numbers([1]), all_numbers, all_cot, experts)
    grad_hidden = expert_back(cot[0], expert_out)
    rows, grad_hidden, near_sent = tied((rows, grad_hidden, near_sent))
    all_rows = lax.all_gather(rows, "group")
    cot[1] = all_exchanged(near_sent)
    hidden, grad_pre, grad_rows = expert_front(rows, grad_hidden, expert_in)
    grad_rows, hidden, cot[1] = tied((grad_rows, hidden, cot[1]))
    grad_got = exchanged(grad_rows)
    produced = expert_produce(hidden, expert_out)
    far_sent = spread_rows(numbers(range(2, groups)), all_numbers, all_cot, experts, produced)
    far_sent, grad_got = tied((far_sent, grad_got))
    far_got = all_exchanged(far_sent)

    grad_resid, grad_attn, grad_attended, sums2 = resid_back(
        grad_got, spread, residual, norm2_gain, cotangent, w_output
    )
    grad_queries, back_first, back_second, back_near, back_own = attend_back(
        near_bias, queries, keys, values, bias, log_total, attended, grad_attended
    )
    backs = (back_first, back_second, back_near, back_own, grad_queries)
    prompt_sums = scatter_relative(back_first, back_second, "expert")
    prompt_sent = next(prompt_sums)
    near_back = lax.ppermute(
        back_near, "expert", [(i + 1, i) for i in range(0, experts, 2)]
    )
    weights = weight_parts(
        (position & 1)[None],
        attended,
        others_in,
        grad_attn,
        grad_queries,
        (back_first, back_second, back_near, back_own),
        groups,
        experts,
    )
    place, _ = tied((group[None], weights))
    own_part = own_out(place, groups, hidden, cot[0])
    weights, prompt_sent, near_back, far_got, own_part = tied(
        (weights, prompt_sent, near_back, far_got, own_part)
    )
    marks = []
    weight_sums = weight_chain(*weights, marks)
    weight_sent = next(weight_sums)
    prompt_sent, prompt_back = moved_on(prompt_sums, prompt_sent)
    result_got = far_got[:, 0].reshape(slots, width)
    result = rounded(residual + matmul_tn(spread, result_got))
    weight_sent, prompt_sent, result = tied((weight_sent, prompt_sent, result))
    weight_sent, _ = moved_on(weight_sums, weight_sent)
    number, _ = tied((numbers(range(groups)), marks[-1]))
    operands = (expert_in, expert_out, (rows, grad_pre), all_rows, cot[1], far_got)
    in_first, *hidden_first = in_sums(number, 0, *operands)
    over_group = lambda values: lax.all_to_all(
        values, "group", split_axis=0, concat_axis=0, tiled=True
    )
    got_first = over_group(in_first)
    weight_sent, prompt_sent, _ = tied((weight_sent, prompt_sent, in_first))
    weight_sent, _ = moved_on(weight_sums, weight_sent)
    prompt_sent, prompt_back = moved_on(prompt_sums, prompt_sent)
    number, _ = tied((number, marks[-1]))
    in_second, *hidden_second = in_sums(number, 1, *operands)
    got_first, in_second, prompt_sent, weight_sent = tied(
        (got_first, in_second, prompt_sent, weight_sent)
    )
    got_second = over_group(in_second)
    prompt_sent, weight_sent, _ = tied((prompt_sent, weight_sent, in_second))
    while prompt_sent is not None:
        prompt_sent, prompt_back = moved_on(prompt_sums, prompt_sent)
    grad_tokens, sums1 = input_back(
        prompt_back,
        back_own,
        near_back,
        grad_queries,
        w_query,
        w_key,
        w_value,
        tokens_in,
        norm1_gain,
        grad_resid,
    )
    weight_sent, own_part, sums1 = tied((weight_sent, own_part, sums1))
    weight_sent, weight_grads = moved_on(weight_sums, weight_sent)
    grad_expert_out = out_sums(own_part, cot[1], far_got, hidden_first + hidden_second)
    vectors = jnp.concatenate([sums1, sums2])
    vectors, got_second, grad_expert_out, weight_sent = tied(
        (vectors, got_second, grad_expert_out, weight_sent)
    )
    vectors = vector_sums(vectors)
    while weight_sent is not None:
        weight_sent, weight_grads = moved_on(weight_sums, weight_sent)
    grad_expert_in = lay_out([got_first, got_second])
    grad_w_output, grad_w_query, grad_w_key, grad_w_value = weight_grads
    return (
        result,
        grad_tokens,
        vectors[0],
        vectors[1],
        grad_w_query,
        grad_w_key,
        grad_w_value,
        grad_w_output,
        vectors[2],
        vectors[3],
        grad_expert_in,
        grad_expert_out,
    )


def solution(mesh):
    both = ("group", "expert")
    return jax.shard_map(
        local,
        mesh=mesh,
        in_specs=(
            P(both, None),
            P(both, None),
            P(both, None),
            P(),
            P(),
            P(),
            P(),
            P(),
            P(),
            P(),
            P(),
            P("expert", None, None),
            P("expert", None, None),
        ),
        out_specs=(
            P(both, None),
            P(both, None),
            P(both),
            P(both),
            P(both, None),
            P(both, None),
            P(both, None),
            P(both, None),
            P(both),
            P(both),
            P("expert", "group", None),
            P("expert", "group", None),
        ),
        check_vma=False,
    )
```

```python
import functools
import math

import jax
import jax.numpy as jnp
from jax import lax
from jax.experimental import pallas as pl
from jax.experimental.pallas import tpu as pltpu
from jax.sharding import PartitionSpec as P

HEADS = 16
PROMPT_DEV = 128
CONT_DEV = 384


norm_eps = 1e-05
masked_score = -1e30
bf16 = jnp.bfloat16
f32 = jnp.float32
MIB = 1 << 20
share = 0.05


def swapped(block, axis, mask):
    return lax.ppermute(block, axis, [(i, i ^ mask) for i in range(lax.axis_size(axis))])


def rounded(values):
    return values.astype(bf16)


def normalize(values, gain, shift):
    average = jnp.mean(values, axis=-1, keepdims=True)
    centered = values - average
    variance = jnp.mean(centered * centered, axis=-1, keepdims=True)
    inverse = lax.rsqrt(variance + norm_eps)
    normed = centered * inverse
    return (normed * gain + shift, normed, inverse)


def norm_back(grad_out, gain, normed, inverse):
    scaled = grad_out * gain
    first_mean = jnp.mean(scaled, axis=-1, keepdims=True)
    second = jnp.mean(scaled * normed, axis=-1, keepdims=True)
    return inverse * (scaled - first_mean - normed * second)


def matmul(a, b, kind=f32):
    return jnp.dot(a, b, preferred_element_type=f32).astype(kind)


def matmul_nt(a, b, kind=f32):
    return lax.dot_general(a, b, (((1,), (1,)), ((), ())), preferred_element_type=f32).astype(kind)


def matmul_tn(a, b, kind=f32):
    return lax.dot_general(a, b, (((0,), (0,)), ((), ())), preferred_element_type=f32).astype(kind)


def outer_bits(size):
    return range(size.bit_length() - 2, 0, -1)


def gather_relative(block, axis, more):
    size = lax.axis_size(axis)
    pieces = {0: block}
    ready, last = [0], []
    while ready:
        fresh = {}
        for r in ready:
            for bit in outer_bits(size):
                if r ^ (1 << bit) not in pieces and r ^ (1 << bit) not in fresh:
                    fresh[r ^ (1 << bit)] = swapped(pieces[r], axis, 1 << bit)
        fresh, more = lax.optimization_barrier((fresh, more))
        pieces.update(fresh)
        ready, last = list(fresh), list(fresh.values()) or last
    near = sorted(pieces)
    for r in near:
        pieces[r ^ 1] = swapped(pieces[r], axis, 1)
    order = near + [r ^ 1 for r in near]
    return [pieces[r] for r in order], order, more, last


def scatter_relative(near, far, axis, marks):
    size = lax.axis_size(axis)
    got = yield swapped(far, axis, 1)
    both = added(near, got)
    count = size // 2
    rows = both.shape[1] // count
    pieces = {2 * i: rounded(both[:, i * rows : (i + 1) * rows]) for i in range(count)}
    marks.append(pieces)
    bits = list(outer_bits(size))
    for level in range(len(bits), 0, -1):
        sent, spans = [], []
        for r in [r for r in sorted(pieces) if bin(r).count("1") == level]:
            ways = [bit for bit in bits if r >> bit & 1]
            if rows % (16 * len(ways)):
                ways = ways[:1]
            part = rows // len(ways)
            piece = pieces.pop(r)
            for i, bit in enumerate(ways):
                span = (i * part, (i + 1) * part)
                sent.append(swapped(piece[:, span[0] : span[1]], axis, 1 << bit))
                spans.append((r ^ (1 << bit), span))
        gots = yield sent
        for r in sorted(pieces):
            total = pieces[r].astype(f32)
            for got, (target, span) in zip(gots, spans):
                if target == r:
                    outside = ((0, 0), (span[0], rows - span[1]), (0, 0))
                    total = total + jnp.pad(got.astype(f32), outside)
            pieces[r] = rounded(total)
    return pieces[0]


def halved(blocks, place, axis, bit):
    own = (lax.axis_index(axis) >> bit) & 1
    return (
        lax.dynamic_index_in_dim(blocks, own, place, keepdims=False),
        lax.dynamic_index_in_dim(blocks, 1 - own, place, keepdims=False),
    )


def added(keep, got):
    return keep.astype(f32) + got.astype(f32)


def places_of(bits, bit, value):
    rest = [other for other in bits if other != bit]
    weight = {other: 1 << (len(bits) - 1 - i) for i, other in enumerate(bits)}
    places = []
    for number in range(1 << len(rest)):
        place = value * weight[bit]
        for i, other in enumerate(rest):
            place = place + (number >> (len(rest) - 1 - i) & 1) * weight[other]
        places.append(place)
    return places


def halve_kernel(lefts, bits, own_ref, *refs):
    sets = len(lefts)
    for k, (left, bit) in enumerate(zip(lefts, bits)):
        keep_ref, got_ref = refs[2 * k : 2 * k + 2]
        outs = refs[2 * sets + 2 * k : 2 * sets + 2 * k + 2]
        own = (own_ref[0] >> bit) & 1
        for ref, value in zip(outs, (own, 1 - own)):
            for i, place in enumerate(places_of(left, bit, value)):
                for j in range(ref.shape[1]):
                    ref[0, j, i] = rounded(added(keep_ref[0, j, place], got_ref[0, j, place]))


def halve(number, states, bits):
    _, groups, count, rows, width = states[0][0].shape
    shape = (2, groups, count // 2, rows, width)
    came = lambda first: pl.BlockSpec(
        (1, groups, count, rows, width), lambda i: (first + i if first else i, 0, 0, 0, 0)
    )
    out = pl.BlockSpec((1, groups, count // 2, rows, width), lambda i: (i, 0, 0, 0, 0))
    size = 2 * math.prod(shape)
    outs = pl.pallas_call(
        functools.partial(halve_kernel, [state[3] for state in states], bits),
        grid=(2,),
        in_specs=[pl.BlockSpec(memory_space=pltpu.SMEM)]
        + [came(state[2]) for state in states for _ in range(2)],
        out_specs=[out] * (2 * len(states)),
        out_shape=[jax.ShapeDtypeStruct(shape, bf16)] * (2 * len(states)),
        compiler_params=params("arbitrary"),
        cost_estimate=cost(2 * size, 12 * size),
        name="halve",
    )(number, *[value for state in states for value in state[:2]])
    return list(zip(outs[::2], outs[1::2]))


def turn_kernel(own_ref, *refs):
    (*sets, own_out_ref, send_ref) = refs
    own = own_ref[0] & 1
    start = 0
    for keep_ref, got_ref in zip(sets[::2], sets[1::2]):
        for i in range(keep_ref.shape[0]):
            for j in range(keep_ref.shape[1] // 2):
                for ref, value in ((own_out_ref, own), (send_ref, 1 - own)):
                    place = 2 * j + value
                    ref[start + i, j] = rounded(added(keep_ref[i, place, 0], got_ref[i, place, 0]))
        start += keep_ref.shape[0]


def turn(number, sets):
    _, groups, _, rows, width = sets[0].shape
    shape = (4, groups // 2, rows, width)
    return pl.pallas_call(
        turn_kernel,
        in_specs=[pl.BlockSpec(memory_space=pltpu.SMEM)]
        + [pl.BlockSpec(memory_space=pltpu.VMEM)] * len(sets),
        out_specs=[pl.BlockSpec(memory_space=pltpu.VMEM)] * 2,
        out_shape=[jax.ShapeDtypeStruct(shape, bf16)] * 2,
        compiler_params=params(),
        cost_estimate=cost(8 * sets[0].size, 8 * sets[0].size),
        name="turn",
    )(number, *sets)


def weight_chain(keep, send, marks):
    bits = list(range(1, lax.axis_size("expert").bit_length() - 1))
    number = lax.axis_index("expert")[None]
    got = yield swapped(send, "expert", 1)
    states = [(keep, got, 0, bits[::-1]), (keep, got, 2, bits[::-1])]
    for pair in zip(bits, bits[::-1]):
        halves = halve(number, states, pair)
        marks.append(halves[0][0])
        gots = yield [swapped(send, "expert", 1 << bit) for bit, (_, send) in zip(pair, halves)]
        states = [
            (keep, got, 0, [other for other in state[3] if other != bit])
            for state, bit, (keep, _), got in zip(states, pair, halves, gots)
        ]
    keep, send = turn(
        lax.axis_index("group")[None], [value for state in states for value in state[:2]]
    )
    marks.append(keep)
    got = yield swapped(send, "group", 1)
    both = added(keep, got)
    bits = list(range(1, lax.axis_size("group").bit_length() - 1))
    both = both.reshape((4,) + (2,) * len(bits) + both.shape[-2:])
    left = bits[::-1]
    for bit in bits:
        keep, send = halved(rounded(both), 1 + left.index(bit), "group", bit)
        left.remove(bit)
        got = yield swapped(send, "group", 1 << bit)
        both = added(keep, got)
    return [both[i] for i in range(both.shape[0])]


def moved_on(chain, came):
    try:
        return chain.send(came), None
    except StopIteration as stop:
        return None, stop.value


def vector_sums(vectors):
    axes = ("group", "expert")
    devices = lax.axis_size("group") * lax.axis_size("expert")
    count, width = vectors.shape
    pieces = vectors.reshape(count, devices, width // devices).swapaxes(0, 1)
    got = lax.all_to_all(pieces, axes, split_axis=0, concat_axis=0, tiled=True)
    return jnp.sum(got, axis=0)


def params(*semantics):
    return pltpu.CompilerParams(dimension_semantics=semantics, vmem_limit_bytes=60 * MIB)


def cost(flops, total_bytes, exps=0):
    return pl.CostEstimate(
        flops=int(flops * share), bytes_accessed=int(total_bytes * share), transcendentals=int(exps * share)
    )


def logistic(values):
    return 0.5 * jnp.tanh(0.5 * values) + 0.5


def back_kernel(cot_ref, wout_ref, out_ref):
    out_ref[...] = matmul_nt(cot_ref[...], wout_ref[0], bf16)


def expert_back(cot, expert_out):
    count, width = cot.shape
    ff = expert_out.shape[1]
    block = 1024
    return pl.pallas_call(
        back_kernel,
        grid=(ff // block,),
        in_specs=[
            pl.BlockSpec((count, width), lambda j: (0, 0)),
            pl.BlockSpec((1, block, width), lambda j: (0, j, 0)),
        ],
        out_specs=pl.BlockSpec((count, block), lambda j: (0, j)),
        out_shape=jax.ShapeDtypeStruct((count, ff), bf16),
        compiler_params=params("arbitrary"),
        cost_estimate=cost(2 * count * width * ff, 2 * count * ff + 2 * width * ff),
        name="expert_back",
    )(cot, expert_out)


def front_kernel(parts, rows_ref, gh_ref, win_ref, hidden_ref, pre_ref, out_ref, acc_ref):
    step = pl.program_id(0)
    count = rows_ref.shape[0] // parts

    @pl.when(step == 0)
    def _():
        acc_ref[...] = jnp.zeros_like(acc_ref)

    first = lambda i: matmul(rows_ref[i * count : (i + 1) * count, :], win_ref[0])
    pre = first(0)
    for i in range(parts):
        later = first(i + 1) if i + 1 < parts else None
        here = pl.ds(i * count, count)
        sig = logistic(pre)
        hidden = pre * sig
        hidden_ref[here, :] = rounded(hidden)
        grad_pre = rounded(gh_ref[here, :].astype(f32) * sig * (1.0 + pre - hidden))
        pre_ref[here, :] = grad_pre
        acc_ref[here, :] += matmul_nt(grad_pre, win_ref[0])
        pre = later

    @pl.when(step == pl.num_programs(0) - 1)
    def _():
        out_ref[...] = rounded(acc_ref[...])


def expert_front(rows, grad_hidden, expert_in):
    count, width = rows.shape
    ff = expert_in.shape[2]
    block = 1024
    whole = pl.BlockSpec((count, width), lambda j: (0, 0))
    part = pl.BlockSpec((count, block), lambda j: (0, j))
    return pl.pallas_call(
        functools.partial(front_kernel, 4),
        grid=(ff // block,),
        in_specs=[whole, part, pl.BlockSpec((1, width, block), lambda j: (0, 0, j))],
        out_specs=[part, part, whole],
        out_shape=[
            jax.ShapeDtypeStruct((count, ff), bf16),
            jax.ShapeDtypeStruct((count, ff), bf16),
            jax.ShapeDtypeStruct((count, width), bf16),
        ],
        scratch_shapes=[pltpu.VMEM((count, width), f32)],
        compiler_params=params("arbitrary"),
        cost_estimate=cost(4 * count * width * ff, 6 * count * ff + 2 * width * ff, count * ff),
        name="expert_front",
    )(rows, grad_hidden, expert_in)


def produce_kernel(hidden_ref, wout_ref, out_ref, acc_ref):
    step = pl.program_id(0)
    part = matmul(hidden_ref[...], wout_ref[0])

    @pl.when(step == 0)
    def _():
        acc_ref[...] = part

    @pl.when(step > 0)
    def _():
        acc_ref[...] += part

    @pl.when(step == pl.num_programs(0) - 1)
    def _():
        out_ref[...] = rounded(acc_ref[...])


def expert_produce(hidden, expert_out):
    count, ff = hidden.shape
    width = expert_out.shape[2]
    block = 1024
    return pl.pallas_call(
        produce_kernel,
        grid=(ff // block,),
        in_specs=[
            pl.BlockSpec((count, block), lambda j: (0, j)),
            pl.BlockSpec((1, block, width), lambda j: (0, j, 0)),
        ],
        out_specs=pl.BlockSpec((count, width), lambda j: (0, 0)),
        out_shape=jax.ShapeDtypeStruct((count, width), bf16),
        scratch_shapes=[pltpu.VMEM((count, width), f32)],
        compiler_params=params("arbitrary"),
        cost_estimate=cost(2 * count * width * ff, 2 * count * ff + 2 * width * ff),
        name="expert_produce",
    )(hidden, expert_out)


def in_kernel(
    half, number_ref, own_rows_ref, own_pre_ref, win_hbm, wout_hbm, rows_hbm, near_hbm, far_hbm,
    in_ref, near_out, far_out, in_sum, win_ref, wout_ref, rows_ref, cot_ref, hidden_ref,
    weight_sems, shard_sems, out_sems,
):
    shards, count, _ = rows_ref.shape
    block = win_ref.shape[1]
    place = pl.multiple_of((2 * number_ref[0] + half) * block, block)
    weights = [
        pltpu.make_async_copy(win_hbm.at[0, :, pl.ds(place, block)], win_ref, weight_sems.at[0]),
        pltpu.make_async_copy(wout_hbm.at[0, pl.ds(place, block), :], wout_ref, weight_sems.at[1]),
    ]
    copies, outs = [], []
    for i in range(shards):
        cot = near_hbm.at[:, 0] if i == 0 else far_hbm.at[:, i]
        rows = rows_hbm.at[number_ref[1 + i]]
        copies.append(
            [
                pltpu.make_async_copy(rows, rows_ref.at[i], shard_sems.at[i, 0]),
                pltpu.make_async_copy(cot, cot_ref.at[i], shard_sems.at[i, 1]),
            ]
        )
        out = near_out if i == 0 else far_out.at[i - 1]
        outs.append(pltpu.make_async_copy(hidden_ref.at[i], out, out_sems.at[i]))
    for copy in weights + [copy for pair in copies for copy in pair]:
        copy.start()
    in_sum[...] = matmul_tn(own_rows_ref[...], own_pre_ref[...])
    for copy in weights:
        copy.wait()
    for i in range(shards):
        for copy in copies[i]:
            copy.wait()
        rows = rows_ref[i]
        pre = matmul(rows, win_ref[...])
        grad_hidden = matmul_nt(cot_ref[i].reshape(rows.shape), wout_ref[...])
        sig = logistic(pre)
        hidden = pre * sig
        hidden_ref[i] = rounded(hidden)
        outs[i].start()
        grad_pre = rounded(grad_hidden * sig * (1.0 + pre - hidden))
        in_sum[...] += matmul_tn(rows, grad_pre)
    in_ref[...] = rounded(in_sum[...]).reshape(in_ref.shape)
    for copy in outs:
        copy.wait()


def in_sums(number, half, expert_in, expert_out, own, rows, near, far):
    groups, count, width = rows.shape
    sources, _, slots, _ = near.shape
    part = expert_in.shape[2] // groups
    block = part // 2
    shards = groups - 1
    there = pl.BlockSpec(memory_space=pl.ANY)
    return pl.pallas_call(
        functools.partial(in_kernel, half),
        grid_spec=pltpu.PrefetchScalarGridSpec(
            num_scalar_prefetch=1,
            grid=(1,),
            in_specs=[
                pl.BlockSpec((count, width), lambda j, w: (0, 0)),
                pl.BlockSpec((count, block), lambda j, w: (0, 2 * w[0] + half)),
            ]
            + [there] * 5,
            out_specs=[
                pl.BlockSpec((groups, width // groups, block), lambda j, w: (0, 0, 0)),
                there,
                there,
            ],
            scratch_shapes=[
                pltpu.VMEM((width, block), f32),
                pltpu.VMEM((width, block), bf16),
                pltpu.VMEM((block, width), bf16),
                pltpu.VMEM((shards, count, width), bf16),
                pltpu.VMEM((shards, sources, slots, width), bf16),
                pltpu.VMEM((shards, count, block), bf16),
                pltpu.SemaphoreType.DMA((2,)),
                pltpu.SemaphoreType.DMA((shards, 2)),
                pltpu.SemaphoreType.DMA((shards,)),
            ],
        ),
        out_shape=[
            jax.ShapeDtypeStruct((groups, width // groups, block), bf16),
            jax.ShapeDtypeStruct((count, block), bf16),
            jax.ShapeDtypeStruct((groups - 2, count, block), bf16),
        ],
        compiler_params=params("arbitrary"),
        cost_estimate=cost(6 * count * width * block * groups, 16e6, count * block * groups),
        name="in_sums",
    )(number, *own, expert_in, expert_out, rows, near, far)


def own_kernel(_, hidden_ref, cot_ref, out_ref):
    out_ref[...] = matmul_tn(hidden_ref[...], cot_ref[...])


def own_out(number, groups, hidden, cot):
    count, width = cot.shape
    part = hidden.shape[1] // groups
    block = part // 2
    return pl.pallas_call(
        own_kernel,
        grid_spec=pltpu.PrefetchScalarGridSpec(
            num_scalar_prefetch=1,
            grid=(2,),
            in_specs=[
                pl.BlockSpec((count, block), lambda j, w: (0, 2 * w[0] + j)),
                pl.BlockSpec((count, width), lambda j, w: (0, 0)),
            ],
            out_specs=pl.BlockSpec((block, width), lambda j, w: (j, 0)),
        ),
        out_shape=jax.ShapeDtypeStruct((part, width), f32),
        compiler_params=params("arbitrary"),
        cost_estimate=cost(2 * count * width * part, 8e6),
        name="own_out",
    )(number, hidden, cot)


def out_kernel(own_ref, near_ref, far_ref, *refs):
    out_ref, total = refs[-2:]
    hiddens = refs[:-2]
    block = total.shape[0] // 2
    count = hiddens[0].shape[0]
    step = pl.program_id(0)

    @pl.when(step == 0)
    def _():
        near = near_ref[...].reshape(count, -1)
        for half in range(2):
            here = pl.ds(half * block, block)
            total[here, :] = own_ref[here, :] + matmul_tn(hiddens[2 * half][...], near)

    far = far_ref[...].reshape(count, -1)
    for half in range(2):
        here = pl.ds(half * block, block)
        total[here, :] += matmul_tn(hiddens[2 * half + 1][0], far)

    @pl.when(step == pl.num_programs(0) - 1)
    def _():
        out_ref[0] = total[...]


def out_sums(own, near, far, hiddens):
    part, width = own.shape
    count = hiddens[0].shape[0]
    sources, _, slots, _ = near.shape
    steps = hiddens[1].shape[0]
    near_hidden = pl.BlockSpec((count, part // 2), lambda j: (0, 0))
    far_hidden = pl.BlockSpec((1, count, part // 2), lambda j: (j, 0, 0))
    return pl.pallas_call(
        out_kernel,
        grid=(steps,),
        in_specs=[
            pl.BlockSpec((part, width), lambda j: (0, 0)),
            pl.BlockSpec((sources, 1, slots, width), lambda j: (0, 0, 0, 0)),
            pl.BlockSpec((sources, 1, slots, width), lambda j: (0, 1 + j, 0, 0)),
        ]
        + [near_hidden, far_hidden] * 2,
        out_specs=pl.BlockSpec((1, part, width), lambda j: (0, 0, 0)),
        out_shape=jax.ShapeDtypeStruct((1, part, width), f32),
        scratch_shapes=[pltpu.VMEM((part, width), f32)],
        compiler_params=params("arbitrary"),
        cost_estimate=cost(2 * count * width * part * (steps + 1), 16e6),
        name="out_sums",
    )(own, near, far, *hiddens)


def lay_kernel(*refs):
    gots, out_ref = refs[:-1], refs[-1]
    block = gots[0].shape[2]
    for i in range(gots[0].shape[0]):
        for j, ref in enumerate(gots):
            start = (i * len(gots) + j) * block
            out_ref[0, :, start : start + block] = ref[i].astype(f32)


def lay_out(gots):
    groups, rows, block = gots[0].shape
    tall = 64
    width = groups * block * len(gots)
    return pl.pallas_call(
        lay_kernel,
        grid=(rows // tall,),
        in_specs=[pl.BlockSpec((groups, tall, block), lambda j: (0, j, 0))] * len(gots),
        out_specs=pl.BlockSpec((1, tall, width), lambda j: (0, j, 0)),
        out_shape=jax.ShapeDtypeStruct((1, rows, width), f32),
        compiler_params=params("arbitrary"),
        cost_estimate=cost(rows * width, 6 * rows * width),
        name="lay_out",
    )(*gots)


def spread_kernel(first, _, ids_ref, values_ref, *refs):
    out_ref = refs[-1]
    experts, _, capacity, width = out_ref.shape

    def spread():
        rows = ids_ref.shape[2]
        ids = ids_ref[0]
        number = lax.broadcasted_iota(jnp.int32, (experts, rows), 0)
        routed = jnp.where(number == ids, f32(1.0), f32(0.0))
        square = (rows, rows)
        before = lax.broadcasted_iota(jnp.int32, square, 0) <= lax.broadcasted_iota(
            jnp.int32, square, 1
        )
        running = matmul(rounded(routed), rounded(jnp.where(before, f32(1.0), f32(0.0))))
        rank = jnp.sum(running * routed, axis=0, keepdims=True).astype(jnp.int32) - 1
        slot = ids * capacity + rank
        places = lax.broadcasted_iota(jnp.int32, (experts * capacity, rows), 0)
        onehot = rounded(jnp.where(places == slot, f32(1.0), f32(0.0)))
        out = matmul(onehot, values_ref[0, :, :width], bf16)
        out_ref[...] = out.reshape(out_ref.shape)

    if first:
        step = pl.program_id(0)

        @pl.when(step == 0)
        def _():
            out_ref[...] = refs[0][...].reshape(out_ref.shape)

        pl.when(step > 0)(spread)
    else:
        spread()


def spread_rows(numbers, ids, values, experts, first=None):
    _, rows, columns = values.shape
    width = columns - 128
    capacity = 2 * rows // experts
    start = 0 if first is None else 1
    count = numbers.shape[0] + start
    which = lambda j, w: w[jnp.maximum(j - start, 0)]
    specs = [
        pl.BlockSpec((1, 1, rows), lambda j, w: (which(j, w), 0, 0)),
        pl.BlockSpec((1, rows, columns), lambda j, w: (which(j, w), 0, 0)),
    ]
    operands = [ids, values]
    if start:
        specs.append(pl.BlockSpec(first.shape, lambda j, w: (0, 0)))
        operands.append(first)
    return pl.pallas_call(
        functools.partial(spread_kernel, start),
        grid_spec=pltpu.PrefetchScalarGridSpec(
            num_scalar_prefetch=1,
            grid=(count,),
            in_specs=specs,
            out_specs=pl.BlockSpec((experts, 1, capacity, width), lambda j, w: (0, j, 0, 0)),
        ),
        out_shape=jax.ShapeDtypeStruct((experts, count, capacity, width), bf16),
        compiler_params=params("arbitrary"),
        cost_estimate=cost(2 * count * experts * capacity * rows * width, 8e6),
        name="spread_rows",
    )(numbers, *operands)


def project_kernel(count, gain_ref, bias_ref, wq_ref, wk_ref, wv_ref, *refs):
    pieces, (in_ref, q_ref, k_ref, v_ref, scratch) = refs[:count], refs[count:]

    @pl.when(pl.program_id(0) == 0)
    def _():
        start = 0
        for ref in pieces:
            end = start + ref.shape[0]
            values = normalize(ref[...].astype(f32), gain_ref[...], bias_ref[...])[0]
            scratch[start:end, :] = rounded(values)
            start = end
        in_ref[...] = scratch[...]

    first, last = pieces[0].shape[0], pieces[-1].shape[0]
    size = scratch.shape[0]
    q_ref[:first, :] = matmul(scratch[:first, :], wq_ref[...], bf16)
    q_ref[first:, :] = matmul(scratch[size - last :, :], wq_ref[...], bf16)
    k_ref[...] = matmul(scratch[...], wk_ref[...], bf16)
    v_ref[...] = matmul(scratch[...], wv_ref[...], bf16)


def project(pieces, gain, shift, w_query, w_key, w_value):
    width = gain.shape[0]
    size = sum(p.shape[0] for p in pieces)
    own = pieces[0].shape[0] + pieces[-1].shape[0]
    block = 512
    whole = lambda rows: pl.BlockSpec((rows, width), lambda j: (0, 0))
    weights = pl.BlockSpec((width, block), lambda j: (0, j))
    columns = lambda rows: pl.BlockSpec((rows, block), lambda j: (0, j))
    return pl.pallas_call(
        functools.partial(project_kernel, len(pieces)),
        grid=(width // block,),
        in_specs=[whole(1), whole(1)] + [weights] * 3 + [whole(p.shape[0]) for p in pieces],
        out_specs=[whole(size), columns(own), columns(size), columns(size)],
        out_shape=[jax.ShapeDtypeStruct((rows, width), bf16) for rows in (size, own, size, size)],
        scratch_shapes=[pltpu.VMEM((size, width), bf16)],
        compiler_params=params("arbitrary"),
        cost_estimate=cost(4 * size * width * width, 8 * size * width + 4 * width * width),
        name="project",
    )(gain[None], shift[None], w_query, w_key, w_value, *pieces)


def weights_kernel(odd_ref, *refs):
    attended_ref, others_ref, grad_ref, dq_ref, *backs = refs[:-2]
    keep_ref, send_ref = refs[-2:]
    size = others_ref.shape[0]
    totals = [
        matmul_tn(attended_ref[...], grad_ref[...]),
        matmul_tn(others_ref[:PROMPT_DEV, :], dq_ref[:PROMPT_DEV, :])
        + matmul_tn(others_ref[size - CONT_DEV :, :], dq_ref[PROMPT_DEV:, :]),
    ]
    for i in range(2):
        total, start = None, 0
        for ref in backs:
            count = ref.shape[1]
            part = matmul_tn(others_ref[start : start + count, :], ref[i])
            total = part if total is None else total + part
            start += count
        totals.append(total)
    half, rows = keep_ref.shape[2:4]

    def put(even_ref, odd_ref):
        for i, total in enumerate(totals):
            for j in range(half):
                start = 2 * j * rows
                even_ref[i, 0, j] = rounded(total[start : start + rows])
                odd_ref[i, 0, j] = rounded(total[start + rows : start + 2 * rows])

    @pl.when(odd_ref[0] == 0)
    def _():
        put(keep_ref, send_ref)

    @pl.when(odd_ref[0] != 0)
    def _():
        put(send_ref, keep_ref)


def weight_parts(odd, attended, others_in, grad_attn, grad_queries, backs, groups, experts):
    width = attended.shape[1]
    part = width // groups
    rows = part // experts
    left = lambda m: pl.BlockSpec((m.shape[0], part), lambda j: (0, j))
    whole = lambda m: pl.BlockSpec(m.shape, lambda j: (0,) * m.ndim)
    lefts, rights = [attended, others_in], [grad_attn, grad_queries, *backs]
    shape = (4, groups, experts // 2, rows, width)
    out = pl.BlockSpec((4, 1) + shape[2:], lambda j: (0, j, 0, 0, 0))
    return pl.pallas_call(
        weights_kernel,
        grid=(groups,),
        in_specs=[pl.BlockSpec(memory_space=pltpu.SMEM)]
        + [left(m) for m in lefts]
        + [whole(m) for m in rights],
        out_specs=[out, out],
        out_shape=[jax.ShapeDtypeStruct(shape, bf16)] * 2,
        compiler_params=params("arbitrary"),
        cost_estimate=cost(10e9, 30e6),
        name="weight_parts",
    )(odd, *lefts, *rights)


def resid_back_kernel(
    got_ref, spread_ref, resid_ref, gain_ref, cot_ref, wo_ref, grad_ref, attn_ref, attended_ref, sums_ref
):
    grad = matmul_tn(spread_ref[...], got_ref[...])
    _, normed, inverse = normalize(resid_ref[...], 1.0, 0.0)
    sums = jnp.concatenate(
        [jnp.sum(grad * normed, axis=0, keepdims=True), jnp.sum(grad, axis=0, keepdims=True)]
    )

    @pl.when(pl.program_id(0) == 0)
    def _():
        sums_ref[...] = sums

    @pl.when(pl.program_id(0) > 0)
    def _():
        sums_ref[...] += sums

    total = cot_ref[...].astype(f32) + norm_back(grad, gain_ref[...], normed, inverse)
    grad_ref[...] = total
    attn_ref[...] = rounded(total)
    attended_ref[...] = matmul_nt(rounded(total), wo_ref[...], bf16)


def resid_back(got, spread, residual, gain, cotangent, w_output):
    rows, width = residual.shape
    slots = got.shape[0]
    block = 256
    whole = lambda count: pl.BlockSpec((count, width), lambda j: (0, 0))
    part = pl.BlockSpec((block, width), lambda j: (j, 0))
    return pl.pallas_call(
        resid_back_kernel,
        grid=(rows // block,),
        in_specs=[
            whole(slots),
            pl.BlockSpec((slots, block), lambda j: (0, j)),
            part,
            whole(1),
            part,
            whole(width),
        ],
        out_specs=[part, part, part, whole(2)],
        out_shape=[
            jax.ShapeDtypeStruct((rows, width), f32),
            jax.ShapeDtypeStruct((rows, width), bf16),
            jax.ShapeDtypeStruct((rows, width), bf16),
            jax.ShapeDtypeStruct((2, width), f32),
        ],
        compiler_params=params("arbitrary"),
        cost_estimate=cost(2 * rows * width * (slots + width), 16 * rows * width),
        name="resid_back",
    )(got, spread, residual, gain[None], cotangent, w_output)


def input_back_kernel(
    prompt_ref, own_ref, near_ref, dq_ref, wq_ref, wk_ref, wv_ref, x_ref, gain_ref, resid_ref,
    out_ref, sums_ref, dk_ref, dv_ref,
):
    step = pl.program_id(0)
    block = dk_ref.shape[0]
    count = prompt_ref.shape[1]

    def put(first):
        for i, ref in enumerate((dk_ref, dv_ref)):
            start, size = (0, block - count) if first else (block - count, block)
            if first:
                ref[:count, :] = prompt_ref[i]
            here = pl.ds(start, size)
            ref[block - size :, :] = rounded(added(own_ref[i, here, :], near_ref[i, here, :]))

    pl.when(step == 0)(lambda: put(True))
    pl.when(step > 0)(lambda: put(False))
    grad = matmul_nt(dq_ref[...], wq_ref[...])
    grad = grad + matmul_nt(dk_ref[...], wk_ref[...])
    grad = grad + matmul_nt(dv_ref[...], wv_ref[...])
    _, normed, inverse = normalize(x_ref[...].astype(f32), 1.0, 0.0)
    sums = jnp.concatenate(
        [jnp.sum(grad * normed, axis=0, keepdims=True), jnp.sum(grad, axis=0, keepdims=True)]
    )

    @pl.when(step == 0)
    def _():
        sums_ref[...] = sums

    @pl.when(step > 0)
    def _():
        sums_ref[...] += sums

    out_ref[...] = rounded(resid_ref[...] + norm_back(grad, gain_ref[...], normed, inverse))


def input_back(prompt, own, near, grad_queries, w_query, w_key, w_value, tokens, gain, grad_resid):
    rows, width = tokens.shape
    block = rows // 2
    whole = lambda count: pl.BlockSpec((count, width), lambda j: (0, 0))
    part = pl.BlockSpec((block, width), lambda j: (j, 0))
    pair = lambda count: pl.BlockSpec((2, count, width), lambda j: (0, 0, 0))
    return pl.pallas_call(
        input_back_kernel,
        grid=(rows // block,),
        in_specs=[
            pair(PROMPT_DEV),
            pair(CONT_DEV),
            pair(CONT_DEV),
            part,
            whole(width),
            whole(width),
            whole(width),
            part,
            whole(1),
            part,
        ],
        out_specs=[part, whole(2)],
        out_shape=[
            jax.ShapeDtypeStruct((rows, width), bf16),
            jax.ShapeDtypeStruct((2, width), f32),
        ],
        scratch_shapes=[pltpu.VMEM((block, width), bf16)] * 2,
        compiler_params=params("arbitrary"),
        cost_estimate=cost(6 * rows * width * width, 20 * rows * width),
        name="input_back",
    )(prompt, own, near, grad_queries, w_query, w_key, w_value, tokens, gain[None], grad_resid)


def head_stack(block):
    first = lax.broadcasted_iota(jnp.int32, block.shape, 1) < block.shape[1] // 2
    zero = jnp.zeros_like(block)
    return jnp.concatenate([jnp.where(first, block, zero), jnp.where(first, zero, block)])


def head_merge(turned):
    half, rows = turned.shape[0] // 2, turned.shape[1] // 2
    return jnp.concatenate([turned[:half, :rows], turned[half:, rows:]]).T


def chunk_scores(chunk, keys, stack, near_bias, bias_ref, prompt_len):
    scores = matmul_nt(keys, stack)
    if chunk == 0:
        bias = bias_ref[...]
        return scores + jnp.concatenate([bias, bias], axis=1)
    tri = (PROMPT_DEV, PROMPT_DEV)
    after = lax.broadcasted_iota(jnp.int32, tri, 0) > lax.broadcasted_iota(jnp.int32, tri, 1)
    diag = jnp.where(after, f32(masked_score), f32(0.0))
    last = keys.shape[0] - PROMPT_DEV
    near_end = prompt_len + CONT_DEV
    pieces = [scores[:prompt_len], scores[prompt_len:near_end] + near_bias]
    if last > near_end:
        pieces.append(scores[near_end:last])
    pieces.append(scores[last:] + jnp.concatenate([diag, diag], axis=1))
    return jnp.concatenate(pieces)


def chunk_keys(chunk, prompt_len):
    return prompt_len if chunk == 0 else prompt_len + CONT_DEV + PROMPT_DEV * chunk


def attend_kernel(prompt_len, near_ref, q_ref, k_ref, v_ref, bias_ref, out_ref, log_ref):
    scale = bf16(1.0 / math.sqrt(q_ref.shape[1] // 2))
    chunks = q_ref.shape[0] // PROMPT_DEV

    def scores_of(chunk):
        stack = head_stack(q_ref[pl.ds(chunk * PROMPT_DEV, PROMPT_DEV), :] * scale)
        keys = k_ref[: chunk_keys(chunk, prompt_len), :]
        return chunk_scores(chunk, keys, stack, near_ref[0], bias_ref, prompt_len)

    scores = scores_of(0)
    for chunk in range(chunks):
        rows = pl.ds(chunk * PROMPT_DEV, PROMPT_DEV)
        size = chunk_keys(chunk, prompt_len)
        later = scores_of(chunk + 1) if chunk + 1 < chunks else None
        top = jnp.max(scores, axis=0, keepdims=True)
        weights = jnp.exp(scores - top)
        total = jnp.sum(weights, axis=0, keepdims=True)
        mixed = matmul_tn(v_ref[:size, :], rounded(weights)) / total
        out_ref[rows, :] = rounded(head_merge(mixed))
        log_ref[0, chunk : chunk + 1, :] = top + jnp.log(total)
        scores = later


def attend_back_kernel(
    prompt_len,
    near_ref,
    q_ref,
    k_ref,
    v_ref,
    bias_ref,
    log_ref,
    out_ref,
    grad_ref,
    dq_ref,
    first_ref,
    second_ref,
    near_out_ref,
    own_ref,
    dk_ref,
    dv_ref,
):
    scale = 1.0 / math.sqrt(q_ref.shape[1] // 2)
    half = q_ref.shape[1] // 2
    dk_ref[...] = jnp.zeros_like(dk_ref)
    dv_ref[...] = jnp.zeros_like(dv_ref)
    for chunk in range(q_ref.shape[0] // PROMPT_DEV):
        rows = pl.ds(chunk * PROMPT_DEV, PROMPT_DEV)
        size = chunk_keys(chunk, prompt_len)
        stack = head_stack(q_ref[rows, :] * bf16(scale))
        grad = grad_ref[rows, :]
        grad_stack = head_stack(grad)
        product = (grad.astype(f32) * out_ref[rows, :].astype(f32)).T
        inner = jnp.concatenate(
            [
                jnp.sum(product[:half], axis=0, keepdims=True),
                jnp.sum(product[half:], axis=0, keepdims=True),
            ],
            axis=1,
        )
        keys = k_ref[:size, :]
        scores = chunk_scores(chunk, keys, stack, near_ref[0], bias_ref, prompt_len)
        weights = jnp.exp(scores - log_ref[0, chunk : chunk + 1, :])
        dv_ref[:size, :] += matmul(rounded(weights), grad_stack)
        grad_prob = matmul_nt(v_ref[:size, :], grad_stack)
        grad_score = rounded(weights * (grad_prob - inner))
        dk_ref[:size, :] += matmul(grad_score, stack)
        dq_ref[rows, :] = rounded(head_merge(matmul_tn(keys, grad_score)) * scale)
    start = 0
    for ref in (first_ref, second_ref, near_out_ref, own_ref):
        count = ref.shape[1]
        ref[0] = rounded(dk_ref[start : start + count, :])
        ref[1] = rounded(dv_ref[start : start + count, :])
        start += count


def attend(near_bias, queries, keys, values, bias):
    rows, width = queries.shape
    size = keys.shape[0]
    prompt_len = bias.shape[0]
    lanes = 2 * width // HEADS
    pairs = HEADS // 2
    chunks = rows // PROMPT_DEV
    block = lambda count: pl.BlockSpec((count, lanes), lambda j: (0, j))
    return pl.pallas_call(
        functools.partial(attend_kernel, prompt_len),
        grid=(pairs,),
        in_specs=[
            pl.BlockSpec(memory_space=pltpu.SMEM),
            block(rows),
            block(size),
            block(size),
            pl.BlockSpec((prompt_len, PROMPT_DEV), lambda j: (0, 0)),
        ],
        out_specs=[
            block(rows),
            pl.BlockSpec((1, chunks, 2 * PROMPT_DEV), lambda j: (j, 0, 0)),
        ],
        out_shape=[
            jax.ShapeDtypeStruct((rows, width), bf16),
            jax.ShapeDtypeStruct((pairs, chunks, 2 * PROMPT_DEV), f32),
        ],
        compiler_params=params("arbitrary"),
        cost_estimate=cost(16 * rows * size * width, 4 * (rows + size) * width, rows * size * HEADS),
        name="attend",
    )(near_bias, queries, keys, values, bias)


def attend_back(near_bias, queries, keys, values, bias, log_total, attended, grad):
    rows, width = queries.shape
    size = keys.shape[0]
    prompt_len = bias.shape[0]
    lanes = 2 * width // HEADS
    pairs = HEADS // 2
    chunks = rows // PROMPT_DEV
    block = lambda count: pl.BlockSpec((count, lanes), lambda j: (0, j))
    counts = (prompt_len // 2, prompt_len // 2, CONT_DEV, CONT_DEV)
    return pl.pallas_call(
        functools.partial(attend_back_kernel, prompt_len),
        grid=(pairs,),
        in_specs=[
            pl.BlockSpec(memory_space=pltpu.SMEM),
            block(rows),
            block(size),
            block(size),
            pl.BlockSpec((prompt_len, PROMPT_DEV), lambda j: (0, 0)),
            pl.BlockSpec((1, chunks, 2 * PROMPT_DEV), lambda j: (j, 0, 0)),
            block(rows),
            block(rows),
        ],
        out_specs=[block(rows)]
        + [pl.BlockSpec((2, count, lanes), lambda j: (0, 0, j)) for count in counts],
        out_shape=[jax.ShapeDtypeStruct((rows, width), bf16)]
        + [jax.ShapeDtypeStruct((2, count, width), bf16) for count in counts],
        scratch_shapes=[pltpu.VMEM((size, lanes), f32), pltpu.VMEM((size, lanes), f32)],
        compiler_params=params("arbitrary"),
        cost_estimate=cost(40 * rows * size * width, 8 * (rows + size) * width, rows * size * HEADS),
        name="attend_back",
    )(near_bias, queries, keys, values, bias, log_total, attended, grad)


def local(
    tokens_in,
    cotangent,
    hash_ids,
    norm1_gain,
    norm1_bias,
    w_query,
    w_key,
    w_value,
    w_output,
    norm2_gain,
    norm2_bias,
    expert_in,
    expert_out,
):
    row_count, width = tokens_in.shape
    experts = lax.axis_size("expert")
    groups = lax.axis_size("group")
    position = lax.axis_index("expert")
    group = lax.axis_index("group")
    capacity = 2 * row_count // experts
    slots = experts * capacity
    tied = lax.optimization_barrier

    def all_exchanged(values):
        return lax.all_to_all(values, "expert", split_axis=0, concat_axis=0, tiled=True)

    def exchanged(values):
        got = all_exchanged(values.reshape(experts, capacity, width))
        return got.reshape(slots, width)

    near_tokens = lax.ppermute(
        tokens_in[PROMPT_DEV:], "expert", [(i, i + 1) for i in range(0, experts, 2)]
    )
    prompts, prompt_ids, near_tokens, last_tokens = gather_relative(
        tokens_in[:PROMPT_DEV], "expert", near_tokens
    )
    ids = jnp.broadcast_to(rounded(hash_ids), (row_count, 128))
    all_cot = lax.all_gather(jnp.concatenate([cotangent, ids], axis=1), "group")

    row_index = jnp.arange(row_count, dtype=jnp.int32)
    lower = rounded(row_index[:, None] >= row_index[None, :])

    routed = rounded(hash_ids == jnp.arange(experts, dtype=jnp.int32)[None, :])
    running = matmul(lower, routed)
    rank = (jnp.sum(running * routed.astype(f32), axis=-1) - 1.0).astype(jnp.int32)
    slot = hash_ids[:, 0] * capacity + rank
    spread = rounded(slot[None, :] == jnp.arange(slots, dtype=jnp.int32)[:, None])

    cot_sent, _ = tied((matmul(spread, cotangent, bf16), last_tokens))
    cot = {0: exchanged(cot_sent)}
    others_in, queries, keys, values = project(
        prompts + [near_tokens, tokens_in[PROMPT_DEV:]],
        norm1_gain,
        norm1_bias,
        w_query,
        w_key,
        w_value,
    )
    block_pos = jnp.stack([(position ^ r) * PROMPT_DEV for r in prompt_ids])
    prompt_pos = jnp.arange(PROMPT_DEV, dtype=jnp.int32)
    key_pos = (block_pos[:, None] + prompt_pos[None, :]).reshape(-1)
    query_pos = position * PROMPT_DEV + row_index[:PROMPT_DEV]
    bias = jnp.where(key_pos[:, None] <= query_pos[None, :], f32(0.0), f32(masked_score))
    near_bias = jnp.where(position % 2 == 1, f32(0.0), f32(masked_score))[None]
    attended, log_total = attend(near_bias, queries, keys, values, bias)

    residual = tokens_in.astype(f32) + matmul(attended, w_output)
    ffn_in = rounded(normalize(residual, norm2_gain, norm2_bias)[0])
    rows = exchanged(matmul(spread, ffn_in, bf16))
    all_numbers = all_cot[:, :, width].astype(jnp.int32)[:, None]
    numbers = lambda masks: jnp.stack([group ^ mask for mask in masks])
    near_sent = spread_rows(numbers([1]), all_numbers, all_cot, experts)
    grad_hidden = expert_back(cot[0], expert_out)
    rows, grad_hidden, near_sent = tied((rows, grad_hidden, near_sent))
    all_rows = lax.all_gather(rows, "group")
    cot[1] = all_exchanged(near_sent)
    hidden, grad_pre, grad_rows = expert_front(rows, grad_hidden, expert_in)
    grad_rows, hidden, cot[1] = tied((grad_rows, hidden, cot[1]))
    grad_got = exchanged(grad_rows)
    produced = expert_produce(hidden, expert_out)
    far_sent = spread_rows(numbers(range(2, groups)), all_numbers, all_cot, experts, produced)
    far_sent, grad_got = tied((far_sent, grad_got))
    far_got = all_exchanged(far_sent)

    grad_resid, grad_attn, grad_attended, sums2 = resid_back(
        grad_got, spread, residual, norm2_gain, cotangent, w_output
    )
    grad_queries, back_first, back_second, back_near, back_own = attend_back(
        near_bias, queries, keys, values, bias, log_total, attended, grad_attended
    )
    backs = (back_first, back_second, back_near, back_own, grad_queries)
    prompt_marks = []
    prompt_sums = scatter_relative(back_first, back_second, "expert", prompt_marks)
    prompt_sent = next(prompt_sums)
    near_back = lax.ppermute(
        back_near, "expert", [(i + 1, i) for i in range(0, experts, 2)]
    )
    weights = weight_parts(
        (position & 1)[None],
        attended,
        others_in,
        grad_attn,
        grad_queries,
        (back_first, back_second, back_near, back_own),
        groups,
        experts,
    )
    place, _ = tied((group[None], weights))
    own_part = own_out(place, groups, hidden, cot[0])
    weights, prompt_sent, near_back, far_got, own_part = tied(
        (weights, prompt_sent, near_back, far_got, own_part)
    )
    marks = []
    weight_sums = weight_chain(*weights, marks)
    weight_sent = next(weight_sums)
    prompt_sent, prompt_back = moved_on(prompt_sums, prompt_sent)
    far_late, _ = tied((far_got, list(prompt_marks[-1].values())))
    result_got = far_late[:, 0].reshape(slots, width)
    result = rounded(residual + matmul_tn(spread, result_got))
    weight_sent, prompt_sent, result = tied((weight_sent, prompt_sent, result))
    weight_sent, _ = moved_on(weight_sums, weight_sent)
    number, _ = tied((numbers(range(groups)), marks[-1]))
    operands = (expert_in, expert_out, (rows, grad_pre), all_rows, cot[1], far_got)
    in_first, *hidden_first = in_sums(number, 0, *operands)
    over_group = lambda values: lax.all_to_all(
        values, "group", split_axis=0, concat_axis=0, tiled=True
    )
    got_first = over_group(in_first)
    weight_sent, prompt_sent, _ = tied((weight_sent, prompt_sent, in_first))
    weight_sent, _ = moved_on(weight_sums, weight_sent)
    prompt_sent, prompt_back = moved_on(prompt_sums, prompt_sent)
    number, _ = tied((number, marks[-1]))
    in_second, *hidden_second = in_sums(number, 1, *operands)
    got_first, in_second, prompt_sent, weight_sent = tied(
        (got_first, in_second, prompt_sent, weight_sent)
    )
    got_second = over_group(in_second)
    prompt_sent, weight_sent, _ = tied((prompt_sent, weight_sent, in_second))
    while prompt_sent is not None:
        prompt_sent, prompt_back = moved_on(prompt_sums, prompt_sent)
    grad_tokens, sums1 = input_back(
        prompt_back,
        back_own,
        near_back,
        grad_queries,
        w_query,
        w_key,
        w_value,
        tokens_in,
        norm1_gain,
        grad_resid,
    )
    weight_sent, own_part, sums1 = tied((weight_sent, own_part, sums1))
    weight_sent, weight_grads = moved_on(weight_sums, weight_sent)
    grad_expert_out = out_sums(own_part, cot[1], far_got, hidden_first + hidden_second)
    vectors = jnp.concatenate([sums1, sums2])
    vectors, got_second, grad_expert_out, weight_sent = tied(
        (vectors, got_second, grad_expert_out, weight_sent)
    )
    vectors = vector_sums(vectors)
    while weight_sent is not None:
        weight_sent, weight_grads = moved_on(weight_sums, weight_sent)
    grad_expert_in = lay_out([got_first, got_second])
    grad_w_output, grad_w_query, grad_w_key, grad_w_value = weight_grads
    return (
        result,
        grad_tokens,
        vectors[0],
        vectors[1],
        grad_w_query,
        grad_w_key,
        grad_w_value,
        grad_w_output,
        vectors[2],
        vectors[3],
        grad_expert_in,
        grad_expert_out,
    )


def solution(mesh):
    both = ("group", "expert")
    return jax.shard_map(
        local,
        mesh=mesh,
        in_specs=(
            P(both, None),
            P(both, None),
            P(both, None),
            P(),
            P(),
            P(),
            P(),
            P(),
            P(),
            P(),
            P(),
            P("expert", None, None),
            P("expert", None, None),
        ),
        out_specs=(
            P(both, None),
            P(both, None),
            P(both),
            P(both),
            P(both, None),
            P(both, None),
            P(both, None),
            P(both, None),
            P(both),
            P(both),
            P("expert", "group", None),
            P("expert", "group", None),
        ),
        check_vma=False,
    )
```

```python
import functools
import math

import jax
import jax.numpy as jnp
from jax import lax
from jax.experimental import pallas as pl
from jax.experimental.pallas import tpu as pltpu
from jax.sharding import PartitionSpec as P

HEADS = 16
PROMPT_DEV = 128
CONT_DEV = 384


norm_eps = 1e-05
masked_score = -1e30
bf16 = jnp.bfloat16
f32 = jnp.float32
MIB = 1 << 20
share = 0.05


def swapped(block, axis, mask):
    return lax.ppermute(block, axis, [(i, i ^ mask) for i in range(lax.axis_size(axis))])


def rounded(values):
    return values.astype(bf16)


def normalize(values, gain, shift):
    average = jnp.mean(values, axis=-1, keepdims=True)
    centered = values - average
    variance = jnp.mean(centered * centered, axis=-1, keepdims=True)
    inverse = lax.rsqrt(variance + norm_eps)
    normed = centered * inverse
    return (normed * gain + shift, normed, inverse)


def norm_back(grad_out, gain, normed, inverse):
    scaled = grad_out * gain
    first_mean = jnp.mean(scaled, axis=-1, keepdims=True)
    second = jnp.mean(scaled * normed, axis=-1, keepdims=True)
    return inverse * (scaled - first_mean - normed * second)


def matmul(a, b, kind=f32):
    return jnp.dot(a, b, preferred_element_type=f32).astype(kind)


def matmul_nt(a, b, kind=f32):
    return lax.dot_general(a, b, (((1,), (1,)), ((), ())), preferred_element_type=f32).astype(kind)


def matmul_tn(a, b, kind=f32):
    return lax.dot_general(a, b, (((0,), (0,)), ((), ())), preferred_element_type=f32).astype(kind)


def outer_bits(size):
    return range(size.bit_length() - 2, 0, -1)


def gather_relative(block, axis, more):
    size = lax.axis_size(axis)
    pieces = {0: block}
    ready, last = [0], []
    while ready:
        fresh = {}
        for r in ready:
            for bit in outer_bits(size):
                if r ^ (1 << bit) not in pieces and r ^ (1 << bit) not in fresh:
                    fresh[r ^ (1 << bit)] = swapped(pieces[r], axis, 1 << bit)
        fresh, more = lax.optimization_barrier((fresh, more))
        pieces.update(fresh)
        ready, last = list(fresh), list(fresh.values()) or last
    near = sorted(pieces)
    for r in near:
        pieces[r ^ 1] = swapped(pieces[r], axis, 1)
    order = near + [r ^ 1 for r in near]
    return [pieces[r] for r in order], order, more, last


def scatter_relative(near, far, axis):
    size = lax.axis_size(axis)
    got = yield swapped(far, axis, 1)
    both = added(near, got)
    count = size // 2
    rows = both.shape[1] // count
    pieces = {2 * i: rounded(both[:, i * rows : (i + 1) * rows]) for i in range(count)}
    bits = list(outer_bits(size))
    for level in range(len(bits), 0, -1):
        sent, spans = [], []
        for r in [r for r in sorted(pieces) if bin(r).count("1") == level]:
            ways = [bit for bit in bits if r >> bit & 1]
            if rows % (16 * len(ways)):
                ways = ways[:1]
            part = rows // len(ways)
            piece = pieces.pop(r)
            for i, bit in enumerate(ways):
                span = (i * part, (i + 1) * part)
                sent.append(swapped(piece[:, span[0] : span[1]], axis, 1 << bit))
                spans.append((r ^ (1 << bit), span))
        gots = yield sent
        for r in sorted(pieces):
            total = pieces[r].astype(f32)
            for got, (target, span) in zip(gots, spans):
                if target == r:
                    outside = ((0, 0), (span[0], rows - span[1]), (0, 0))
                    total = total + jnp.pad(got.astype(f32), outside)
            pieces[r] = rounded(total)
    return pieces[0]


def halved(blocks, place, axis, bit):
    own = (lax.axis_index(axis) >> bit) & 1
    return (
        lax.dynamic_index_in_dim(blocks, own, place, keepdims=False),
        lax.dynamic_index_in_dim(blocks, 1 - own, place, keepdims=False),
    )


def added(keep, got):
    return keep.astype(f32) + got.astype(f32)


def places_of(bits, bit, value):
    rest = [other for other in bits if other != bit]
    weight = {other: 1 << (len(bits) - 1 - i) for i, other in enumerate(bits)}
    places = []
    for number in range(1 << len(rest)):
        place = value * weight[bit]
        for i, other in enumerate(rest):
            place = place + (number >> (len(rest) - 1 - i) & 1) * weight[other]
        places.append(place)
    return places


def halve_kernel(lefts, bits, own_ref, *refs):
    sets = len(lefts)
    for k, (left, bit) in enumerate(zip(lefts, bits)):
        keep_ref, got_ref = refs[2 * k : 2 * k + 2]
        outs = refs[2 * sets + 2 * k : 2 * sets + 2 * k + 2]
        own = (own_ref[0] >> bit) & 1
        for ref, value in zip(outs, (own, 1 - own)):
            for i, place in enumerate(places_of(left, bit, value)):
                for j in range(ref.shape[1]):
                    ref[0, j, i] = rounded(added(keep_ref[0, j, place], got_ref[0, j, place]))


def halve(number, states, bits):
    _, groups, count, rows, width = states[0][0].shape
    shape = (2, groups, count // 2, rows, width)
    came = lambda first: pl.BlockSpec(
        (1, groups, count, rows, width), lambda i: (first + i if first else i, 0, 0, 0, 0)
    )
    out = pl.BlockSpec((1, groups, count // 2, rows, width), lambda i: (i, 0, 0, 0, 0))
    size = 2 * math.prod(shape)
    outs = pl.pallas_call(
        functools.partial(halve_kernel, [state[3] for state in states], bits),
        grid=(2,),
        in_specs=[pl.BlockSpec(memory_space=pltpu.SMEM)]
        + [came(state[2]) for state in states for _ in range(2)],
        out_specs=[out] * (2 * len(states)),
        out_shape=[jax.ShapeDtypeStruct(shape, bf16)] * (2 * len(states)),
        compiler_params=params("arbitrary"),
        cost_estimate=cost(2 * size, 12 * size),
        name="halve",
    )(number, *[value for state in states for value in state[:2]])
    return list(zip(outs[::2], outs[1::2]))


def turn_kernel(own_ref, *refs):
    (*sets, own_out_ref, send_ref) = refs
    own = own_ref[0] & 1
    start = 0
    for keep_ref, got_ref in zip(sets[::2], sets[1::2]):
        for i in range(keep_ref.shape[0]):
            for j in range(keep_ref.shape[1] // 2):
                for ref, value in ((own_out_ref, own), (send_ref, 1 - own)):
                    place = 2 * j + value
                    ref[start + i, j] = rounded(added(keep_ref[i, place, 0], got_ref[i, place, 0]))
        start += keep_ref.shape[0]


def turn(number, sets):
    _, groups, _, rows, width = sets[0].shape
    shape = (4, groups // 2, rows, width)
    return pl.pallas_call(
        turn_kernel,
        in_specs=[pl.BlockSpec(memory_space=pltpu.SMEM)]
        + [pl.BlockSpec(memory_space=pltpu.VMEM)] * len(sets),
        out_specs=[pl.BlockSpec(memory_space=pltpu.VMEM)] * 2,
        out_shape=[jax.ShapeDtypeStruct(shape, bf16)] * 2,
        compiler_params=params(),
        cost_estimate=cost(8 * sets[0].size, 8 * sets[0].size),
        name="turn",
    )(number, *sets)


def weight_chain(keep, send, marks):
    bits = list(range(1, lax.axis_size("expert").bit_length() - 1))
    number = lax.axis_index("expert")[None]
    got = yield swapped(send, "expert", 1)
    states = [(keep, got, 0, bits[::-1]), (keep, got, 2, bits[::-1])]
    for pair in zip(bits, bits[::-1]):
        halves = halve(number, states, pair)
        marks.append(halves[0][0])
        gots = yield [swapped(send, "expert", 1 << bit) for bit, (_, send) in zip(pair, halves)]
        states = [
            (keep, got, 0, [other for other in state[3] if other != bit])
            for state, bit, (keep, _), got in zip(states, pair, halves, gots)
        ]
    keep, send = turn(
        lax.axis_index("group")[None], [value for state in states for value in state[:2]]
    )
    marks.append(keep)
    got = yield swapped(send, "group", 1)
    both = added(keep, got)
    bits = list(range(1, lax.axis_size("group").bit_length() - 1))
    both = both.reshape((4,) + (2,) * len(bits) + both.shape[-2:])
    left = bits[::-1]
    for bit in bits:
        keep, send = halved(rounded(both), 1 + left.index(bit), "group", bit)
        left.remove(bit)
        got = yield swapped(send, "group", 1 << bit)
        both = added(keep, got)
    return [both[i] for i in range(both.shape[0])]


def moved_on(chain, came):
    try:
        return chain.send(came), None
    except StopIteration as stop:
        return None, stop.value


def vector_sums(vectors):
    axes = ("group", "expert")
    devices = lax.axis_size("group") * lax.axis_size("expert")
    count, width = vectors.shape
    pieces = vectors.reshape(count, devices, width // devices).swapaxes(0, 1)
    got = lax.all_to_all(pieces, axes, split_axis=0, concat_axis=0, tiled=True)
    return jnp.sum(got, axis=0)


def params(*semantics):
    return pltpu.CompilerParams(dimension_semantics=semantics, vmem_limit_bytes=60 * MIB)


def cost(flops, total_bytes, exps=0):
    return pl.CostEstimate(
        flops=int(flops * share), bytes_accessed=int(total_bytes * share), transcendentals=int(exps * share)
    )


def logistic(values):
    return 0.5 * jnp.tanh(0.5 * values) + 0.5


def back_kernel(cot_ref, wout_ref, out_ref):
    out_ref[...] = matmul_nt(cot_ref[...], wout_ref[0], bf16)


def expert_back(cot, expert_out):
    count, width = cot.shape
    ff = expert_out.shape[1]
    block = 1024
    return pl.pallas_call(
        back_kernel,
        grid=(ff // block,),
        in_specs=[
            pl.BlockSpec((count, width), lambda j: (0, 0)),
            pl.BlockSpec((1, block, width), lambda j: (0, j, 0)),
        ],
        out_specs=pl.BlockSpec((count, block), lambda j: (0, j)),
        out_shape=jax.ShapeDtypeStruct((count, ff), bf16),
        compiler_params=params("arbitrary"),
        cost_estimate=cost(2 * count * width * ff, 2 * count * ff + 2 * width * ff),
        name="expert_back",
    )(cot, expert_out)


def front_kernel(parts, rows_ref, gh_ref, win_ref, hidden_ref, pre_ref, out_ref, acc_ref):
    step = pl.program_id(0)
    count = rows_ref.shape[0] // parts

    @pl.when(step == 0)
    def _():
        acc_ref[...] = jnp.zeros_like(acc_ref)

    first = lambda i: matmul(rows_ref[i * count : (i + 1) * count, :], win_ref[0])
    pre = first(0)
    for i in range(parts):
        later = first(i + 1) if i + 1 < parts else None
        here = pl.ds(i * count, count)
        sig = logistic(pre)
        hidden = pre * sig
        hidden_ref[here, :] = rounded(hidden)
        grad_pre = rounded(gh_ref[here, :].astype(f32) * sig * (1.0 + pre - hidden))
        pre_ref[here, :] = grad_pre
        acc_ref[here, :] += matmul_nt(grad_pre, win_ref[0])
        pre = later

    @pl.when(step == pl.num_programs(0) - 1)
    def _():
        out_ref[...] = rounded(acc_ref[...])


def expert_front(rows, grad_hidden, expert_in):
    count, width = rows.shape
    ff = expert_in.shape[2]
    block = 1024
    whole = pl.BlockSpec((count, width), lambda j: (0, 0))
    part = pl.BlockSpec((count, block), lambda j: (0, j))
    return pl.pallas_call(
        functools.partial(front_kernel, 4),
        grid=(ff // block,),
        in_specs=[whole, part, pl.BlockSpec((1, width, block), lambda j: (0, 0, j))],
        out_specs=[part, part, whole],
        out_shape=[
            jax.ShapeDtypeStruct((count, ff), bf16),
            jax.ShapeDtypeStruct((count, ff), bf16),
            jax.ShapeDtypeStruct((count, width), bf16),
        ],
        scratch_shapes=[pltpu.VMEM((count, width), f32)],
        compiler_params=params("arbitrary"),
        cost_estimate=cost(4 * count * width * ff, 6 * count * ff + 2 * width * ff, count * ff),
        name="expert_front",
    )(rows, grad_hidden, expert_in)


def produce_kernel(hidden_ref, wout_ref, out_ref, acc_ref):
    step = pl.program_id(0)
    part = matmul(hidden_ref[...], wout_ref[0])

    @pl.when(step == 0)
    def _():
        acc_ref[...] = part

    @pl.when(step > 0)
    def _():
        acc_ref[...] += part

    @pl.when(step == pl.num_programs(0) - 1)
    def _():
        out_ref[...] = rounded(acc_ref[...])


def expert_produce(hidden, expert_out):
    count, ff = hidden.shape
    width = expert_out.shape[2]
    block = 1024
    return pl.pallas_call(
        produce_kernel,
        grid=(ff // block,),
        in_specs=[
            pl.BlockSpec((count, block), lambda j: (0, j)),
            pl.BlockSpec((1, block, width), lambda j: (0, j, 0)),
        ],
        out_specs=pl.BlockSpec((count, width), lambda j: (0, 0)),
        out_shape=jax.ShapeDtypeStruct((count, width), bf16),
        scratch_shapes=[pltpu.VMEM((count, width), f32)],
        compiler_params=params("arbitrary"),
        cost_estimate=cost(2 * count * width * ff, 2 * count * ff + 2 * width * ff),
        name="expert_produce",
    )(hidden, expert_out)


def in_kernel(
    half, number_ref, own_rows_ref, own_pre_ref, win_hbm, wout_hbm, rows_hbm, near_hbm, far_hbm,
    in_ref, near_out, far_out, in_sum, win_ref, wout_ref, rows_ref, cot_ref, hidden_ref,
    weight_sems, shard_sems, out_sems,
):
    shards, count, _ = rows_ref.shape
    block = win_ref.shape[1]
    place = pl.multiple_of((2 * number_ref[0] + half) * block, block)
    weights = [
        pltpu.make_async_copy(win_hbm.at[0, :, pl.ds(place, block)], win_ref, weight_sems.at[0]),
        pltpu.make_async_copy(wout_hbm.at[0, pl.ds(place, block), :], wout_ref, weight_sems.at[1]),
    ]
    copies, outs = [], []
    for i in range(shards):
        cot = near_hbm.at[:, 0] if i == 0 else far_hbm.at[:, i]
        rows = rows_hbm.at[number_ref[1 + i]]
        copies.append(
            [
                pltpu.make_async_copy(rows, rows_ref.at[i], shard_sems.at[i, 0]),
                pltpu.make_async_copy(cot, cot_ref.at[i], shard_sems.at[i, 1]),
            ]
        )
        out = near_out if i == 0 else far_out.at[i - 1]
        outs.append(pltpu.make_async_copy(hidden_ref.at[i], out, out_sems.at[i]))
    for copy in weights + [copy for pair in copies for copy in pair]:
        copy.start()
    in_sum[...] = matmul_tn(own_rows_ref[...], own_pre_ref[...])
    for copy in weights:
        copy.wait()
    for i in range(shards):
        for copy in copies[i]:
            copy.wait()
        rows = rows_ref[i]
        pre = matmul(rows, win_ref[...])
        grad_hidden = matmul_nt(cot_ref[i].reshape(rows.shape), wout_ref[...])
        sig = logistic(pre)
        hidden = pre * sig
        hidden_ref[i] = rounded(hidden)
        outs[i].start()
        grad_pre = rounded(grad_hidden * sig * (1.0 + pre - hidden))
        in_sum[...] += matmul_tn(rows, grad_pre)
    in_ref[...] = rounded(in_sum[...]).reshape(in_ref.shape)
    for copy in outs:
        copy.wait()


def in_sums(number, half, expert_in, expert_out, own, rows, near, far):
    groups, count, width = rows.shape
    sources, _, slots, _ = near.shape
    part = expert_in.shape[2] // groups
    block = part // 2
    shards = groups - 1
    there = pl.BlockSpec(memory_space=pl.ANY)
    return pl.pallas_call(
        functools.partial(in_kernel, half),
        grid_spec=pltpu.PrefetchScalarGridSpec(
            num_scalar_prefetch=1,
            grid=(1,),
            in_specs=[
                pl.BlockSpec((count, width), lambda j, w: (0, 0)),
                pl.BlockSpec((count, block), lambda j, w: (0, 2 * w[0] + half)),
            ]
            + [there] * 5,
            out_specs=[
                pl.BlockSpec((groups, width // groups, block), lambda j, w: (0, 0, 0)),
                there,
                there,
            ],
            scratch_shapes=[
                pltpu.VMEM((width, block), f32),
                pltpu.VMEM((width, block), bf16),
                pltpu.VMEM((block, width), bf16),
                pltpu.VMEM((shards, count, width), bf16),
                pltpu.VMEM((shards, sources, slots, width), bf16),
                pltpu.VMEM((shards, count, block), bf16),
                pltpu.SemaphoreType.DMA((2,)),
                pltpu.SemaphoreType.DMA((shards, 2)),
                pltpu.SemaphoreType.DMA((shards,)),
            ],
        ),
        out_shape=[
            jax.ShapeDtypeStruct((groups, width // groups, block), bf16),
            jax.ShapeDtypeStruct((count, block), bf16),
            jax.ShapeDtypeStruct((groups - 2, count, block), bf16),
        ],
        compiler_params=params("arbitrary"),
        cost_estimate=cost(6 * count * width * block * groups, 16e6, count * block * groups),
        name="in_sums",
    )(number, *own, expert_in, expert_out, rows, near, far)


def own_kernel(_, hidden_ref, cot_ref, out_ref):
    out_ref[...] = matmul_tn(hidden_ref[...], cot_ref[...])


def own_out(number, groups, hidden, cot):
    count, width = cot.shape
    part = hidden.shape[1] // groups
    block = part // 2
    return pl.pallas_call(
        own_kernel,
        grid_spec=pltpu.PrefetchScalarGridSpec(
            num_scalar_prefetch=1,
            grid=(2,),
            in_specs=[
                pl.BlockSpec((count, block), lambda j, w: (0, 2 * w[0] + j)),
                pl.BlockSpec((count, width), lambda j, w: (0, 0)),
            ],
            out_specs=pl.BlockSpec((block, width), lambda j, w: (j, 0)),
        ),
        out_shape=jax.ShapeDtypeStruct((part, width), f32),
        compiler_params=params("arbitrary"),
        cost_estimate=cost(2 * count * width * part, 8e6),
        name="own_out",
    )(number, hidden, cot)


def out_kernel(own_ref, near_ref, far_ref, *refs):
    out_ref, total = refs[-2:]
    hiddens = refs[:-2]
    block = total.shape[0] // 2
    count = hiddens[0].shape[0]
    step = pl.program_id(0)

    @pl.when(step == 0)
    def _():
        near = near_ref[...].reshape(count, -1)
        for half in range(2):
            here = pl.ds(half * block, block)
            total[here, :] = own_ref[here, :] + matmul_tn(hiddens[2 * half][...], near)

    far = far_ref[...].reshape(count, -1)
    for half in range(2):
        here = pl.ds(half * block, block)
        total[here, :] += matmul_tn(hiddens[2 * half + 1][0], far)

    @pl.when(step == pl.num_programs(0) - 1)
    def _():
        out_ref[0] = total[...]


def out_sums(own, near, far, hiddens):
    part, width = own.shape
    count = hiddens[0].shape[0]
    sources, _, slots, _ = near.shape
    steps = hiddens[1].shape[0]
    near_hidden = pl.BlockSpec((count, part // 2), lambda j: (0, 0))
    far_hidden = pl.BlockSpec((1, count, part // 2), lambda j: (j, 0, 0))
    return pl.pallas_call(
        out_kernel,
        grid=(steps,),
        in_specs=[
            pl.BlockSpec((part, width), lambda j: (0, 0)),
            pl.BlockSpec((sources, 1, slots, width), lambda j: (0, 0, 0, 0)),
            pl.BlockSpec((sources, 1, slots, width), lambda j: (0, 1 + j, 0, 0)),
        ]
        + [near_hidden, far_hidden] * 2,
        out_specs=pl.BlockSpec((1, part, width), lambda j: (0, 0, 0)),
        out_shape=jax.ShapeDtypeStruct((1, part, width), f32),
        scratch_shapes=[pltpu.VMEM((part, width), f32)],
        compiler_params=params("arbitrary"),
        cost_estimate=cost(2 * count * width * part * (steps + 1), 16e6),
        name="out_sums",
    )(own, near, far, *hiddens)


def lay_kernel(*refs):
    gots, out_ref = refs[:-1], refs[-1]
    block = gots[0].shape[2]
    for i in range(gots[0].shape[0]):
        for j, ref in enumerate(gots):
            start = (i * len(gots) + j) * block
            out_ref[0, :, start : start + block] = ref[i].astype(f32)


def lay_out(gots):
    groups, rows, block = gots[0].shape
    tall = 64
    width = groups * block * len(gots)
    return pl.pallas_call(
        lay_kernel,
        grid=(rows // tall,),
        in_specs=[pl.BlockSpec((groups, tall, block), lambda j: (0, j, 0))] * len(gots),
        out_specs=pl.BlockSpec((1, tall, width), lambda j: (0, j, 0)),
        out_shape=jax.ShapeDtypeStruct((1, rows, width), f32),
        compiler_params=params("arbitrary"),
        cost_estimate=cost(rows * width, 6 * rows * width),
        name="lay_out",
    )(*gots)


def spread_kernel(first, _, ids_ref, values_ref, *refs):
    out_ref = refs[-1]
    experts, _, capacity, width = out_ref.shape

    def spread():
        rows = ids_ref.shape[2]
        ids = ids_ref[0]
        number = lax.broadcasted_iota(jnp.int32, (experts, rows), 0)
        routed = jnp.where(number == ids, f32(1.0), f32(0.0))
        square = (rows, rows)
        before = lax.broadcasted_iota(jnp.int32, square, 0) <= lax.broadcasted_iota(
            jnp.int32, square, 1
        )
        running = matmul(rounded(routed), rounded(jnp.where(before, f32(1.0), f32(0.0))))
        rank = jnp.sum(running * routed, axis=0, keepdims=True).astype(jnp.int32) - 1
        slot = ids * capacity + rank
        places = lax.broadcasted_iota(jnp.int32, (experts * capacity, rows), 0)
        onehot = rounded(jnp.where(places == slot, f32(1.0), f32(0.0)))
        out = matmul(onehot, values_ref[0, :, :width], bf16)
        out_ref[...] = out.reshape(out_ref.shape)

    if first:
        step = pl.program_id(0)

        @pl.when(step == 0)
        def _():
            out_ref[...] = refs[0][...].reshape(out_ref.shape)

        pl.when(step > 0)(spread)
    else:
        spread()


def spread_rows(numbers, ids, values, experts, first=None):
    _, rows, columns = values.shape
    width = columns - 128
    capacity = 2 * rows // experts
    start = 0 if first is None else 1
    count = numbers.shape[0] + start
    which = lambda j, w: w[jnp.maximum(j - start, 0)]
    specs = [
        pl.BlockSpec((1, 1, rows), lambda j, w: (which(j, w), 0, 0)),
        pl.BlockSpec((1, rows, columns), lambda j, w: (which(j, w), 0, 0)),
    ]
    operands = [ids, values]
    if start:
        specs.append(pl.BlockSpec(first.shape, lambda j, w: (0, 0)))
        operands.append(first)
    return pl.pallas_call(
        functools.partial(spread_kernel, start),
        grid_spec=pltpu.PrefetchScalarGridSpec(
            num_scalar_prefetch=1,
            grid=(count,),
            in_specs=specs,
            out_specs=pl.BlockSpec((experts, 1, capacity, width), lambda j, w: (0, j, 0, 0)),
        ),
        out_shape=jax.ShapeDtypeStruct((experts, count, capacity, width), bf16),
        compiler_params=params("arbitrary"),
        cost_estimate=cost(2 * count * experts * capacity * rows * width, 8e6),
        name="spread_rows",
    )(numbers, *operands)


def project_kernel(count, gain_ref, bias_ref, wq_ref, wk_ref, wv_ref, *refs):
    pieces, (in_ref, q_ref, k_ref, v_ref, scratch) = refs[:count], refs[count:]

    @pl.when(pl.program_id(0) == 0)
    def _():
        start = 0
        for ref in pieces:
            end = start + ref.shape[0]
            values = normalize(ref[...].astype(f32), gain_ref[...], bias_ref[...])[0]
            scratch[start:end, :] = rounded(values)
            start = end
        in_ref[...] = scratch[...]

    first, last = pieces[0].shape[0], pieces[-1].shape[0]
    size = scratch.shape[0]
    q_ref[:first, :] = matmul(scratch[:first, :], wq_ref[...], bf16)
    q_ref[first:, :] = matmul(scratch[size - last :, :], wq_ref[...], bf16)
    k_ref[...] = matmul(scratch[...], wk_ref[...], bf16)
    v_ref[...] = matmul(scratch[...], wv_ref[...], bf16)


def project(pieces, gain, shift, w_query, w_key, w_value):
    width = gain.shape[0]
    size = sum(p.shape[0] for p in pieces)
    own = pieces[0].shape[0] + pieces[-1].shape[0]
    block = 256
    whole = lambda rows: pl.BlockSpec((rows, width), lambda j: (0, 0))
    weights = pl.BlockSpec((width, block), lambda j: (0, j))
    columns = lambda rows: pl.BlockSpec((rows, block), lambda j: (0, j))
    return pl.pallas_call(
        functools.partial(project_kernel, len(pieces)),
        grid=(width // block,),
        in_specs=[whole(1), whole(1)] + [weights] * 3 + [whole(p.shape[0]) for p in pieces],
        out_specs=[whole(size), columns(own), columns(size), columns(size)],
        out_shape=[jax.ShapeDtypeStruct((rows, width), bf16) for rows in (size, own, size, size)],
        scratch_shapes=[pltpu.VMEM((size, width), bf16)],
        compiler_params=params("arbitrary"),
        cost_estimate=cost(4 * size * width * width, 8 * size * width + 4 * width * width),
        name="project",
    )(gain[None], shift[None], w_query, w_key, w_value, *pieces)


def weights_kernel(odd_ref, *refs):
    attended_ref, others_ref, grad_ref, dq_ref, *backs = refs[:-2]
    keep_ref, send_ref = refs[-2:]
    size = others_ref.shape[0]
    totals = [
        matmul_tn(attended_ref[...], grad_ref[...]),
        matmul_tn(others_ref[:PROMPT_DEV, :], dq_ref[:PROMPT_DEV, :])
        + matmul_tn(others_ref[size - CONT_DEV :, :], dq_ref[PROMPT_DEV:, :]),
    ]
    for i in range(2):
        total, start = None, 0
        for ref in backs:
            count = ref.shape[1]
            part = matmul_tn(others_ref[start : start + count, :], ref[i])
            total = part if total is None else total + part
            start += count
        totals.append(total)
    half, rows = keep_ref.shape[2:4]

    def put(even_ref, odd_ref):
        for i, total in enumerate(totals):
            for j in range(half):
                start = 2 * j * rows
                even_ref[i, 0, j] = rounded(total[start : start + rows])
                odd_ref[i, 0, j] = rounded(total[start + rows : start + 2 * rows])

    @pl.when(odd_ref[0] == 0)
    def _():
        put(keep_ref, send_ref)

    @pl.when(odd_ref[0] != 0)
    def _():
        put(send_ref, keep_ref)


def weight_parts(odd, attended, others_in, grad_attn, grad_queries, backs, groups, experts):
    width = attended.shape[1]
    part = width // groups
    rows = part // experts
    left = lambda m: pl.BlockSpec((m.shape[0], part), lambda j: (0, j))
    whole = lambda m: pl.BlockSpec(m.shape, lambda j: (0,) * m.ndim)
    lefts, rights = [attended, others_in], [grad_attn, grad_queries, *backs]
    shape = (4, groups, experts // 2, rows, width)
    out = pl.BlockSpec((4, 1) + shape[2:], lambda j: (0, j, 0, 0, 0))
    return pl.pallas_call(
        weights_kernel,
        grid=(groups,),
        in_specs=[pl.BlockSpec(memory_space=pltpu.SMEM)]
        + [left(m) for m in lefts]
        + [whole(m) for m in rights],
        out_specs=[out, out],
        out_shape=[jax.ShapeDtypeStruct(shape, bf16)] * 2,
        compiler_params=params("arbitrary"),
        cost_estimate=cost(10e9, 30e6),
        name="weight_parts",
    )(odd, *lefts, *rights)


def resid_back_kernel(
    got_ref, spread_ref, resid_ref, gain_ref, cot_ref, wo_ref, grad_ref, attn_ref, attended_ref, sums_ref
):
    grad = matmul_tn(spread_ref[...], got_ref[...])
    _, normed, inverse = normalize(resid_ref[...], 1.0, 0.0)
    sums = jnp.concatenate(
        [jnp.sum(grad * normed, axis=0, keepdims=True), jnp.sum(grad, axis=0, keepdims=True)]
    )

    @pl.when(pl.program_id(0) == 0)
    def _():
        sums_ref[...] = sums

    @pl.when(pl.program_id(0) > 0)
    def _():
        sums_ref[...] += sums

    total = cot_ref[...].astype(f32) + norm_back(grad, gain_ref[...], normed, inverse)
    grad_ref[...] = total
    attn_ref[...] = rounded(total)
    attended_ref[...] = matmul_nt(rounded(total), wo_ref[...], bf16)


def resid_back(got, spread, residual, gain, cotangent, w_output):
    rows, width = residual.shape
    slots = got.shape[0]
    block = 256
    whole = lambda count: pl.BlockSpec((count, width), lambda j: (0, 0))
    part = pl.BlockSpec((block, width), lambda j: (j, 0))
    return pl.pallas_call(
        resid_back_kernel,
        grid=(rows // block,),
        in_specs=[
            whole(slots),
            pl.BlockSpec((slots, block), lambda j: (0, j)),
            part,
            whole(1),
            part,
            whole(width),
        ],
        out_specs=[part, part, part, whole(2)],
        out_shape=[
            jax.ShapeDtypeStruct((rows, width), f32),
            jax.ShapeDtypeStruct((rows, width), bf16),
            jax.ShapeDtypeStruct((rows, width), bf16),
            jax.ShapeDtypeStruct((2, width), f32),
        ],
        compiler_params=params("arbitrary"),
        cost_estimate=cost(2 * rows * width * (slots + width), 16 * rows * width),
        name="resid_back",
    )(got, spread, residual, gain[None], cotangent, w_output)


def input_back_kernel(
    prompt_ref, own_ref, near_ref, dq_ref, wq_ref, wk_ref, wv_ref, x_ref, gain_ref, resid_ref,
    out_ref, sums_ref, dk_ref, dv_ref,
):
    step = pl.program_id(0)
    block = dk_ref.shape[0]
    count = prompt_ref.shape[1]

    def put(first):
        for i, ref in enumerate((dk_ref, dv_ref)):
            start, size = (0, block - count) if first else (block - count, block)
            if first:
                ref[:count, :] = prompt_ref[i]
            here = pl.ds(start, size)
            ref[block - size :, :] = rounded(added(own_ref[i, here, :], near_ref[i, here, :]))

    pl.when(step == 0)(lambda: put(True))
    pl.when(step > 0)(lambda: put(False))
    grad = matmul_nt(dq_ref[...], wq_ref[...])
    grad = grad + matmul_nt(dk_ref[...], wk_ref[...])
    grad = grad + matmul_nt(dv_ref[...], wv_ref[...])
    _, normed, inverse = normalize(x_ref[...].astype(f32), 1.0, 0.0)
    sums = jnp.concatenate(
        [jnp.sum(grad * normed, axis=0, keepdims=True), jnp.sum(grad, axis=0, keepdims=True)]
    )

    @pl.when(step == 0)
    def _():
        sums_ref[...] = sums

    @pl.when(step > 0)
    def _():
        sums_ref[...] += sums

    out_ref[...] = rounded(resid_ref[...] + norm_back(grad, gain_ref[...], normed, inverse))


def input_back(prompt, own, near, grad_queries, w_query, w_key, w_value, tokens, gain, grad_resid):
    rows, width = tokens.shape
    block = rows // 2
    whole = lambda count: pl.BlockSpec((count, width), lambda j: (0, 0))
    part = pl.BlockSpec((block, width), lambda j: (j, 0))
    pair = lambda count: pl.BlockSpec((2, count, width), lambda j: (0, 0, 0))
    return pl.pallas_call(
        input_back_kernel,
        grid=(rows // block,),
        in_specs=[
            pair(PROMPT_DEV),
            pair(CONT_DEV),
            pair(CONT_DEV),
            part,
            whole(width),
            whole(width),
            whole(width),
            part,
            whole(1),
            part,
        ],
        out_specs=[part, whole(2)],
        out_shape=[
            jax.ShapeDtypeStruct((rows, width), bf16),
            jax.ShapeDtypeStruct((2, width), f32),
        ],
        scratch_shapes=[pltpu.VMEM((block, width), bf16)] * 2,
        compiler_params=params("arbitrary"),
        cost_estimate=cost(6 * rows * width * width, 20 * rows * width),
        name="input_back",
    )(prompt, own, near, grad_queries, w_query, w_key, w_value, tokens, gain[None], grad_resid)


def head_stack(block):
    first = lax.broadcasted_iota(jnp.int32, block.shape, 1) < block.shape[1] // 2
    zero = jnp.zeros_like(block)
    return jnp.concatenate([jnp.where(first, block, zero), jnp.where(first, zero, block)])


def head_merge(turned):
    half, rows = turned.shape[0] // 2, turned.shape[1] // 2
    return jnp.concatenate([turned[:half, :rows], turned[half:, rows:]]).T


def chunk_scores(chunk, keys, stack, near_bias, bias_ref, prompt_len):
    scores = matmul_nt(keys, stack)
    if chunk == 0:
        bias = bias_ref[...]
        return scores + jnp.concatenate([bias, bias], axis=1)
    tri = (PROMPT_DEV, PROMPT_DEV)
    after = lax.broadcasted_iota(jnp.int32, tri, 0) > lax.broadcasted_iota(jnp.int32, tri, 1)
    diag = jnp.where(after, f32(masked_score), f32(0.0))
    last = keys.shape[0] - PROMPT_DEV
    near_end = prompt_len + CONT_DEV
    pieces = [scores[:prompt_len], scores[prompt_len:near_end] + near_bias]
    if last > near_end:
        pieces.append(scores[near_end:last])
    pieces.append(scores[last:] + jnp.concatenate([diag, diag], axis=1))
    return jnp.concatenate(pieces)


def chunk_keys(chunk, prompt_len):
    return prompt_len if chunk == 0 else prompt_len + CONT_DEV + PROMPT_DEV * chunk


def attend_kernel(prompt_len, near_ref, q_ref, k_ref, v_ref, bias_ref, out_ref, log_ref):
    scale = bf16(1.0 / math.sqrt(q_ref.shape[1] // 2))
    chunks = q_ref.shape[0] // PROMPT_DEV

    def scores_of(chunk):
        stack = head_stack(q_ref[pl.ds(chunk * PROMPT_DEV, PROMPT_DEV), :] * scale)
        keys = k_ref[: chunk_keys(chunk, prompt_len), :]
        return chunk_scores(chunk, keys, stack, near_ref[0], bias_ref, prompt_len)

    scores = scores_of(0)
    for chunk in range(chunks):
        rows = pl.ds(chunk * PROMPT_DEV, PROMPT_DEV)
        size = chunk_keys(chunk, prompt_len)
        later = scores_of(chunk + 1) if chunk + 1 < chunks else None
        top = jnp.max(scores, axis=0, keepdims=True)
        weights = jnp.exp(scores - top)
        total = jnp.sum(weights, axis=0, keepdims=True)
        mixed = matmul_tn(v_ref[:size, :], rounded(weights)) / total
        out_ref[rows, :] = rounded(head_merge(mixed))
        log_ref[0, chunk : chunk + 1, :] = top + jnp.log(total)
        scores = later


def attend_back_kernel(
    prompt_len,
    near_ref,
    q_ref,
    k_ref,
    v_ref,
    bias_ref,
    log_ref,
    out_ref,
    grad_ref,
    dq_ref,
    first_ref,
    second_ref,
    near_out_ref,
    own_ref,
    dk_ref,
    dv_ref,
):
    scale = 1.0 / math.sqrt(q_ref.shape[1] // 2)
    half = q_ref.shape[1] // 2
    dk_ref[...] = jnp.zeros_like(dk_ref)
    dv_ref[...] = jnp.zeros_like(dv_ref)
    for chunk in range(q_ref.shape[0] // PROMPT_DEV):
        rows = pl.ds(chunk * PROMPT_DEV, PROMPT_DEV)
        size = chunk_keys(chunk, prompt_len)
        stack = head_stack(q_ref[rows, :] * bf16(scale))
        grad = grad_ref[rows, :]
        grad_stack = head_stack(grad)
        product = (grad.astype(f32) * out_ref[rows, :].astype(f32)).T
        inner = jnp.concatenate(
            [
                jnp.sum(product[:half], axis=0, keepdims=True),
                jnp.sum(product[half:], axis=0, keepdims=True),
            ],
            axis=1,
        )
        keys = k_ref[:size, :]
        scores = chunk_scores(chunk, keys, stack, near_ref[0], bias_ref, prompt_len)
        weights = jnp.exp(scores - log_ref[0, chunk : chunk + 1, :])
        dv_ref[:size, :] += matmul(rounded(weights), grad_stack)
        grad_prob = matmul_nt(v_ref[:size, :], grad_stack)
        grad_score = rounded(weights * (grad_prob - inner))
        dk_ref[:size, :] += matmul(grad_score, stack)
        dq_ref[rows, :] = rounded(head_merge(matmul_tn(keys, grad_score)) * scale)
    start = 0
    for ref in (first_ref, second_ref, near_out_ref, own_ref):
        count = ref.shape[1]
        ref[0] = rounded(dk_ref[start : start + count, :])
        ref[1] = rounded(dv_ref[start : start + count, :])
        start += count


def attend(near_bias, queries, keys, values, bias):
    rows, width = queries.shape
    size = keys.shape[0]
    prompt_len = bias.shape[0]
    lanes = 2 * width // HEADS
    pairs = HEADS // 2
    chunks = rows // PROMPT_DEV
    block = lambda count: pl.BlockSpec((count, lanes), lambda j: (0, j))
    return pl.pallas_call(
        functools.partial(attend_kernel, prompt_len),
        grid=(pairs,),
        in_specs=[
            pl.BlockSpec(memory_space=pltpu.SMEM),
            block(rows),
            block(size),
            block(size),
            pl.BlockSpec((prompt_len, PROMPT_DEV), lambda j: (0, 0)),
        ],
        out_specs=[
            block(rows),
            pl.BlockSpec((1, chunks, 2 * PROMPT_DEV), lambda j: (j, 0, 0)),
        ],
        out_shape=[
            jax.ShapeDtypeStruct((rows, width), bf16),
            jax.ShapeDtypeStruct((pairs, chunks, 2 * PROMPT_DEV), f32),
        ],
        compiler_params=params("arbitrary"),
        cost_estimate=cost(16 * rows * size * width, 4 * (rows + size) * width, rows * size * HEADS),
        name="attend",
    )(near_bias, queries, keys, values, bias)


def attend_back(near_bias, queries, keys, values, bias, log_total, attended, grad):
    rows, width = queries.shape
    size = keys.shape[0]
    prompt_len = bias.shape[0]
    lanes = 2 * width // HEADS
    pairs = HEADS // 2
    chunks = rows // PROMPT_DEV
    block = lambda count: pl.BlockSpec((count, lanes), lambda j: (0, j))
    counts = (prompt_len // 2, prompt_len // 2, CONT_DEV, CONT_DEV)
    return pl.pallas_call(
        functools.partial(attend_back_kernel, prompt_len),
        grid=(pairs,),
        in_specs=[
            pl.BlockSpec(memory_space=pltpu.SMEM),
            block(rows),
            block(size),
            block(size),
            pl.BlockSpec((prompt_len, PROMPT_DEV), lambda j: (0, 0)),
            pl.BlockSpec((1, chunks, 2 * PROMPT_DEV), lambda j: (j, 0, 0)),
            block(rows),
            block(rows),
        ],
        out_specs=[block(rows)]
        + [pl.BlockSpec((2, count, lanes), lambda j: (0, 0, j)) for count in counts],
        out_shape=[jax.ShapeDtypeStruct((rows, width), bf16)]
        + [jax.ShapeDtypeStruct((2, count, width), bf16) for count in counts],
        scratch_shapes=[pltpu.VMEM((size, lanes), f32), pltpu.VMEM((size, lanes), f32)],
        compiler_params=params("arbitrary"),
        cost_estimate=cost(40 * rows * size * width, 8 * (rows + size) * width, rows * size * HEADS),
        name="attend_back",
    )(near_bias, queries, keys, values, bias, log_total, attended, grad)


def local(
    tokens_in,
    cotangent,
    hash_ids,
    norm1_gain,
    norm1_bias,
    w_query,
    w_key,
    w_value,
    w_output,
    norm2_gain,
    norm2_bias,
    expert_in,
    expert_out,
):
    row_count, width = tokens_in.shape
    experts = lax.axis_size("expert")
    groups = lax.axis_size("group")
    position = lax.axis_index("expert")
    group = lax.axis_index("group")
    capacity = 2 * row_count // experts
    slots = experts * capacity
    tied = lax.optimization_barrier

    def all_exchanged(values):
        return lax.all_to_all(values, "expert", split_axis=0, concat_axis=0, tiled=True)

    def exchanged(values):
        got = all_exchanged(values.reshape(experts, capacity, width))
        return got.reshape(slots, width)

    near_tokens = lax.ppermute(
        tokens_in[PROMPT_DEV:], "expert", [(i, i + 1) for i in range(0, experts, 2)]
    )
    prompts, prompt_ids, near_tokens, last_tokens = gather_relative(
        tokens_in[:PROMPT_DEV], "expert", near_tokens
    )
    ids = jnp.broadcast_to(rounded(hash_ids), (row_count, 128))
    all_cot = lax.all_gather(jnp.concatenate([cotangent, ids], axis=1), "group")

    row_index = jnp.arange(row_count, dtype=jnp.int32)
    lower = rounded(row_index[:, None] >= row_index[None, :])

    routed = rounded(hash_ids == jnp.arange(experts, dtype=jnp.int32)[None, :])
    running = matmul(lower, routed)
    rank = (jnp.sum(running * routed.astype(f32), axis=-1) - 1.0).astype(jnp.int32)
    slot = hash_ids[:, 0] * capacity + rank
    spread = rounded(slot[None, :] == jnp.arange(slots, dtype=jnp.int32)[:, None])

    cot_sent, _ = tied((matmul(spread, cotangent, bf16), last_tokens))
    cot = {0: exchanged(cot_sent)}
    others_in, queries, keys, values = project(
        prompts + [near_tokens, tokens_in[PROMPT_DEV:]],
        norm1_gain,
        norm1_bias,
        w_query,
        w_key,
        w_value,
    )
    block_pos = jnp.stack([(position ^ r) * PROMPT_DEV for r in prompt_ids])
    prompt_pos = jnp.arange(PROMPT_DEV, dtype=jnp.int32)
    key_pos = (block_pos[:, None] + prompt_pos[None, :]).reshape(-1)
    query_pos = position * PROMPT_DEV + row_index[:PROMPT_DEV]
    bias = jnp.where(key_pos[:, None] <= query_pos[None, :], f32(0.0), f32(masked_score))
    near_bias = jnp.where(position % 2 == 1, f32(0.0), f32(masked_score))[None]
    attended, log_total = attend(near_bias, queries, keys, values, bias)

    residual = tokens_in.astype(f32) + matmul(attended, w_output)
    ffn_in = rounded(normalize(residual, norm2_gain, norm2_bias)[0])
    rows = exchanged(matmul(spread, ffn_in, bf16))
    all_numbers = all_cot[:, :, width].astype(jnp.int32)[:, None]
    numbers = lambda masks: jnp.stack([group ^ mask for mask in masks])
    near_sent = spread_rows(numbers([1]), all_numbers, all_cot, experts)
    grad_hidden = expert_back(cot[0], expert_out)
    rows, grad_hidden, near_sent = tied((rows, grad_hidden, near_sent))
    all_rows = lax.all_gather(rows, "group")
    cot[1] = all_exchanged(near_sent)
    hidden, grad_pre, grad_rows = expert_front(rows, grad_hidden, expert_in)
    grad_rows, hidden, cot[1] = tied((grad_rows, hidden, cot[1]))
    grad_got = exchanged(grad_rows)
    produced = expert_produce(hidden, expert_out)
    far_sent = spread_rows(numbers(range(2, groups)), all_numbers, all_cot, experts, produced)
    far_sent, grad_got = tied((far_sent, grad_got))
    far_got = all_exchanged(far_sent)

    grad_resid, grad_attn, grad_attended, sums2 = resid_back(
        grad_got, spread, residual, norm2_gain, cotangent, w_output
    )
    grad_queries, back_first, back_second, back_near, back_own = attend_back(
        near_bias, queries, keys, values, bias, log_total, attended, grad_attended
    )
    backs = (back_first, back_second, back_near, back_own, grad_queries)
    prompt_sums = scatter_relative(back_first, back_second, "expert")
    prompt_sent = next(prompt_sums)
    near_back = lax.ppermute(
        back_near, "expert", [(i + 1, i) for i in range(0, experts, 2)]
    )
    weights = weight_parts(
        (position & 1)[None],
        attended,
        others_in,
        grad_attn,
        grad_queries,
        (back_first, back_second, back_near, back_own),
        groups,
        experts,
    )
    place, _ = tied((group[None], weights))
    own_part = own_out(place, groups, hidden, cot[0])
    weights, prompt_sent, near_back, far_got, own_part = tied(
        (weights, prompt_sent, near_back, far_got, own_part)
    )
    marks = []
    weight_sums = weight_chain(*weights, marks)
    weight_sent = next(weight_sums)
    prompt_sent, prompt_back = moved_on(prompt_sums, prompt_sent)
    result_got = far_got[:, 0].reshape(slots, width)
    result = rounded(residual + matmul_tn(spread, result_got))
    weight_sent, prompt_sent, result = tied((weight_sent, prompt_sent, result))
    weight_sent, _ = moved_on(weight_sums, weight_sent)
    number, _ = tied((numbers(range(groups)), marks[-1]))
    operands = (expert_in, expert_out, (rows, grad_pre), all_rows, cot[1], far_got)
    in_first, *hidden_first = in_sums(number, 0, *operands)
    over_group = lambda values: lax.all_to_all(
        values, "group", split_axis=0, concat_axis=0, tiled=True
    )
    got_first = over_group(in_first)
    weight_sent, prompt_sent, _ = tied((weight_sent, prompt_sent, in_first))
    weight_sent, _ = moved_on(weight_sums, weight_sent)
    prompt_sent, prompt_back = moved_on(prompt_sums, prompt_sent)
    number, _ = tied((number, marks[-1]))
    in_second, *hidden_second = in_sums(number, 1, *operands)
    got_first, in_second, prompt_sent, weight_sent = tied(
        (got_first, in_second, prompt_sent, weight_sent)
    )
    got_second = over_group(in_second)
    prompt_sent, weight_sent, _ = tied((prompt_sent, weight_sent, in_second))
    while prompt_sent is not None:
        prompt_sent, prompt_back = moved_on(prompt_sums, prompt_sent)
    grad_tokens, sums1 = input_back(
        prompt_back,
        back_own,
        near_back,
        grad_queries,
        w_query,
        w_key,
        w_value,
        tokens_in,
        norm1_gain,
        grad_resid,
    )
    weight_sent, own_part, sums1 = tied((weight_sent, own_part, sums1))
    weight_sent, weight_grads = moved_on(weight_sums, weight_sent)
    grad_expert_out = out_sums(own_part, cot[1], far_got, hidden_first + hidden_second)
    vectors = jnp.concatenate([sums1, sums2])
    vectors, got_second, grad_expert_out, weight_sent = tied(
        (vectors, got_second, grad_expert_out, weight_sent)
    )
    vectors = vector_sums(vectors)
    while weight_sent is not None:
        weight_sent, weight_grads = moved_on(weight_sums, weight_sent)
    grad_expert_in = lay_out([got_first, got_second])
    grad_w_output, grad_w_query, grad_w_key, grad_w_value = weight_grads
    return (
        result,
        grad_tokens,
        vectors[0],
        vectors[1],
        grad_w_query,
        grad_w_key,
        grad_w_value,
        grad_w_output,
        vectors[2],
        vectors[3],
        grad_expert_in,
        grad_expert_out,
    )


def solution(mesh):
    both = ("group", "expert")
    return jax.shard_map(
        local,
        mesh=mesh,
        in_specs=(
            P(both, None),
            P(both, None),
            P(both, None),
            P(),
            P(),
            P(),
            P(),
            P(),
            P(),
            P(),
            P(),
            P("expert", None, None),
            P("expert", None, None),
        ),
        out_specs=(
            P(both, None),
            P(both, None),
            P(both),
            P(both),
            P(both, None),
            P(both, None),
            P(both, None),
            P(both, None),
            P(both),
            P(both),
            P("expert", "group", None),
            P("expert", "group", None),
        ),
        check_vma=False,
    )
```
